32 devices in a mesh: fsdp: 4 (over z), ctx: 2 (over x), tp: 4 (over y, core).
Axes of the slice: x: 2, y: 2, z: 4, core: 2. Of those that a mesh axis runs over, the one named last changes fastest.
Arguments:
- residual: bfloat16 [8, 1024, 1024], P('fsdp', ('ctx', 'tp')), may hold values from -6 to 6
- query_weight: bfloat16 [1024, 1024], P('fsdp', 'tp'), may hold values from -0.1875 to 0.1875
- key_weight: bfloat16 [1024, 1024], P('fsdp', 'tp'), may hold values from -0.1875 to 0.1875
- value_weight: bfloat16 [1024, 1024], P('fsdp', 'tp'), may hold values from -0.1875 to 0.1875
- output_weight: bfloat16 [1024, 1024], P('tp', 'fsdp'), may hold values from -0.1875 to 0.1875
- sharpness: float32 [1024], P('tp'), may hold values from 1 to 1.8
- attend_rate: float32 [1024], replicated, may hold values from 0.15 to 0.9
- up_weight: bfloat16 [1024, 4096], P('fsdp', 'tp'), may hold values from -0.1875 to 0.1875
- gate_weight: bfloat16 [1024, 4096], P('fsdp', 'tp'), may hold values from -0.1875 to 0.1875
- down_weight: bfloat16 [4096, 1024], P('tp', 'fsdp'), may hold values from -0.09375 to 0.09375
- amplitude: float32 [4096], P('tp'), may hold values from 0.5 to 2
- steepness: float32 [4096], P('tp'), may hold values from 0.5 to 2
- mixer_rate: float32 [1024], replicated, may hold values from 0.15 to 0.9
- block_ids: int32 [8, 1024], P('fsdp'), may hold values from 0 to 4, as said below
- positions: int32 [8, 1024], P('fsdp', 'ctx'), may hold values from 0 to 4095
- cotangent: bfloat16 [8, 1024, 1024], P('fsdp', ('ctx', 'tp')), may hold values from -6 to 6
Outputs:
- layer_out: bfloat16 [8, 1024, 1024], P('fsdp', ('ctx', 'tp'))
- grad_input: float32 [8, 1024, 1024], P('fsdp', ('ctx', 'tp'))
- grad_query: float32 [1024, 1024], P('fsdp', 'tp')
- grad_key: float32 [1024, 1024], P('fsdp', 'tp')
- grad_value: float32 [1024, 1024], P('fsdp', 'tp')
- grad_output: float32 [1024, 1024], P('tp', 'fsdp')
- grad_sharpness: float32 [1024], replicated
- grad_attend: float32 [1024], replicated
- grad_up: float32 [1024, 4096], P('fsdp', 'tp')
- grad_gate: float32 [1024, 4096], P('fsdp', 'tp')
- grad_down: float32 [4096, 1024], P('tp', 'fsdp')
- grad_amplitude: float32 [4096], replicated
- grad_steepness: float32 [4096], replicated
- grad_mixer: float32 [1024], replicated
The draws below stay inside these ranges and needn't reach their ends.
Inputs may be any that keep to these rules, and one draw needn't show every extreme that they name: `block_ids`: in each sequence the block id of the token at index t is (t + offset) // 256, with an offset of 1 to 255 drawn for each sequence: full blocks of 256 tokens, a shorter first and last block.
All inputs are finite; a program needn't handle non-finite values.
Results may differ from the reference program's by a relative error of at most 0.02.
Values may be sent and summed in bfloat16 or wider, within the bound.
A program may use at most 128 MiB of HBM per device.

```python
import math
import jax
import jax.numpy as jnp
from jax import lax

D = 1024
HEADS = 16
HD = 64
FF = 4096
SEQ_DEV = 2
LEN = 1024
BLK = 256
SEQS = 8


def draw_block_ids(key, part):
    offset = jax.random.randint(jax.random.fold_in(key, 17), (SEQS, 1), 1, BLK)
    index = jnp.arange(LEN, dtype=jnp.int32)[None, :]
    return ((index + offset) // BLK).astype(jnp.int32)


def with_ends(values, rng, least, largest):
    shape = values.shape
    place = [jax.random.randint(jax.random.fold_in(rng, axis), (), 0, shape[axis]) for axis in range(len(shape))]
    values = values.at[tuple(place)].set(least)
    longest = shape.index(max(shape))
    place[longest] = (place[longest] + 1) % shape[longest]
    return values.at[tuple(place)].set(largest)


def level_of(own_key, shape, cuts, smallest, high):
    gain = 1.0
    for position, shards_of in cuts:
        draws = jax.random.uniform(jax.random.fold_in(jax.random.fold_in(own_key, 6), position), (shards_of,), jnp.float32, smallest / len(cuts), high / len(cuts))
        gain = gain * jnp.repeat(jnp.exp(draws), shape[position] // shards_of).reshape((-1,) + (1,) * (len(shape) - 1 - position))
    return gain


def gaussian(rng, dims, scale, most, shards=(), kind=jnp.bfloat16):
    result = jax.random.normal(rng, dims, jnp.float32) * scale
    if len(shards) > 0:
        result = level_of(rng, dims, shards, -0.22, 0.18) * result
    return jnp.clip(result, min=-most, max=most).astype(kind)


def setup_inputs(seed: int = 0) -> dict:
    splits = jax.random.split(jax.random.key(seed), 17)
    residual = gaussian(splits[0], (SEQS, LEN, D), 1.0, 6.0, ((0, 4), (1, 8)))
    query_weight = gaussian(splits[1], (D, D), D ** -0.5, 0.1875, ((0, 4), (1, 4)))
    key_weight = gaussian(splits[2], (D, D), D ** -0.5, 0.1875, ((0, 4), (1, 4)))
    value_weight = gaussian(splits[3], (D, D), D ** -0.5, 0.1875, ((0, 4), (1, 4)))
    output_weight = gaussian(splits[4], (D, D), D ** -0.5, 0.1875, ((0, 4), (1, 4)))
    sharpness = jnp.clip(jnp.exp(math.log(1.8) - 0.5877866 * jax.random.uniform(splits[5], (D,), jnp.float32) ** level_of(splits[5], (D,), ((0, 4),), -0.2, 0.2)), 1.0, 1.8)
    attend_rate = jnp.clip(jnp.exp(jax.random.uniform(splits[6], (D,), jnp.float32, math.log(0.15), math.log(0.9))), 0.15, 0.9)
    up_weight = gaussian(splits[7], (D, FF), D ** -0.5, 0.1875, ((0, 4), (1, 4)))
    gate_weight = gaussian(splits[8], (D, FF), D ** -0.5, 0.1875, ((0, 4), (1, 4)))
    down_weight = gaussian(splits[9], (FF, D), FF ** -0.5, 0.09375, ((0, 4), (1, 4)))
    amplitude = jnp.clip(jnp.exp(math.log(2.0) - 1.3862944 * jax.random.uniform(splits[10], (FF,), jnp.float32) ** level_of(splits[10], (FF,), ((0, 4),), -0.2, 0.2)), 0.5, 2.0)
    steepness = jnp.clip(jnp.exp(math.log(2.0) - 1.3862944 * jax.random.uniform(splits[11], (FF,), jnp.float32) ** level_of(splits[11], (FF,), ((0, 4),), -0.2, 0.2)), 0.5, 2.0)
    mixer_rate = jnp.clip(jnp.exp(jax.random.uniform(splits[12], (D,), jnp.float32, math.log(0.15), math.log(0.9))), 0.15, 0.9)
    block_ids = draw_block_ids(jax.random.fold_in(splits[16], 71), 0)
    positions = with_ends(jax.random.randint(splits[14], (SEQS, LEN), 0, 4 * LEN), jax.random.fold_in(splits[14], 1), 0, (4 * LEN) - 1).astype(jnp.int32)
    cotangent = gaussian(splits[15], (SEQS, LEN, D), 1.0, 6.0, ((0, 4), (1, 8)))
    return {"residual": residual, "query_weight": query_weight, "key_weight": key_weight, "value_weight": value_weight, "output_weight": output_weight, "sharpness": sharpness, "attend_rate": attend_rate, "up_weight": up_weight, "gate_weight": gate_weight, "down_weight": down_weight, "amplitude": amplitude, "steepness": steepness, "mixer_rate": mixer_rate, "block_ids": block_ids, "positions": positions, "cotangent": cotangent}


norm_eps = 1e-06
rope_base = 10000.0

@jax.custom_vjp
def low(v):
    return lax.optimization_barrier(v.astype(jnp.bfloat16)).astype(jnp.float32)

@jax.custom_vjp
def low_back(v):
    return v

def low_keep(v):
    return (low(v), None)

def low_pass(kept, grad):
    return (grad,)

def back_keep(v):
    return (v, None)

def back_low(kept, grad):
    return (low(grad),)
low.defvjp(low_keep, low_pass)
low_back.defvjp(back_keep, back_low)

def unit_rows(values):
    return values * lax.rsqrt(lax.optimization_barrier(jnp.mean(values * values, axis=-1, keepdims=True)) + norm_eps)

def rotate_pairs(values, angles):
    middle = values.shape[-1] // 2
    leading = values[..., :middle]
    trailing = values[..., middle:]
    cosine = jnp.cos(angles)[..., None, :]
    sine_part = jnp.sin(angles)[..., None, :]
    return jnp.concatenate([leading * cosine - trailing * sine_part, trailing * cosine + leading * sine_part], axis=-1)

def angles_for(positions, head_size):
    middle = head_size // 2
    frequency = rope_base ** (-2.0 * jnp.arange(middle).astype(jnp.float32) / head_size)
    return positions.astype(jnp.float32)[..., None] * frequency

def prepare_heads(projected, angles, gains, head_size):
    heads_here = projected.shape[-1] // head_size
    shaped = projected.reshape(projected.shape[:-1] + (heads_here, head_size))
    normed = unit_rows(rotate_pairs(shaped, angles)) * gains.reshape(heads_here, head_size)
    return normed.reshape(projected.shape)

def project(left, right):
    return jnp.einsum('gld,de->gle', left, right, precision=lax.Precision.HIGHEST)

def attend_sequence(operands):
    seq_query, seq_key, seq_value, seq_ids = operands
    shaped_query = seq_query.reshape(seq_query.shape[0], HEADS, HD)
    shaped_key = seq_key.reshape(seq_key.shape[0], HEADS, HD)
    shaped_value = seq_value.reshape(seq_value.shape[0], HEADS, HD)
    scores = jnp.einsum('qhd,khd->hqk', shaped_query, shaped_key, precision=lax.Precision.HIGHEST) / math.sqrt(HD)
    scores = low_back(scores)
    allowed = seq_ids[None, :] <= seq_ids[:, None]
    scores = jnp.where(allowed[None], scores, -1e+30)
    row_max = lax.optimization_barrier(jnp.max(scores, axis=-1, keepdims=True))
    exponent = jnp.exp(scores - row_max)
    weights_low = low(exponent / lax.optimization_barrier(jnp.sum(exponent, axis=-1, keepdims=True)))
    attended_seq = jnp.einsum('hqk,khd->qhd', weights_low, shaped_value, precision=lax.Precision.HIGHEST)
    return attended_seq.reshape(seq_query.shape)

def layer_forward(layer_in, params, group_ids, group_positions):
    query_weight, key_weight, value_weight, output_weight, sharpness, attend_rate, up_weight, gate_weight, down_weight, amplitude, steepness, mixer_rate = params
    angles = angles_for(group_positions, HD)
    queries = low(prepare_heads(low_back(project(layer_in, query_weight)), angles, sharpness, HD))
    keys_ready = low(prepare_heads(low_back(project(layer_in, key_weight)), angles, sharpness, HD))
    values_ready = low(low_back(project(layer_in, value_weight)))
    attended = lax.map(jax.checkpoint(attend_sequence), (queries, keys_ready, values_ready, group_ids))
    attended = low(low_back(attended))
    branch_attend = low_back(project(attended, output_weight))
    first = unit_rows(layer_in + attend_rate * (unit_rows(branch_attend) - layer_in))
    first_low = low(first)
    upper = low_back(project(first_low, up_weight))
    gated_raw = low_back(project(first_low, gate_weight))
    scaled = gated_raw * steepness
    hidden = low(upper * amplitude * (scaled * jax.nn.sigmoid(scaled)))
    branch_mixer = low_back(project(hidden, down_weight))
    return unit_rows(first + mixer_rate * (unit_rows(branch_mixer) - first))

def reference(residual, query_weight, key_weight, value_weight, output_weight, sharpness, attend_rate, up_weight, gate_weight, down_weight, amplitude, steepness, mixer_rate, block_ids, positions, cotangent):
    params = (query_weight.astype(jnp.float32), key_weight.astype(jnp.float32), value_weight.astype(jnp.float32), output_weight.astype(jnp.float32), sharpness.astype(jnp.float32), attend_rate.astype(jnp.float32), up_weight.astype(jnp.float32), gate_weight.astype(jnp.float32), down_weight.astype(jnp.float32), amplitude.astype(jnp.float32), steepness.astype(jnp.float32), mixer_rate.astype(jnp.float32))
    groups = SEQS // SEQ_DEV

    def regroup(values):
        return values.reshape((groups, SEQ_DEV) + values.shape[1:])

    def group_step(totals, operands):
        group_res, group_ids, group_positions, group_cot = operands

        def forward_only(layer_in, weights):
            return layer_forward(layer_in, weights, group_ids, group_positions)
        outcome, pullback = jax.vjp(forward_only, group_res, params)
        grad_in, grad_params = pullback(group_cot)
        totals = jax.tree.map(jnp.add, totals, grad_params)
        return (totals, (outcome.astype(jnp.bfloat16), grad_in))
    initial = jax.tree.map(jnp.zeros_like, params)
    totals, (outputs, input_grads) = lax.scan(group_step, initial, (regroup(residual.astype(jnp.float32)), regroup(block_ids), regroup(positions), regroup(cotangent.astype(jnp.float32))))
    return (outputs.reshape(SEQS, LEN, D), input_grads.reshape(SEQS, LEN, D), totals[0], totals[1], totals[2], totals[3], totals[4], totals[5], totals[6], totals[7], totals[8], totals[9], totals[10], totals[11])
```

```python
import math

import jax
import jax.numpy as jnp
from jax import lax
from jax.sharding import PartitionSpec as P

HD = 64
norm_eps = 1e-06
rope_base = 10000.0
BF = jnp.bfloat16
F32 = jnp.float32


def unit_rows(values):
    return values * lax.rsqrt(jnp.mean(values * values, axis=-1, keepdims=True) + norm_eps)


def rotate_pairs(values, angles):
    middle = values.shape[-1] // 2
    leading = values[..., :middle]
    trailing = values[..., middle:]
    cosine = jnp.cos(angles)[..., None, :]
    sine_part = jnp.sin(angles)[..., None, :]
    return jnp.concatenate(
        [leading * cosine - trailing * sine_part, trailing * cosine + leading * sine_part], axis=-1
    )


def angles_for(positions, head_size):
    middle = head_size // 2
    frequency = rope_base ** (-2.0 * jnp.arange(middle).astype(F32) / head_size)
    return positions.astype(F32)[..., None] * frequency


def prepare_heads(projected, angles, gains, head_size):
    heads_here = projected.shape[-1] // head_size
    shaped = projected.reshape(projected.shape[:-1] + (heads_here, head_size))
    normed = unit_rows(rotate_pairs(shaped, angles)) * gains.reshape(heads_here, head_size)
    return normed.reshape(projected.shape)


def product(left, right):
    return jnp.dot(left, right, preferred_element_type=F32)


def transposed_left(left, right):
    return lax.dot_general(left, right, (((0,), (0,)), ((), ())), preferred_element_type=F32)


def transposed_right(left, right):
    return lax.dot_general(left, right, (((1,), (1,)), ((), ())), preferred_element_type=F32)


def gather_rows(values):
    return lax.all_gather(values, "tp", axis=1, tiled=True)


def reduce_rows(values):
    return lax.psum_scatter(values.astype(BF), "tp", scatter_dimension=1, tiled=True).astype(F32)


def branch_mix(branch, base, rate):
    return unit_rows(base + rate * (unit_rows(branch) - base))


def activate(upper, gated_raw, amplitude, steepness):
    scaled = gated_raw * steepness
    return upper * amplitude * (scaled * jax.nn.sigmoid(scaled))


def trade(values, sizes):
    n = sizes["ctx"]
    me = lax.axis_index("ctx")
    if n == 2:
        own = lax.dynamic_index_in_dim(values, me, 0, keepdims=False)
        other = lax.dynamic_index_in_dim(values, 1 - me, 0, keepdims=False)
        got = lax.ppermute(other, "ctx", [(0, 1), (1, 0)])
        first = jnp.where(me == 0, own, got)
        second = jnp.where(me == 0, got, own)
        return jnp.stack([first, second])
    return lax.all_to_all(values, "ctx", split_axis=0, concat_axis=0, tiled=True)


def attend_both(query_low, key_low, value_low, ids):
    length, width = query_low.shape
    heads = width // HD
    q = query_low.reshape(length, heads, HD)
    k = key_low.reshape(length, heads, HD)
    v = value_low.reshape(length, heads, HD)
    scores = jnp.einsum("qhd,khd->hqk", q, k, preferred_element_type=F32) / math.sqrt(HD)
    allowed = ids[None, :] <= ids[:, None]
    scores = jnp.where(allowed[None], scores, -1e30)
    row_max = jnp.max(scores, axis=-1, keepdims=True)
    exponent = jnp.exp(scores - row_max)
    row_total = jnp.sum(exponent, axis=-1, keepdims=True)
    weights_low = (exponent / row_total).astype(BF)
    out = jnp.einsum("hqk,khd->qhd", weights_low, v, preferred_element_type=F32)
    return out.reshape(length, width).astype(BF), (row_max + jnp.log(row_total))[..., 0]


def attend_back(query_low, key_low, value_low, ids, logsum, grad):
    length, width = query_low.shape
    heads = width // HD
    q = query_low.reshape(length, heads, HD)
    k = key_low.reshape(length, heads, HD)
    v = value_low.reshape(length, heads, HD)
    g = grad.reshape(length, heads, HD)
    scores = jnp.einsum("qhd,khd->hqk", q, k, preferred_element_type=F32) / math.sqrt(HD)
    allowed = ids[None, :] <= ids[:, None]
    scores = jnp.where(allowed[None], scores, -1e30)
    soft = jnp.exp(scores - logsum[..., None])
    grad_v = jnp.einsum("hqk,qhd->khd", soft.astype(BF), g, preferred_element_type=F32)
    grad_w = jnp.einsum("qhd,khd->hqk", g, v, preferred_element_type=F32)
    grad_s = soft * (grad_w - jnp.sum(grad_w * soft, axis=-1, keepdims=True))
    low = grad_s.astype(BF)
    grad_q = jnp.einsum("hqk,khd->qhd", low, k, preferred_element_type=F32) / math.sqrt(HD)
    grad_k = jnp.einsum("hqk,qhd->khd", low, q, preferred_element_type=F32) / math.sqrt(HD)
    return (
        grad_q.reshape(length, width),
        grad_k.reshape(length, width),
        grad_v.reshape(length, width),
    )


def per_device(sizes):
    def run(
        residual,
        query_weight,
        key_weight,
        value_weight,
        output_weight,
        sharpness,
        attend_rate,
        up_weight,
        gate_weight,
        down_weight,
        amplitude,
        steepness,
        mixer_rate,
        block_ids,
        positions,
        cotangent,
    ):
        z = sizes["fsdp"]
        width = residual.shape[2]
        hidden_here = up_weight.shape[1]
        heads_width = query_weight.shape[1]

        mine = trade(residual, sizes)
        qkv_shard = jnp.concatenate([query_weight, key_weight, value_weight], axis=1)
        full_qkv = lax.all_gather(qkv_shard, "fsdp", axis=0, tiled=True)
        full_output = lax.all_gather(output_weight, "fsdp", axis=1, tiled=True)
        ug_shard = jnp.concatenate([up_weight, gate_weight], axis=1)
        full_ug = lax.all_gather(ug_shard, "fsdp", axis=0, tiled=True)
        full_down = lax.all_gather(down_weight, "fsdp", axis=1, tiled=True)

        ctx = lax.axis_index("ctx")
        ids = lax.dynamic_index_in_dim(block_ids, ctx, 0, keepdims=False)
        all_positions = lax.all_gather(positions, "ctx", axis=1, tiled=True)
        my_positions = lax.dynamic_index_in_dim(all_positions, ctx, 0, keepdims=False)
        angles = angles_for(my_positions, HD)

        gathered = gather_rows(mine)
        shape3 = gathered.shape
        flat_in = gathered.reshape(-1, width)
        raw = product(flat_in, full_qkv)
        raw_query, raw_key, raw_value = jnp.split(raw, 3, axis=1)

        def prepare_local(projected, gains):
            return prepare_heads(projected, angles, gains, HD)

        query_ready, query_back = jax.vjp(prepare_local, raw_query, sharpness)
        key_ready, key_back = jax.vjp(prepare_local, raw_key, sharpness)
        query_low = query_ready.astype(BF)
        key_low = key_ready.astype(BF)
        value_low = raw_value.astype(BF)
        attended, logsum = attend_both(query_low, key_low, value_low, ids)
        attend_sum = reduce_rows(product(attended, full_output).reshape(shape3))
        residual_float = mine.astype(F32)
        first, attend_back_mix = jax.vjp(branch_mix, attend_sum, residual_float, attend_rate)
        first_all = gather_rows(first.astype(BF)).reshape(-1, width)
        ug_raw = product(first_all, full_ug)
        up_raw, gate_raw = ug_raw[:, :hidden_here], ug_raw[:, hidden_here:]
        hidden, activate_back = jax.vjp(activate, up_raw, gate_raw, amplitude, steepness)
        hidden_low = hidden.astype(BF)
        down_sum = reduce_rows(product(hidden_low, full_down).reshape(shape3))
        outcome, mixer_back = jax.vjp(branch_mix, down_sum, first, mixer_rate)
        layer_out = trade(outcome.astype(BF), sizes)
        my_cot = trade(cotangent, sizes)
        grad_down_sum, grad_first, grad_mixer_part = mixer_back(my_cot.astype(F32))
        down_grad_all = gather_rows(grad_down_sum.astype(BF)).reshape(-1, width)
        grad_hidden = transposed_right(down_grad_all, full_down)
        grad_down_part = transposed_left(hidden_low, down_grad_all)
        grad_up_raw, grad_gate_raw, grad_amplitude_part, grad_steepness_part = activate_back(
            grad_hidden
        )
        ug_grad = jnp.concatenate([grad_up_raw.astype(BF), grad_gate_raw.astype(BF)], axis=1)
        first_back = transposed_right(ug_grad, full_ug)
        grad_first = grad_first + reduce_rows(first_back.reshape(shape3))
        grad_ug_part = transposed_left(first_all, ug_grad)
        grad_attend_sum, grad_residual, grad_attend_part = attend_back_mix(grad_first)
        attend_grad_all = gather_rows(grad_attend_sum.astype(BF)).reshape(-1, width)
        grad_output_part = transposed_left(attended, attend_grad_all)
        grad_attended = transposed_right(attend_grad_all, full_output).astype(BF)
        grad_query_ready, grad_key_ready, grad_value_ready = attend_back(
            query_low, key_low, value_low, ids, logsum, grad_attended
        )
        grad_raw_query, sharp_query = query_back(grad_query_ready)
        grad_raw_key, sharp_key = key_back(grad_key_ready)
        qkv_grad = jnp.concatenate(
            [grad_raw_query.astype(BF), grad_raw_key.astype(BF), grad_value_ready.astype(BF)], axis=1
        )
        input_back = transposed_right(qkv_grad, full_qkv)
        grad_input = grad_residual + reduce_rows(input_back.reshape(shape3))
        grad_input = trade(grad_input.astype(BF), sizes).astype(F32)
        grad_qkv_part = transposed_left(flat_in, qkv_grad)

        def sum_rows(part):
            share = lax.psum_scatter(
                part.astype(BF), ("fsdp", "ctx"), scatter_dimension=0, tiled=True
            )
            return lax.all_gather(share, "ctx", axis=0, tiled=True).astype(F32)

        def sum_columns(part):
            share = lax.psum_scatter(
                part.astype(BF), ("fsdp", "ctx"), scatter_dimension=1, tiled=True
            )
            return lax.all_gather(share, "ctx", axis=1, tiled=True).astype(F32)

        grad_down = sum_columns(grad_down_part)
        grad_ug = sum_rows(grad_ug_part)
        grad_output = sum_columns(grad_output_part)
        grad_qkv = sum_rows(grad_qkv_part)
        grad_up, grad_gate = grad_ug[:, :hidden_here], grad_ug[:, hidden_here:]
        grad_query, grad_key, grad_value = jnp.split(grad_qkv, 3, axis=1)
        tensor_index = lax.axis_index("tp")
        tp = sizes["tp"]

        def spread_slice(section):
            return lax.dynamic_update_slice_in_dim(
                jnp.zeros((section.shape[0] * tp,), F32),
                section,
                tensor_index * section.shape[0],
                0,
            )

        grad_sharpness, grad_amplitude, grad_steepness, grad_attend, grad_mixer = lax.psum(
            (
                spread_slice(sharp_query + sharp_key),
                spread_slice(grad_amplitude_part),
                spread_slice(grad_steepness_part),
                grad_attend_part,
                grad_mixer_part,
            ),
            ("fsdp", "ctx", "tp"),
        )
        return (
            layer_out,
            grad_input,
            grad_query,
            grad_key,
            grad_value,
            grad_output,
            grad_sharpness,
            grad_attend,
            grad_up,
            grad_gate,
            grad_down,
            grad_amplitude,
            grad_steepness,
            grad_mixer,
        )

    return run


def solution(mesh):
    return jax.shard_map(
        per_device(dict(mesh.shape)),
        mesh=mesh,
        in_specs=(
            P("fsdp", ("ctx", "tp"), None),
            P("fsdp", "tp"),
            P("fsdp", "tp"),
            P("fsdp", "tp"),
            P("tp", "fsdp"),
            P("tp"),
            P(),
            P("fsdp", "tp"),
            P("fsdp", "tp"),
            P("tp", "fsdp"),
            P("tp"),
            P("tp"),
            P(),
            P("fsdp", None),
            P("fsdp", "ctx"),
            P("fsdp", ("ctx", "tp"), None),
        ),
        out_specs=(
            P("fsdp", ("ctx", "tp"), None),
            P("fsdp", ("ctx", "tp"), None),
            P("fsdp", "tp"),
            P("fsdp", "tp"),
            P("fsdp", "tp"),
            P("tp", "fsdp"),
            P(),
            P(),
            P("fsdp", "tp"),
            P("fsdp", "tp"),
            P("tp", "fsdp"),
            P(),
            P(),
            P(),
        ),
        check_vma=False,
    )
```

```python
import functools
import math

import jax
import jax.numpy as jnp
from jax import lax
from jax.experimental import pallas as pl
from jax.experimental.pallas import tpu as pltpu
from jax.sharding import PartitionSpec as P

HD = 64
norm_eps = 1e-06
rope_base = 10000.0
BF = jnp.bfloat16
F32 = jnp.float32
MESH = pl.DeviceIdType.MESH
IN_VMEM = pl.BlockSpec(memory_space=pltpu.VMEM)


def remote(source, target, send, receive, **where):
    return pltpu.make_async_remote_copy(
        src_ref=source,
        dst_ref=target,
        send_sem=send,
        recv_sem=receive,
        device_id=where,
        device_id_type=MESH,
    )


def meet(peers):
    barrier = pltpu.get_barrier_semaphore()
    for where in peers:
        pl.semaphore_signal(barrier, inc=1, device_id=where, device_id_type=MESH)
    pl.semaphore_wait(barrier, len(peers))


def tensor_peers():
    me = lax.axis_index("tp")
    core = lax.rem(me, 2)
    chip = lax.div(me, 2)
    return (
        me,
        chip * 2 + (1 - core),
        (1 - chip) * 2 + core,
        (1 - chip) * 2 + (1 - core),
    )


def row_chunks(halves, rows, parts):
    step = rows // parts
    return [(h, pl.ds(i * step, step)) for h in range(halves) for i in range(parts)]


def gather_kernel(chunks, x_ref, out_ref, local_sem, send, receive):
    me, partner, across, _ = tensor_peers()
    meet([{"tp": partner}, {"tp": across}])
    own = pltpu.make_async_copy(x_ref, out_ref.at[:, me], local_sem)
    own.start()
    count = len(chunks)
    over, side, relay = [], [], []
    for i, (h, rows) in enumerate(chunks):
        over.append(
            remote(
                x_ref.at[h, rows],
                out_ref.at[h, me, rows],
                send.at[i],
                receive.at[i],
                tp=across,
            )
        )
        over[-1].start()
    for i, (h, rows) in enumerate(chunks):
        side.append(
            remote(
                x_ref.at[h, rows],
                out_ref.at[h, me, rows],
                send.at[count + i],
                receive.at[count + i],
                tp=partner,
            )
        )
        side[-1].start()
    for i, (h, rows) in enumerate(chunks):
        over[i].wait_recv()
        relay.append(
            remote(
                out_ref.at[h, across, rows],
                out_ref.at[h, across, rows],
                send.at[2 * count + i],
                receive.at[2 * count + i],
                tp=partner,
            )
        )
        relay[-1].start()
    for i in range(count):
        side[i].wait_recv()
        relay[i].wait_recv()
    for i in range(count):
        over[i].wait_send()
        side[i].wait_send()
        relay[i].wait_send()
    own.wait()


def tensor_gather(values):
    halves, rows, width = values.shape
    chunks = row_chunks(halves, rows, 2)
    return pl.pallas_call(
        functools.partial(gather_kernel, chunks),
        out_shape=jax.ShapeDtypeStruct((halves, 4, rows, width), values.dtype),
        in_specs=[IN_VMEM],
        out_specs=IN_VMEM,
        scratch_shapes=[
            pltpu.SemaphoreType.DMA,
            pltpu.SemaphoreType.DMA((3 * len(chunks),)),
            pltpu.SemaphoreType.DMA((3 * len(chunks),)),
        ],
        compiler_params=pltpu.CompilerParams(collective_id=0, has_side_effects=True),
        cost_estimate=pl.CostEstimate(flops=0, bytes_accessed=40_000_000, transcendentals=0),
        name="tensor_gather",
    )(values)


def scatter_kernel(chunks, p_ref, out_ref, pair, mine, far, joined, send, receive):
    me, partner, across, diagonal = tensor_peers()
    meet([{"tp": partner}, {"tp": across}])
    count = len(chunks)
    first, second, third = [], [], []
    for i, (h, rows) in enumerate(chunks):
        first.append(
            remote(
                p_ref.at[h, diagonal, rows],
                pair.at[h, rows],
                send.at[i],
                receive.at[i],
                tp=partner,
            )
        )
        first[-1].start()
    for i, (h, rows) in enumerate(chunks):
        second.append(
            remote(
                p_ref.at[h, partner, rows],
                mine.at[h, rows],
                send.at[count + i],
                receive.at[count + i],
                tp=partner,
            )
        )
        second[-1].start()
    for i, (h, rows) in enumerate(chunks):
        first[i].wait_recv()
        joined[h, rows] = (
            p_ref[h, across, rows].astype(F32) + pair[h, rows].astype(F32)
        ).astype(BF)
        third.append(
            remote(
                joined.at[h, rows],
                far.at[h, rows],
                send.at[2 * count + i],
                receive.at[2 * count + i],
                tp=across,
            )
        )
        if i > 0:
            third[i - 1].start()
    for i, (h, rows) in enumerate(chunks):
        second[i].wait_recv()
        out_ref[h, rows] = p_ref[h, me, rows].astype(F32) + mine[h, rows].astype(F32)
        if i == 0:
            third[-1].start()
    for i, (h, rows) in enumerate(chunks):
        third[i].wait_recv()
        out_ref[h, rows] += far[h, rows].astype(F32)
    for i in range(count):
        first[i].wait_send()
        second[i].wait_send()
        third[i].wait_send()


def tensor_scatter(partial):
    halves, _, rows, width = partial.shape
    chunks = row_chunks(halves, rows, 2)
    block = pltpu.VMEM((halves, rows, width), BF)
    return pl.pallas_call(
        functools.partial(scatter_kernel, chunks),
        out_shape=jax.ShapeDtypeStruct((halves, rows, width), F32),
        in_specs=[IN_VMEM],
        out_specs=IN_VMEM,
        scratch_shapes=[block] * 4
        + [
            pltpu.SemaphoreType.DMA((3 * len(chunks),)),
            pltpu.SemaphoreType.DMA((3 * len(chunks),)),
        ],
        compiler_params=pltpu.CompilerParams(collective_id=1, has_side_effects=True),
        cost_estimate=pl.CostEstimate(flops=0, bytes_accessed=40_000_000, transcendentals=0),
        name="tensor_scatter",
    )(partial)


def opening_kernel(
    n, x_ref, q_ref, k_ref, v_ref, o_ref, out_ref, qkv_ref, full_o_ref, local, send, receive
):
    me, partner, across, _ = tensor_peers()
    ctx = lax.axis_index("ctx")
    other = 1 - ctx
    z = lax.axis_index("fsdp")
    weights = [(q_ref, 0), (k_ref, 1), (v_ref, 2)]
    rows_w = q_ref.shape[0]
    cols_w = q_ref.shape[1]
    half = rows_w // 2
    o_half = o_ref.shape[0] // 2
    o_cols = o_ref.shape[1]
    others = [lax.rem(z + d, n) for d in range(1, n)]
    meet(
        [{"tp": partner}, {"tp": across}, {"ctx": other}] + [{"fsdp": target} for target in others]
    )
    used = [0]

    def launch(source, target, **where):
        i = used[0]
        used[0] += 1
        copy = remote(source, target, send.at[i], receive.at[i], **where)
        copy.start()
        return copy

    def weight_rows(h):
        return pl.ds(pl.multiple_of(h * half, half), half)

    def output_rows(h):
        return pl.ds(pl.multiple_of(h * o_half, o_half), o_half)

    def output_cols(block):
        return pl.ds(pl.multiple_of(block * o_cols, o_cols), o_cols)

    swap = launch(x_ref.at[other], out_ref.at[ctx, me], ctx=other)
    over = [launch(x_ref.at[ctx], out_ref.at[ctx, me], tp=across)]
    side = [launch(x_ref.at[ctx], out_ref.at[ctx, me], tp=partner)]
    along = {}
    order = sorted(range(1, n), key=lambda d: min(d, n - d))
    for d in order:
        target = others[d - 1]
        group = []
        for ref, at in weights:
            group.append(
                launch(
                    ref.at[weight_rows(ctx)],
                    qkv_ref.at[z, weight_rows(ctx), pl.ds(at * cols_w, cols_w)],
                    fsdp=target,
                )
            )
        group.append(
            launch(
                o_ref.at[output_rows(ctx)],
                full_o_ref.at[output_rows(ctx), output_cols(z)],
                fsdp=target,
            )
        )
        along[d] = group
    own = [pltpu.make_async_copy(x_ref.at[ctx], out_ref.at[ctx, me], local.at[0])]
    for ref, at in weights:
        own.append(
            pltpu.make_async_copy(
                ref, qkv_ref.at[z, :, pl.ds(at * cols_w, cols_w)], local.at[1 + at]
            )
        )
    own.append(pltpu.make_async_copy(o_ref, full_o_ref.at[:, output_cols(z)], local.at[4]))
    for copy in own:
        copy.start()
    swap.wait_recv()
    over.append(launch(out_ref.at[other, me], out_ref.at[other, me], tp=across))
    side.append(launch(out_ref.at[other, me], out_ref.at[other, me], tp=partner))
    over[0].wait_recv()
    relay = [launch(out_ref.at[ctx, across], out_ref.at[ctx, across], tp=partner)]
    handed = []
    for d in order:
        for copy in along[d]:
            copy.wait_recv()
        block = lax.rem(z + n - d, n)
        handed.append(
            launch(
                qkv_ref.at[block, weight_rows(ctx)],
                qkv_ref.at[block, weight_rows(ctx)],
                ctx=other,
            )
        )
        handed.append(
            launch(
                full_o_ref.at[output_rows(ctx), output_cols(block)],
                full_o_ref.at[output_rows(ctx), output_cols(block)],
                ctx=other,
            )
        )
        if d == order[0]:
            over[1].wait_recv()
            relay.append(launch(out_ref.at[other, across], out_ref.at[other, across], tp=partner))
    for copy in side + relay + handed:
        copy.wait_recv()
    for copy in [swap] + over + side + relay + handed:
        copy.wait_send()
    for d in order:
        for copy in along[d]:
            copy.wait_send()
    for copy in own:
        copy.wait()


def opening(n, rows, query, key, value, output):
    _, count, width = rows.shape
    copies = 7 + 6 * (n - 1)
    gathered, qkv, full_output = pl.pallas_call(
        functools.partial(opening_kernel, n),
        out_shape=(
            jax.ShapeDtypeStruct((2, 4, count, width), BF),
            jax.ShapeDtypeStruct((n, query.shape[0], 3 * query.shape[1]), BF),
            jax.ShapeDtypeStruct((output.shape[0], n * output.shape[1]), BF),
        ),
        in_specs=[IN_VMEM] * 5,
        out_specs=(IN_VMEM,) * 3,
        scratch_shapes=[
            pltpu.SemaphoreType.DMA((5,)),
            pltpu.SemaphoreType.DMA((copies,)),
            pltpu.SemaphoreType.DMA((copies,)),
        ],
        compiler_params=pltpu.CompilerParams(collective_id=2, has_side_effects=True),
        cost_estimate=pl.CostEstimate(flops=0, bytes_accessed=60_000_000, transcendentals=0),
        name="opening",
    )(rows, query, key, value, output)
    return gathered, qkv.reshape(n * query.shape[0], 3 * query.shape[1]), full_output


def grads_kernel(n, g_ref, out_ref, arrived, reduced, far, total, send, receive):
    ctx = lax.axis_index("ctx")
    other = 1 - ctx
    z = lax.axis_index("fsdp")
    blocks = [lax.rem(z + d, n) for d in range(n)]
    meet([{"ctx": other}] + [{"fsdp": block} for block in blocks[1:]])
    order = sorted(range(1, n), key=lambda d: -min(d, n - d)) + [0]
    near = {}
    for d in order:
        near[d] = remote(
            g_ref.at[blocks[d], other], arrived.at[d], send.at[d], receive.at[d], ctx=other
        )
        near[d].start()
    along = {}
    for step, d in enumerate(order):
        near[d].wait_recv()
        value = g_ref[blocks[d], ctx].astype(F32) + arrived[d].astype(F32)
        if d:
            reduced[d] = value.astype(BF)
            along[d] = remote(
                reduced.at[d], far.at[d], send.at[n + d], receive.at[n + d], fsdp=blocks[d]
            )
        else:
            total[...] = value
        if step:
            along[order[step - 1]].start()
    for d in order[:-1]:
        along[d].wait_recv()
        total[...] += far[d].astype(F32)
    out_ref[ctx] = total[...].astype(BF)
    last = remote(out_ref.at[ctx], out_ref.at[ctx], send.at[0], receive.at[n], ctx=other)
    for d in order:
        near[d].wait_send()
    last.start()
    for d in order[:-1]:
        along[d].wait_send()
    last.wait_recv()
    last.wait_send()


def sum_grads(n, parts):
    total_rows, width = parts.shape
    rows = total_rows // (2 * n)
    out = pl.pallas_call(
        functools.partial(grads_kernel, n),
        out_shape=jax.ShapeDtypeStruct((2, rows, width), BF),
        in_specs=[IN_VMEM],
        out_specs=IN_VMEM,
        scratch_shapes=[
            pltpu.VMEM((n, rows, width), BF),
            pltpu.VMEM((n, rows, width), BF),
            pltpu.VMEM((n, rows, width), BF),
            pltpu.VMEM((rows, width), F32),
            pltpu.SemaphoreType.DMA((2 * n,)),
            pltpu.SemaphoreType.DMA((2 * n,)),
        ],
        compiler_params=pltpu.CompilerParams(collective_id=3, has_side_effects=True),
        cost_estimate=pl.CostEstimate(flops=0, bytes_accessed=120_000_000, transcendentals=0),
        name="sum_grads",
    )(parts.reshape(n, 2, rows, width))
    return out.reshape(2 * rows, width)


def vectors_kernel(n, v_ref, out_ref, group, send, receive):
    me, _, _, _ = tensor_peers()
    ctx = lax.axis_index("ctx")
    z = lax.axis_index("fsdp")
    peers = []
    for d in range(n):
        for flip in range(2):
            if d or flip:
                peers.append({"fsdp": lax.rem(z + d, n), "ctx": lax.rem(ctx + flip, 2)})
    around = [{"tp": lax.rem(me + d, 4)} for d in range(1, 4)]
    meet(peers + around)
    mine = z * 2 + ctx
    copies = []
    for i, where in enumerate(peers):
        copies.append(remote(v_ref, group.at[mine], send.at[i], receive.at[i], **where))
        copies[-1].start()
    group[mine] = v_ref[...]
    for copy in copies:
        copy.wait_recv()
    total = group[0]
    for i in range(1, 2 * n):
        total = total + group[i]
    out_ref[me] = total
    base = len(peers)
    for copy in copies:
        copy.wait_send()
    final = []
    for i, where in enumerate(around):
        final.append(
            remote(out_ref.at[me], out_ref.at[me], send.at[base + i], receive.at[base + i], **where)
        )
        final[-1].start()
    for copy in final:
        copy.wait_recv()
    for copy in final:
        copy.wait_send()


def sum_vectors(n, values):
    rows, width = values.shape
    count = 2 * n - 1 + 3
    return pl.pallas_call(
        functools.partial(vectors_kernel, n),
        out_shape=jax.ShapeDtypeStruct((4, rows, width), F32),
        in_specs=[IN_VMEM],
        out_specs=IN_VMEM,
        scratch_shapes=[
            pltpu.VMEM((2 * n, rows, width), F32),
            pltpu.SemaphoreType.DMA((count,)),
            pltpu.SemaphoreType.DMA((count,)),
        ],
        compiler_params=pltpu.CompilerParams(collective_id=4, has_side_effects=True),
        cost_estimate=pl.CostEstimate(flops=0, bytes_accessed=20_000_000, transcendentals=0),
        name="sum_vectors",
    )(values)


def unit_rows(values):
    return values * lax.rsqrt(jnp.mean(values * values, axis=-1, keepdims=True) + norm_eps)


def rotate_pairs(values, angles):
    middle = values.shape[-1] // 2
    leading = values[..., :middle]
    trailing = values[..., middle:]
    cosine = jnp.cos(angles)[..., None, :]
    sine_part = jnp.sin(angles)[..., None, :]
    return jnp.concatenate(
        [leading * cosine - trailing * sine_part, trailing * cosine + leading * sine_part], axis=-1
    )


def angles_for(positions, head_size):
    middle = head_size // 2
    frequency = rope_base ** (-2.0 * jnp.arange(middle).astype(F32) / head_size)
    return positions.astype(F32)[..., None] * frequency


def prepare_heads(projected, angles, gains, head_size):
    heads_here = projected.shape[-1] // head_size
    shaped = projected.reshape(projected.shape[:-1] + (heads_here, head_size))
    normed = unit_rows(rotate_pairs(shaped, angles)) * gains.reshape(heads_here, head_size)
    return normed.reshape(projected.shape)


def product(left, right):
    return jnp.dot(left, right, preferred_element_type=F32)


def transposed_left(left, right):
    return lax.dot_general(left, right, (((0,), (0,)), ((), ())), preferred_element_type=F32)


def transposed_right(left, right):
    return lax.dot_general(left, right, (((1,), (1,)), ((), ())), preferred_element_type=F32)


def branch_mix(branch, base, rate):
    return unit_rows(base + rate * (unit_rows(branch) - base))


def activate(upper, gated_raw, amplitude, steepness):
    scaled = gated_raw * steepness
    return upper * amplitude * (scaled * jax.nn.sigmoid(scaled))


def trade(values, sizes):
    n = sizes["ctx"]
    me = lax.axis_index("ctx")
    if n == 2:
        own = lax.dynamic_index_in_dim(values, me, 0, keepdims=False)
        other = lax.dynamic_index_in_dim(values, 1 - me, 0, keepdims=False)
        got = lax.ppermute(other, "ctx", [(0, 1), (1, 0)])
        first = jnp.where(me == 0, own, got)
        second = jnp.where(me == 0, got, own)
        return jnp.stack([first, second])
    return lax.all_to_all(values, "ctx", split_axis=0, concat_axis=0, tiled=True)


def swap_halves(share, ctx):
    got = lax.ppermute(share, "ctx", [(0, 1), (1, 0)])
    first = jnp.where(ctx == 0, share, got)
    second = jnp.where(ctx == 0, got, share)
    return jnp.concatenate([first, second], axis=0)


def attend_both(query_low, key_low, value_low, ids):
    length, width = query_low.shape
    heads = width // HD
    q = query_low.reshape(length, heads, HD)
    k = key_low.reshape(length, heads, HD)
    v = value_low.reshape(length, heads, HD)
    scores = jnp.einsum("qhd,khd->hqk", q, k, preferred_element_type=F32) / math.sqrt(HD)
    allowed = ids[None, :] <= ids[:, None]
    scores = jnp.where(allowed[None], scores, -1e30)
    row_max = jnp.max(scores, axis=-1, keepdims=True)
    exponent = jnp.exp(scores - row_max)
    row_total = jnp.sum(exponent, axis=-1, keepdims=True)
    weights_low = (exponent / row_total).astype(BF)
    out = jnp.einsum("hqk,khd->qhd", weights_low, v, preferred_element_type=F32)
    return out.reshape(length, width).astype(BF), (row_max + jnp.log(row_total))[..., 0]


def attend_back(query_low, key_low, value_low, ids, logsum, grad):
    length, width = query_low.shape
    heads = width // HD
    q = query_low.reshape(length, heads, HD)
    k = key_low.reshape(length, heads, HD)
    v = value_low.reshape(length, heads, HD)
    g = grad.reshape(length, heads, HD)
    scores = jnp.einsum("qhd,khd->hqk", q, k, preferred_element_type=F32) / math.sqrt(HD)
    allowed = ids[None, :] <= ids[:, None]
    scores = jnp.where(allowed[None], scores, -1e30)
    soft = jnp.exp(scores - logsum[..., None])
    grad_v = jnp.einsum("hqk,qhd->khd", soft.astype(BF), g, preferred_element_type=F32)
    grad_w = jnp.einsum("qhd,khd->hqk", g, v, preferred_element_type=F32)
    grad_s = soft * (grad_w - jnp.sum(grad_w * soft, axis=-1, keepdims=True))
    low = grad_s.astype(BF)
    grad_q = jnp.einsum("hqk,khd->qhd", low, k, preferred_element_type=F32) / math.sqrt(HD)
    grad_k = jnp.einsum("hqk,qhd->khd", low, q, preferred_element_type=F32) / math.sqrt(HD)
    return (
        grad_q.reshape(length, width),
        grad_k.reshape(length, width),
        grad_v.reshape(length, width),
    )


def per_device(sizes):
    def run(
        residual,
        query_weight,
        key_weight,
        value_weight,
        output_weight,
        sharpness,
        attend_rate,
        up_weight,
        gate_weight,
        down_weight,
        amplitude,
        steepness,
        mixer_rate,
        block_ids,
        positions,
        cotangent,
    ):
        n = sizes["fsdp"]
        tp = sizes["tp"]
        rows, width = residual.shape[1:]
        hidden_here = up_weight.shape[1]
        heads_width = query_weight.shape[1]
        small = n <= 4
        shape4 = (2, tp, rows, width)

        ug_shard = jnp.concatenate([up_weight, gate_weight], axis=1)
        full_ug = lax.all_gather(ug_shard, "fsdp", axis=0, tiled=True)
        full_down = lax.all_gather(down_weight.T, "fsdp", axis=0, tiled=True)
        ctx = lax.axis_index("ctx")
        if small:
            gathered, full_qkv, full_output = opening(
                n, residual, query_weight, key_weight, value_weight, output_weight
            )
            tensor_index = lax.axis_index("tp")
            mine = lax.dynamic_index_in_dim(gathered, tensor_index, 1, keepdims=False)
        else:
            mine = trade(residual, sizes)
            qkv_shard = jnp.concatenate([query_weight, key_weight, value_weight], axis=1)
            full_qkv = lax.all_gather(qkv_shard, "fsdp", axis=0, tiled=True)
            full_output = lax.all_gather(output_weight, "fsdp", axis=1, tiled=True)
            gathered = tensor_gather(mine)

        ids = lax.dynamic_index_in_dim(block_ids, ctx, 0, keepdims=False)
        my_positions = trade(positions, sizes).reshape(-1)
        angles = angles_for(my_positions, HD)

        flat_in = gathered.reshape(-1, width)
        raw = product(flat_in, full_qkv)
        raw_query, raw_key, raw_value = jnp.split(raw, 3, axis=1)

        def prepare_local(projected, gains):
            return prepare_heads(projected, angles, gains, HD)

        query_ready, query_back = jax.vjp(prepare_local, raw_query, sharpness)
        key_ready, key_back = jax.vjp(prepare_local, raw_key, sharpness)
        query_low = query_ready.astype(BF)
        key_low = key_ready.astype(BF)
        value_low = raw_value.astype(BF)
        attended, logsum = attend_both(query_low, key_low, value_low, ids)

        def reduce_rows(partial):
            return tensor_scatter(partial.astype(BF).reshape(shape4))

        def gather_rows(values):
            return tensor_gather(values.astype(BF)).reshape(-1, width)

        attend_sum = reduce_rows(product(attended, full_output))
        residual_float = mine.astype(F32)
        first, attend_back_mix = jax.vjp(branch_mix, attend_sum, residual_float, attend_rate)
        first_all = gather_rows(first)
        ug_raw = product(first_all, full_ug)
        up_raw, gate_raw = ug_raw[:, :hidden_here], ug_raw[:, hidden_here:]
        hidden, activate_back = jax.vjp(activate, up_raw, gate_raw, amplitude, steepness)
        hidden_low = hidden.astype(BF)
        down_sum = reduce_rows(transposed_right(hidden_low, full_down))
        outcome, mixer_back = jax.vjp(branch_mix, down_sum, first, mixer_rate)
        layer_out = trade(outcome.astype(BF), sizes)
        my_cot = trade(cotangent, sizes)
        grad_down_sum, grad_first, grad_mixer_part = mixer_back(my_cot.astype(F32))
        down_grad_all = gather_rows(grad_down_sum)
        grad_hidden = product(down_grad_all, full_down)
        grad_down_part = transposed_left(down_grad_all, hidden_low)
        grad_up_raw, grad_gate_raw, grad_amplitude_part, grad_steepness_part = activate_back(
            grad_hidden
        )
        ug_grad = jnp.concatenate([grad_up_raw.astype(BF), grad_gate_raw.astype(BF)], axis=1)
        grad_first = grad_first + reduce_rows(transposed_right(ug_grad, full_ug))
        grad_ug_part = transposed_left(first_all, ug_grad)
        grad_attend_sum, grad_residual, grad_attend_part = attend_back_mix(grad_first)
        attend_grad_all = gather_rows(grad_attend_sum)
        grad_output_part = transposed_left(attend_grad_all, attended)
        grad_attended = transposed_right(attend_grad_all, full_output).astype(BF)
        grad_query_ready, grad_key_ready, grad_value_ready = attend_back(
            query_low, key_low, value_low, ids, logsum, grad_attended
        )
        grad_raw_query, sharp_query = query_back(grad_query_ready)
        grad_raw_key, sharp_key = key_back(grad_key_ready)
        qkv_grad = jnp.concatenate(
            [grad_raw_query.astype(BF), grad_raw_key.astype(BF), grad_value_ready.astype(BF)], axis=1
        )
        grad_input = grad_residual + reduce_rows(transposed_right(qkv_grad, full_qkv))
        grad_input = trade(grad_input.astype(BF), sizes).astype(F32)
        grad_qkv_part = transposed_left(flat_in, qkv_grad)

        def sum_rows(part):
            share = lax.psum_scatter(
                part.astype(BF), ("fsdp", "ctx"), scatter_dimension=0, tiled=True
            )
            return swap_halves(share, ctx)

        grad_down = sum_rows(grad_down_part).astype(F32).T
        grad_ug = sum_rows(grad_ug_part).astype(F32)
        late = jnp.concatenate([grad_qkv_part.astype(BF), grad_output_part.astype(BF)], axis=1)
        late = (sum_grads(n, late) if small else sum_rows(late)).astype(F32)
        grad_up, grad_gate = grad_ug[:, :hidden_here], grad_ug[:, hidden_here:]
        grad_query, grad_key, grad_value = jnp.split(late[:, : 3 * heads_width], 3, axis=1)
        grad_output = late[:, 3 * heads_width :].T

        vectors = [
            sharp_query + sharp_key,
            grad_amplitude_part,
            grad_steepness_part,
            grad_attend_part,
            grad_mixer_part,
        ]
        lengths = [vector.shape[0] for vector in vectors]
        packed = jnp.concatenate(vectors)
        packed = jnp.pad(packed, (0, -packed.shape[0] % 1024)).reshape(-1, 128)
        if small:
            sums = sum_vectors(n, packed)
        else:
            sums = lax.all_gather(lax.psum(packed, ("fsdp", "ctx")), "tp", axis=0)
        sums = sums.reshape(tp, -1)
        pieces = []
        start = 0
        for length in lengths:
            pieces.append(sums[:, start : start + length])
            start += length
        grad_sharpness, grad_amplitude, grad_steepness = [p.reshape(-1) for p in pieces[:3]]
        grad_attend, grad_mixer = [p.sum(axis=0) for p in pieces[3:]]
        return (
            layer_out,
            grad_input,
            grad_query,
            grad_key,
            grad_value,
            grad_output,
            grad_sharpness,
            grad_attend,
            grad_up,
            grad_gate,
            grad_down,
            grad_amplitude,
            grad_steepness,
            grad_mixer,
        )

    return run


def solution(mesh):
    return jax.shard_map(
        per_device(dict(mesh.shape)),
        mesh=mesh,
        in_specs=(
            P("fsdp", ("ctx", "tp"), None),
            P("fsdp", "tp"),
            P("fsdp", "tp"),
            P("fsdp", "tp"),
            P("tp", "fsdp"),
            P("tp"),
            P(),
            P("fsdp", "tp"),
            P("fsdp", "tp"),
            P("tp", "fsdp"),
            P("tp"),
            P("tp"),
            P(),
            P("fsdp", None),
            P("fsdp", "ctx"),
            P("fsdp", ("ctx", "tp"), None),
        ),
        out_specs=(
            P("fsdp", ("ctx", "tp"), None),
            P("fsdp", ("ctx", "tp"), None),
            P("fsdp", "tp"),
            P("fsdp", "tp"),
            P("fsdp", "tp"),
            P("tp", "fsdp"),
            P(),
            P(),
            P("fsdp", "tp"),
            P("fsdp", "tp"),
            P("tp", "fsdp"),
            P(),
            P(),
            P(),
        ),
        check_vma=False,
    )
```

```python
import functools
import math

import jax
import jax.numpy as jnp
from jax import lax
from jax.experimental import pallas as pl
from jax.experimental.pallas import tpu as pltpu
from jax.sharding import PartitionSpec as P

HD = 64
norm_eps = 1e-06
rope_base = 10000.0
BF = jnp.bfloat16
F32 = jnp.float32
MESH = pl.DeviceIdType.MESH
IN_VMEM = pl.BlockSpec(memory_space=pltpu.VMEM)


def remote(source, target, send, receive, **where):
    return pltpu.make_async_remote_copy(
        src_ref=source,
        dst_ref=target,
        send_sem=send,
        recv_sem=receive,
        device_id=where,
        device_id_type=MESH,
    )


def meet(peers):
    barrier = pltpu.get_barrier_semaphore()
    for where in peers:
        pl.semaphore_signal(barrier, inc=1, device_id=where, device_id_type=MESH)
    pl.semaphore_wait(barrier, len(peers))


def tensor_peers():
    me = lax.axis_index("tp")
    core = lax.rem(me, 2)
    chip = lax.div(me, 2)
    return (
        me,
        chip * 2 + (1 - core),
        (1 - chip) * 2 + core,
        (1 - chip) * 2 + (1 - core),
    )


def row_chunks(halves, rows, parts):
    step = rows // parts
    return [(h, pl.ds(i * step, step)) for h in range(halves) for i in range(parts)]


def gather_kernel(chunks, x_ref, out_ref, local_sem, send, receive):
    me, partner, across, _ = tensor_peers()
    meet([{"tp": partner}, {"tp": across}])
    own = pltpu.make_async_copy(x_ref, out_ref.at[:, me], local_sem)
    own.start()
    count = len(chunks)
    over, side, relay = [], [], []
    for i, (h, rows) in enumerate(chunks):
        over.append(
            remote(
                x_ref.at[h, rows],
                out_ref.at[h, me, rows],
                send.at[i],
                receive.at[i],
                tp=across,
            )
        )
        over[-1].start()
    for i, (h, rows) in enumerate(chunks):
        side.append(
            remote(
                x_ref.at[h, rows],
                out_ref.at[h, me, rows],
                send.at[count + i],
                receive.at[count + i],
                tp=partner,
            )
        )
        side[-1].start()
    for i, (h, rows) in enumerate(chunks):
        over[i].wait_recv()
        relay.append(
            remote(
                out_ref.at[h, across, rows],
                out_ref.at[h, across, rows],
                send.at[2 * count + i],
                receive.at[2 * count + i],
                tp=partner,
            )
        )
        relay[-1].start()
    for i in range(count):
        side[i].wait_recv()
        relay[i].wait_recv()
    for i in range(count):
        over[i].wait_send()
        side[i].wait_send()
        relay[i].wait_send()
    own.wait()


def tensor_gather(values):
    halves, rows, width = values.shape
    chunks = row_chunks(halves, rows, 2)
    return pl.pallas_call(
        functools.partial(gather_kernel, chunks),
        out_shape=jax.ShapeDtypeStruct((halves, 4, rows, width), values.dtype),
        in_specs=[IN_VMEM],
        out_specs=IN_VMEM,
        scratch_shapes=[
            pltpu.SemaphoreType.DMA,
            pltpu.SemaphoreType.DMA((3 * len(chunks),)),
            pltpu.SemaphoreType.DMA((3 * len(chunks),)),
        ],
        compiler_params=pltpu.CompilerParams(collective_id=0, has_side_effects=True),
        cost_estimate=pl.CostEstimate(flops=0, bytes_accessed=40_000_000, transcendentals=0),
        name="tensor_gather",
    )(values)


def scatter_kernel(chunks, p_ref, out_ref, pair, mine, far, joined, send, receive):
    me, partner, across, diagonal = tensor_peers()
    meet([{"tp": partner}, {"tp": across}])
    count = len(chunks)
    first, second, third = [], [], []
    for i, (h, rows) in enumerate(chunks):
        first.append(
            remote(
                p_ref.at[h, diagonal, rows],
                pair.at[h, rows],
                send.at[i],
                receive.at[i],
                tp=partner,
            )
        )
        first[-1].start()
    for i, (h, rows) in enumerate(chunks):
        second.append(
            remote(
                p_ref.at[h, partner, rows],
                mine.at[h, rows],
                send.at[count + i],
                receive.at[count + i],
                tp=partner,
            )
        )
        second[-1].start()
    for i, (h, rows) in enumerate(chunks):
        first[i].wait_recv()
        joined[h, rows] = (
            p_ref[h, across, rows].astype(F32) + pair[h, rows].astype(F32)
        ).astype(BF)
        third.append(
            remote(
                joined.at[h, rows],
                far.at[h, rows],
                send.at[2 * count + i],
                receive.at[2 * count + i],
                tp=across,
            )
        )
        if i > 0:
            third[i - 1].start()
    for i, (h, rows) in enumerate(chunks):
        second[i].wait_recv()
        out_ref[h, rows] = p_ref[h, me, rows].astype(F32) + mine[h, rows].astype(F32)
        if i == 0:
            third[-1].start()
    for i, (h, rows) in enumerate(chunks):
        third[i].wait_recv()
        out_ref[h, rows] += far[h, rows].astype(F32)
    for i in range(count):
        first[i].wait_send()
        second[i].wait_send()
        third[i].wait_send()


def tensor_scatter(partial):
    halves, _, rows, width = partial.shape
    chunks = row_chunks(halves, rows, 2)
    block = pltpu.VMEM((halves, rows, width), BF)
    return pl.pallas_call(
        functools.partial(scatter_kernel, chunks),
        out_shape=jax.ShapeDtypeStruct((halves, rows, width), F32),
        in_specs=[IN_VMEM],
        out_specs=IN_VMEM,
        scratch_shapes=[block] * 4
        + [
            pltpu.SemaphoreType.DMA((3 * len(chunks),)),
            pltpu.SemaphoreType.DMA((3 * len(chunks),)),
        ],
        compiler_params=pltpu.CompilerParams(collective_id=1, has_side_effects=True),
        cost_estimate=pl.CostEstimate(flops=0, bytes_accessed=40_000_000, transcendentals=0),
        name="tensor_scatter",
    )(partial)


def opening_kernel(
    n, x_ref, q_ref, k_ref, v_ref, o_ref, out_ref, qkv_ref, full_o_ref, local, send, receive
):
    me, partner, across, _ = tensor_peers()
    ctx = lax.axis_index("ctx")
    other = 1 - ctx
    z = lax.axis_index("fsdp")
    weights = [(q_ref, 0), (k_ref, 1), (v_ref, 2)]
    rows_w = q_ref.shape[0]
    cols_w = q_ref.shape[1]
    half = rows_w // 2
    o_half = o_ref.shape[0] // 2
    o_cols = o_ref.shape[1]
    others = [lax.rem(z + d, n) for d in range(1, n)]
    meet(
        [{"tp": partner}, {"tp": across}, {"ctx": other}] + [{"fsdp": target} for target in others]
    )
    used = [0]

    def launch(source, target, **where):
        i = used[0]
        used[0] += 1
        copy = remote(source, target, send.at[i], receive.at[i], **where)
        copy.start()
        return copy

    def weight_rows(h):
        return pl.ds(pl.multiple_of(h * half, half), half)

    def output_rows(h):
        return pl.ds(pl.multiple_of(h * o_half, o_half), o_half)

    def output_cols(block):
        return pl.ds(pl.multiple_of(block * o_cols, o_cols), o_cols)

    swap = launch(x_ref.at[other], out_ref.at[ctx, me], ctx=other)
    over = [launch(x_ref.at[ctx], out_ref.at[ctx, me], tp=across)]
    side = [launch(x_ref.at[ctx], out_ref.at[ctx, me], tp=partner)]
    along = {}
    order = sorted(range(1, n), key=lambda d: min(d, n - d))
    for d in order:
        target = others[d - 1]
        group = []
        for ref, at in weights:
            group.append(
                launch(
                    ref.at[weight_rows(ctx)],
                    qkv_ref.at[z, weight_rows(ctx), pl.ds(at * cols_w, cols_w)],
                    fsdp=target,
                )
            )
        group.append(
            launch(
                o_ref.at[output_rows(ctx)],
                full_o_ref.at[output_rows(ctx), output_cols(z)],
                fsdp=target,
            )
        )
        along[d] = group
    own = [pltpu.make_async_copy(x_ref.at[ctx], out_ref.at[ctx, me], local.at[0])]
    for ref, at in weights:
        own.append(
            pltpu.make_async_copy(
                ref, qkv_ref.at[z, :, pl.ds(at * cols_w, cols_w)], local.at[1 + at]
            )
        )
    own.append(pltpu.make_async_copy(o_ref, full_o_ref.at[:, output_cols(z)], local.at[4]))
    for copy in own:
        copy.start()
    swap.wait_recv()
    over.append(launch(out_ref.at[other, me], out_ref.at[other, me], tp=across))
    side.append(launch(out_ref.at[other, me], out_ref.at[other, me], tp=partner))
    over[0].wait_recv()
    relay = [launch(out_ref.at[ctx, across], out_ref.at[ctx, across], tp=partner)]
    handed = []
    for d in order:
        for copy in along[d]:
            copy.wait_recv()
        block = lax.rem(z + n - d, n)
        handed.append(
            launch(
                qkv_ref.at[block, weight_rows(ctx)],
                qkv_ref.at[block, weight_rows(ctx)],
                ctx=other,
            )
        )
        handed.append(
            launch(
                full_o_ref.at[output_rows(ctx), output_cols(block)],
                full_o_ref.at[output_rows(ctx), output_cols(block)],
                ctx=other,
            )
        )
        if d == order[0]:
            over[1].wait_recv()
            relay.append(launch(out_ref.at[other, across], out_ref.at[other, across], tp=partner))
    for copy in side + relay + handed:
        copy.wait_recv()
    for copy in [swap] + over + side + relay + handed:
        copy.wait_send()
    for d in order:
        for copy in along[d]:
            copy.wait_send()
    for copy in own:
        copy.wait()


def opening(n, rows, query, key, value, output):
    _, count, width = rows.shape
    copies = 7 + 6 * (n - 1)
    gathered, qkv, full_output = pl.pallas_call(
        functools.partial(opening_kernel, n),
        out_shape=(
            jax.ShapeDtypeStruct((2, 4, count, width), BF),
            jax.ShapeDtypeStruct((n, query.shape[0], 3 * query.shape[1]), BF),
            jax.ShapeDtypeStruct((output.shape[0], n * output.shape[1]), BF),
        ),
        in_specs=[IN_VMEM] * 5,
        out_specs=(IN_VMEM,) * 3,
        scratch_shapes=[
            pltpu.SemaphoreType.DMA((5,)),
            pltpu.SemaphoreType.DMA((copies,)),
            pltpu.SemaphoreType.DMA((copies,)),
        ],
        compiler_params=pltpu.CompilerParams(collective_id=2, has_side_effects=True),
        cost_estimate=pl.CostEstimate(flops=0, bytes_accessed=60_000_000, transcendentals=0),
        name="opening",
    )(rows, query, key, value, output)
    return gathered, qkv.reshape(n * query.shape[0], 3 * query.shape[1]), full_output


def grads_kernel(
    n,
    g_ref,
    v_ref,
    down_ref,
    ug_ref,
    input_ref,
    out_ref,
    sums_ref,
    full_down_ref,
    full_ug_ref,
    traded_ref,
    arrived,
    reduced,
    far,
    total,
    pair,
    joined,
    group,
    send,
    receive,
    vector_send,
    vector_receive,
    share_send,
    share_receive,
    local,
):
    me, _, _, _ = tensor_peers()
    ctx = lax.axis_index("ctx")
    other = 1 - ctx
    z = lax.axis_index("fsdp")
    blocks = [lax.rem(z + d, n) for d in range(n)]
    around = [lax.rem(me + d, 4) for d in range(1, 4)]
    meet(
        [{"ctx": other}]
        + [{"fsdp": block} for block in blocks[1:]]
        + [{"tp": index} for index in around]
    )
    swap = remote(v_ref, pair, vector_send.at[0], vector_receive.at[0], ctx=other)
    swap.start()
    order = sorted(range(1, n), key=lambda d: -min(d, n - d)) + [0]
    near = {}
    for d in order:
        near[d] = remote(
            g_ref.at[blocks[d], other], arrived.at[d], send.at[d], receive.at[d], ctx=other
        )
        near[d].start()
    shares = [
        remote(input_ref.at[other], traded_ref.at[ctx], share_send.at[0], share_receive.at[0], ctx=other),
        remote(down_ref, full_down_ref.at[ctx], share_send.at[1], share_receive.at[1], ctx=other),
        remote(ug_ref, full_ug_ref.at[ctx], share_send.at[2], share_receive.at[2], ctx=other),
    ]
    own = [
        pltpu.make_async_copy(input_ref.at[ctx], traded_ref.at[ctx], local.at[0]),
        pltpu.make_async_copy(down_ref, full_down_ref.at[ctx], local.at[1]),
        pltpu.make_async_copy(ug_ref, full_ug_ref.at[ctx], local.at[2]),
    ]
    for copy in shares + own:
        copy.start()
    swap.wait_recv()
    joined[...] = v_ref[...] + pair[...]
    group[z] = joined[...]
    line = [
        remote(joined, group.at[z], vector_send.at[d], vector_receive.at[d], fsdp=blocks[d])
        for d in range(1, n)
    ]
    along = {}
    for step, d in enumerate(order):
        near[d].wait_recv()
        value = g_ref[blocks[d], ctx].astype(F32) + arrived[d].astype(F32)
        if d:
            reduced[d] = value.astype(BF)
            along[d] = remote(
                reduced.at[d], far.at[d], send.at[n + d], receive.at[n + d], fsdp=blocks[d]
            )
        else:
            total[...] = value
        if step:
            along[order[step - 1]].start()
        if step == 0:
            for copy in line:
                copy.start()
    for copy in line:
        copy.wait_recv()
    summed = group[0]
    for i in range(1, n):
        summed = summed + group[i]
    sums_ref[me] = summed
    ring = [
        remote(
            sums_ref.at[me],
            sums_ref.at[me],
            vector_send.at[n + i],
            vector_receive.at[n + i],
            tp=index,
        )
        for i, index in enumerate(around)
    ]
    for step, d in enumerate(order[:-1]):
        along[d].wait_recv()
        total[...] += far[d].astype(F32)
        if step == 0:
            for copy in ring:
                copy.start()
    out_ref[ctx] = total[...].astype(BF)
    last = remote(out_ref.at[ctx], out_ref.at[ctx], send.at[n], receive.at[n], ctx=other)
    for d in order:
        near[d].wait_send()
    last.start()
    for d in order[:-1]:
        along[d].wait_send()
    for copy in ring + shares:
        copy.wait_recv()
    for copy in [swap] + line + ring + shares:
        copy.wait_send()
    for copy in own:
        copy.wait()
    last.wait_recv()
    last.wait_send()


def sum_grads(n, parts, vectors, down_share, ug_share, traded):
    total_rows, width = parts.shape
    rows = total_rows // (2 * n)
    vector = pltpu.VMEM(vectors.shape, F32)
    out, sums, down, ug, traded = pl.pallas_call(
        functools.partial(grads_kernel, n),
        out_shape=(
            jax.ShapeDtypeStruct((2, rows, width), BF),
            jax.ShapeDtypeStruct((4,) + vectors.shape, F32),
            jax.ShapeDtypeStruct((2,) + down_share.shape, BF),
            jax.ShapeDtypeStruct((2,) + ug_share.shape, BF),
            jax.ShapeDtypeStruct(traded.shape, BF),
        ),
        in_specs=[IN_VMEM] * 5,
        out_specs=(IN_VMEM,) * 5,
        scratch_shapes=[
            pltpu.VMEM((n, rows, width), BF),
            pltpu.VMEM((n, rows, width), BF),
            pltpu.VMEM((n, rows, width), BF),
            pltpu.VMEM((rows, width), F32),
            vector,
            vector,
            pltpu.VMEM((n,) + vectors.shape, F32),
            pltpu.SemaphoreType.DMA((2 * n,)),
            pltpu.SemaphoreType.DMA((2 * n,)),
            pltpu.SemaphoreType.DMA((n + 3,)),
            pltpu.SemaphoreType.DMA((n + 3,)),
            pltpu.SemaphoreType.DMA((3,)),
            pltpu.SemaphoreType.DMA((3,)),
            pltpu.SemaphoreType.DMA((3,)),
        ],
        compiler_params=pltpu.CompilerParams(collective_id=3, has_side_effects=True),
        cost_estimate=pl.CostEstimate(flops=0, bytes_accessed=120_000_000, transcendentals=0),
        name="sum_grads",
    )(parts.reshape(n, 2, rows, width), vectors, down_share, ug_share, traded)
    return (
        out.reshape(2 * rows, width),
        sums,
        down.reshape(-1, down.shape[2]),
        ug.reshape(-1, ug.shape[2]),
        traded,
    )


def unit_rows(values):
    return values * lax.rsqrt(jnp.mean(values * values, axis=-1, keepdims=True) + norm_eps)


def rotate_pairs(values, angles):
    middle = values.shape[-1] // 2
    leading = values[..., :middle]
    trailing = values[..., middle:]
    cosine = jnp.cos(angles)[..., None, :]
    sine_part = jnp.sin(angles)[..., None, :]
    return jnp.concatenate(
        [leading * cosine - trailing * sine_part, trailing * cosine + leading * sine_part], axis=-1
    )


def angles_for(positions, head_size):
    middle = head_size // 2
    frequency = rope_base ** (-2.0 * jnp.arange(middle).astype(F32) / head_size)
    return positions.astype(F32)[..., None] * frequency


def prepare_heads(projected, angles, gains, head_size):
    heads_here = projected.shape[-1] // head_size
    shaped = projected.reshape(projected.shape[:-1] + (heads_here, head_size))
    normed = unit_rows(rotate_pairs(shaped, angles)) * gains.reshape(heads_here, head_size)
    return normed.reshape(projected.shape)


def product(left, right):
    return jnp.dot(left, right, preferred_element_type=F32)


def transposed_left(left, right):
    return lax.dot_general(left, right, (((0,), (0,)), ((), ())), preferred_element_type=F32)


def transposed_right(left, right):
    return lax.dot_general(left, right, (((1,), (1,)), ((), ())), preferred_element_type=F32)


def branch_mix(branch, base, rate):
    return unit_rows(base + rate * (unit_rows(branch) - base))


def activate(upper, gated_raw, amplitude, steepness):
    scaled = gated_raw * steepness
    return upper * amplitude * (scaled * jax.nn.sigmoid(scaled))


def trade(values, sizes):
    n = sizes["ctx"]
    me = lax.axis_index("ctx")
    if n == 2:
        own = lax.dynamic_index_in_dim(values, me, 0, keepdims=False)
        other = lax.dynamic_index_in_dim(values, 1 - me, 0, keepdims=False)
        got = lax.ppermute(other, "ctx", [(0, 1), (1, 0)])
        first = jnp.where(me == 0, own, got)
        second = jnp.where(me == 0, got, own)
        return jnp.stack([first, second])
    return lax.all_to_all(values, "ctx", split_axis=0, concat_axis=0, tiled=True)


def swap_halves(share, ctx):
    got = lax.ppermute(share, "ctx", [(0, 1), (1, 0)])
    first = jnp.where(ctx == 0, share, got)
    second = jnp.where(ctx == 0, got, share)
    return jnp.concatenate([first, second], axis=0)


def attend_both(query_low, key_low, value_low, ids):
    length, width = query_low.shape
    heads = width // HD
    q = query_low.reshape(length, heads, HD)
    k = key_low.reshape(length, heads, HD)
    v = value_low.reshape(length, heads, HD)
    scores = jnp.einsum("qhd,khd->hqk", q, k, preferred_element_type=F32) / math.sqrt(HD)
    allowed = ids[None, :] <= ids[:, None]
    scores = jnp.where(allowed[None], scores, -1e30)
    row_max = jnp.max(scores, axis=-1, keepdims=True)
    exponent = jnp.exp(scores - row_max)
    row_total = jnp.sum(exponent, axis=-1, keepdims=True)
    weights_low = (exponent / row_total).astype(BF)
    out = jnp.einsum("hqk,khd->qhd", weights_low, v, preferred_element_type=F32)
    return out.reshape(length, width).astype(BF), (row_max + jnp.log(row_total))[..., 0]


def attend_back(query_low, key_low, value_low, ids, logsum, grad):
    length, width = query_low.shape
    heads = width // HD
    q = query_low.reshape(length, heads, HD)
    k = key_low.reshape(length, heads, HD)
    v = value_low.reshape(length, heads, HD)
    g = grad.reshape(length, heads, HD)
    scores = jnp.einsum("qhd,khd->hqk", q, k, preferred_element_type=F32) / math.sqrt(HD)
    allowed = ids[None, :] <= ids[:, None]
    scores = jnp.where(allowed[None], scores, -1e30)
    soft = jnp.exp(scores - logsum[..., None])
    grad_v = jnp.einsum("hqk,qhd->khd", soft.astype(BF), g, preferred_element_type=F32)
    grad_w = jnp.einsum("qhd,khd->hqk", g, v, preferred_element_type=F32)
    grad_s = soft * (grad_w - jnp.sum(grad_w * soft, axis=-1, keepdims=True))
    low = grad_s.astype(BF)
    grad_q = jnp.einsum("hqk,khd->qhd", low, k, preferred_element_type=F32) / math.sqrt(HD)
    grad_k = jnp.einsum("hqk,qhd->khd", low, q, preferred_element_type=F32) / math.sqrt(HD)
    return (
        grad_q.reshape(length, width),
        grad_k.reshape(length, width),
        grad_v.reshape(length, width),
    )


def per_device(sizes):
    def run(
        residual,
        query_weight,
        key_weight,
        value_weight,
        output_weight,
        sharpness,
        attend_rate,
        up_weight,
        gate_weight,
        down_weight,
        amplitude,
        steepness,
        mixer_rate,
        block_ids,
        positions,
        cotangent,
    ):
        n = sizes["fsdp"]
        tp = sizes["tp"]
        rows, width = residual.shape[1:]
        hidden_here = up_weight.shape[1]
        heads_width = query_weight.shape[1]
        small = n <= 4
        shape4 = (2, tp, rows, width)

        ctx = lax.axis_index("ctx")

        def own_half(shard):
            half = shard.shape[0] // 2
            return lax.dynamic_slice_in_dim(shard, ctx * half, half, 0)

        ug_half = own_half(jnp.concatenate([up_weight, gate_weight], axis=1))
        down_half = own_half(down_weight.T)
        if small:
            gathered, full_qkv, full_output = opening(
                n, residual, query_weight, key_weight, value_weight, output_weight
            )
            gathered, ug_half, down_half = lax.optimization_barrier((gathered, ug_half, down_half))
            tensor_index = lax.axis_index("tp")
            mine = lax.dynamic_index_in_dim(gathered, tensor_index, 1, keepdims=False)
        else:
            mine = trade(residual, sizes)
            qkv_shard = jnp.concatenate([query_weight, key_weight, value_weight], axis=1)
            full_qkv = lax.all_gather(qkv_shard, "fsdp", axis=0, tiled=True)
            full_output = lax.all_gather(output_weight, "fsdp", axis=1, tiled=True)
            gathered = tensor_gather(mine)
        full_ug = lax.all_gather(ug_half, ("fsdp", "ctx"), axis=0, tiled=True)
        full_down = lax.all_gather(down_half, ("fsdp", "ctx"), axis=0, tiled=True)

        ids = lax.dynamic_index_in_dim(block_ids, ctx, 0, keepdims=False)
        my_positions = trade(positions, sizes).reshape(-1)
        angles = angles_for(my_positions, HD)

        flat_in = gathered.reshape(-1, width)
        raw = product(flat_in, full_qkv)
        raw_query, raw_key, raw_value = jnp.split(raw, 3, axis=1)

        def prepare_local(projected, gains):
            return prepare_heads(projected, angles, gains, HD)

        query_ready, query_back = jax.vjp(prepare_local, raw_query, sharpness)
        key_ready, key_back = jax.vjp(prepare_local, raw_key, sharpness)
        query_low = query_ready.astype(BF)
        key_low = key_ready.astype(BF)
        value_low = raw_value.astype(BF)
        attended, logsum = attend_both(query_low, key_low, value_low, ids)

        def reduce_rows(partial):
            return tensor_scatter(partial.astype(BF).reshape(shape4))

        def gather_rows(values):
            return tensor_gather(values.astype(BF)).reshape(-1, width)

        attend_sum = reduce_rows(product(attended, full_output))
        residual_float = mine.astype(F32)
        first, attend_back_mix = jax.vjp(branch_mix, attend_sum, residual_float, attend_rate)
        first_all = gather_rows(first)
        ug_raw = product(first_all, full_ug)
        up_raw, gate_raw = ug_raw[:, :hidden_here], ug_raw[:, hidden_here:]
        hidden, activate_back = jax.vjp(activate, up_raw, gate_raw, amplitude, steepness)
        hidden_low = hidden.astype(BF)
        down_sum = reduce_rows(transposed_right(hidden_low, full_down))
        outcome, mixer_back = jax.vjp(branch_mix, down_sum, first, mixer_rate)
        layer_out = trade(outcome.astype(BF), sizes)
        my_cot = trade(cotangent, sizes)
        grad_down_sum, grad_first, grad_mixer_part = mixer_back(my_cot.astype(F32))
        down_grad_all = gather_rows(grad_down_sum)
        grad_hidden = product(down_grad_all, full_down)
        grad_down_part = transposed_left(down_grad_all, hidden_low)
        grad_up_raw, grad_gate_raw, grad_amplitude_part, grad_steepness_part = activate_back(
            grad_hidden
        )
        ug_grad = jnp.concatenate([grad_up_raw.astype(BF), grad_gate_raw.astype(BF)], axis=1)
        grad_first = grad_first + reduce_rows(transposed_right(ug_grad, full_ug))
        grad_ug_part = transposed_left(first_all, ug_grad)
        grad_attend_sum, grad_residual, grad_attend_part = attend_back_mix(grad_first)
        attend_grad_all = gather_rows(grad_attend_sum)
        grad_output_part = transposed_left(attend_grad_all, attended)
        grad_attended = transposed_right(attend_grad_all, full_output).astype(BF)
        grad_query_ready, grad_key_ready, grad_value_ready = attend_back(
            query_low, key_low, value_low, ids, logsum, grad_attended
        )
        grad_raw_query, sharp_query = query_back(grad_query_ready)
        grad_raw_key, sharp_key = key_back(grad_key_ready)
        qkv_grad = jnp.concatenate(
            [grad_raw_query.astype(BF), grad_raw_key.astype(BF), grad_value_ready.astype(BF)], axis=1
        )
        grad_input = grad_residual + reduce_rows(transposed_right(qkv_grad, full_qkv))
        grad_input = grad_input.astype(BF)
        grad_qkv_part = transposed_left(flat_in, qkv_grad)

        def scatter_rows(part):
            return lax.psum_scatter(
                part.astype(BF), ("fsdp", "ctx"), scatter_dimension=0, tiled=True
            )

        vectors = [
            sharp_query + sharp_key,
            grad_amplitude_part,
            grad_steepness_part,
            grad_attend_part,
            grad_mixer_part,
        ]
        lengths = [vector.shape[0] for vector in vectors]
        packed = jnp.concatenate(vectors)
        packed = jnp.pad(packed, (0, -packed.shape[0] % 1024)).reshape(-1, 128)
        down_share = scatter_rows(grad_down_part)
        ug_share = scatter_rows(grad_ug_part)
        late = jnp.concatenate([grad_qkv_part.astype(BF), grad_output_part.astype(BF)], axis=1)
        if small:
            late, sums, grad_down, grad_ug, grad_input = sum_grads(
                n, late, packed, down_share, ug_share, grad_input
            )
        else:
            late = swap_halves(scatter_rows(late), ctx)
            sums = lax.all_gather(lax.psum(packed, ("fsdp", "ctx")), "tp", axis=0)
            grad_down = swap_halves(down_share, ctx)
            grad_ug = swap_halves(ug_share, ctx)
            grad_input = trade(grad_input, sizes)
        late = late.astype(F32)
        grad_down = grad_down.astype(F32).T
        grad_ug = grad_ug.astype(F32)
        grad_input = grad_input.astype(F32)
        grad_up, grad_gate = grad_ug[:, :hidden_here], grad_ug[:, hidden_here:]
        grad_query, grad_key, grad_value = jnp.split(late[:, : 3 * heads_width], 3, axis=1)
        grad_output = late[:, 3 * heads_width :].T
        sums = sums.reshape(tp, -1)
        pieces = []
        start = 0
        for length in lengths:
            pieces.append(sums[:, start : start + length])
            start += length
        grad_sharpness, grad_amplitude, grad_steepness = [p.reshape(-1) for p in pieces[:3]]
        grad_attend, grad_mixer = [p.sum(axis=0) for p in pieces[3:]]
        return (
            layer_out,
            grad_input,
            grad_query,
            grad_key,
            grad_value,
            grad_output,
            grad_sharpness,
            grad_attend,
            grad_up,
            grad_gate,
            grad_down,
            grad_amplitude,
            grad_steepness,
            grad_mixer,
        )

    return run


def solution(mesh):
    return jax.shard_map(
        per_device(dict(mesh.shape)),
        mesh=mesh,
        in_specs=(
            P("fsdp", ("ctx", "tp"), None),
            P("fsdp", "tp"),
            P("fsdp", "tp"),
            P("fsdp", "tp"),
            P("tp", "fsdp"),
            P("tp"),
            P(),
            P("fsdp", "tp"),
            P("fsdp", "tp"),
            P("tp", "fsdp"),
            P("tp"),
            P("tp"),
            P(),
            P("fsdp", None),
            P("fsdp", "ctx"),
            P("fsdp", ("ctx", "tp"), None),
        ),
        out_specs=(
            P("fsdp", ("ctx", "tp"), None),
            P("fsdp", ("ctx", "tp"), None),
            P("fsdp", "tp"),
            P("fsdp", "tp"),
            P("fsdp", "tp"),
            P("tp", "fsdp"),
            P(),
            P(),
            P("fsdp", "tp"),
            P("fsdp", "tp"),
            P("tp", "fsdp"),
            P(),
            P(),
            P(),
        ),
        check_vma=False,
    )
```

```python
import functools
import math

import jax
import jax.numpy as jnp
from jax import lax
from jax.experimental import pallas as pl
from jax.experimental.pallas import tpu as pltpu
from jax.sharding import PartitionSpec as P

HD = 64
norm_eps = 1e-06
rope_base = 10000.0
BF = jnp.bfloat16
F32 = jnp.float32
MESH = pl.DeviceIdType.MESH
IN_VMEM = pl.BlockSpec(memory_space=pltpu.VMEM)


def remote(source, target, send, receive, **where):
    return pltpu.make_async_remote_copy(
        src_ref=source,
        dst_ref=target,
        send_sem=send,
        recv_sem=receive,
        device_id=where,
        device_id_type=MESH,
    )


def meet(peers):
    barrier = pltpu.get_barrier_semaphore()
    for where in peers:
        pl.semaphore_signal(barrier, inc=1, device_id=where, device_id_type=MESH)
    pl.semaphore_wait(barrier, len(peers))


def tensor_peers():
    me = lax.axis_index("tp")
    core = lax.rem(me, 2)
    chip = lax.div(me, 2)
    return (
        me,
        chip * 2 + (1 - core),
        (1 - chip) * 2 + core,
        (1 - chip) * 2 + (1 - core),
    )


def row_chunks(halves, rows, parts):
    step = rows // parts
    return [(h, pl.ds(i * step, step)) for h in range(halves) for i in range(parts)]


class Rider:
    arrays = ()
    shapes = ()
    scratch = ()
    remote_copies = 0
    local_copies = 0

    def place(self):
        ctx = lax.axis_index("ctx")
        z = lax.axis_index("fsdp")
        return ctx, 1 - ctx, z

    def finish_copies(self, copies, own):
        for copy in copies:
            copy.wait_recv()
        for copy in copies:
            copy.wait_send()
        for copy in own:
            copy.wait()


class Spread(Rider):
    def __init__(self, n, half):
        self.n = n
        self.arrays = (half,)
        self.shapes = (jax.ShapeDtypeStruct((n,) + half.shape, half.dtype),)
        self.remote_copies = n - 1
        self.local_copies = 1

    def peers(self):
        _, _, z = self.place()
        return [{"fsdp": lax.rem(z + d, self.n)} for d in range(1, self.n)]

    def start(self, inputs, outputs, scratch, send, receive, local):
        _, _, z = self.place()
        own = [pltpu.make_async_copy(inputs[0], outputs[0].at[z], local.at[0])]
        copies = [
            remote(inputs[0], outputs[0].at[z], send.at[i], receive.at[i], **where)
            for i, where in enumerate(self.peers())
        ]
        for copy in copies + own:
            copy.start()
        return lambda: self.finish_copies(copies, own)


class Hand(Rider):
    def __init__(self, n, halves, rest):
        self.n = n
        self.arrays = (halves, rest)
        self.shapes = (jax.ShapeDtypeStruct((n, 2) + rest.shape, rest.dtype),)
        self.remote_copies = n - 1
        self.local_copies = 2

    def peers(self):
        return [{"ctx": self.place()[1]}]

    def start(self, inputs, outputs, scratch, send, receive, local):
        ctx, other, z = self.place()
        halves, rest = inputs
        full = outputs[0]
        copies = []
        for d in range(1, self.n):
            block = lax.rem(z + d, self.n)
            copies.append(
                remote(
                    halves.at[block],
                    full.at[block, ctx],
                    send.at[d - 1],
                    receive.at[d - 1],
                    ctx=other,
                )
            )
        own = [
            pltpu.make_async_copy(halves, full.at[:, ctx], local.at[0]),
            pltpu.make_async_copy(rest, full.at[z, other], local.at[1]),
        ]
        for copy in copies + own:
            copy.start()
        return lambda: self.finish_copies(copies, own)


class Near(Rider):
    def __init__(self, n, partial):
        self.n = n
        block = (n,) + partial.shape[2:]
        self.arrays = (partial,)
        self.shapes = (jax.ShapeDtypeStruct(block, BF),)
        self.scratch = (pltpu.VMEM(block, BF),)
        self.remote_copies = n

    def peers(self):
        return [{"ctx": self.place()[1]}]

    def start(self, inputs, outputs, scratch, send, receive, local):
        ctx, other, _ = self.place()
        partial, out, arrived = inputs[0], outputs[0], scratch[0]
        copies = [
            remote(partial.at[i, other], arrived.at[i], send.at[i], receive.at[i], ctx=other)
            for i in range(self.n)
        ]
        for copy in copies:
            copy.start()

        def finish():
            for i, copy in enumerate(copies):
                copy.wait_recv()
                out[i] = (partial[i, ctx].astype(F32) + arrived[i].astype(F32)).astype(BF)
            for copy in copies:
                copy.wait_send()

        return finish


class Line(Rider):
    def __init__(self, n, terms):
        self.n = n
        self.arrays = (terms,)
        self.shapes = (jax.ShapeDtypeStruct(terms.shape[1:], BF),)
        self.scratch = (pltpu.VMEM((n,) + terms.shape[1:], BF),)
        self.remote_copies = n - 1

    def peers(self):
        _, _, z = self.place()
        return [{"fsdp": lax.rem(z + d, self.n)} for d in range(1, self.n)]

    def start(self, inputs, outputs, scratch, send, receive, local):
        _, _, z = self.place()
        terms, out, far = inputs[0], outputs[0], scratch[0]
        copies = []
        for d in range(1, self.n):
            block = lax.rem(z + d, self.n)
            copies.append(
                remote(
                    terms.at[block], far.at[d], send.at[d - 1], receive.at[d - 1], fsdp=block
                )
            )
            copies[-1].start()

        def finish():
            total = terms[z].astype(F32)
            for d in range(1, self.n):
                copies[d - 1].wait_recv()
                total = total + far[d].astype(F32)
            out[...] = total.astype(BF)
            for copy in copies:
                copy.wait_send()

        return finish


class Swap(Rider):
    def __init__(self, share):
        self.arrays = (share,)
        self.shapes = (jax.ShapeDtypeStruct((2,) + share.shape, share.dtype),)
        self.remote_copies = 1
        self.local_copies = 1

    def peers(self):
        return [{"ctx": self.place()[1]}]

    def start(self, inputs, outputs, scratch, send, receive, local):
        ctx, other, _ = self.place()
        copies = [remote(inputs[0], outputs[0].at[ctx], send.at[0], receive.at[0], ctx=other)]
        own = [pltpu.make_async_copy(inputs[0], outputs[0].at[ctx], local.at[0])]
        for copy in copies + own:
            copy.start()
        return lambda: self.finish_copies(copies, own)


def with_rider(body, rider, own_scratch, *refs):
    if rider is None:
        body([], lambda: (lambda: None), *refs)
        return
    sizes = [1, len(rider.arrays), 1, len(rider.shapes), own_scratch, len(rider.scratch), 3]
    groups = []
    start = 0
    for size in sizes:
        groups.append(refs[start : start + size])
        start += size
    x, inputs, out, outputs, scratch, extra, semaphores = groups

    def launch():
        return rider.start(inputs, outputs, extra, *semaphores)

    body(rider.peers(), launch, *x, *out, *scratch)


def call_tensor(body, array, shape, scratch, rider, number, name):
    own_scratch = len(scratch)
    arrays, shapes = [array], [shape]
    if rider is not None:
        arrays += rider.arrays
        shapes += rider.shapes
        scratch = (
            list(scratch)
            + list(rider.scratch)
            + [
                pltpu.SemaphoreType.DMA((rider.remote_copies,)),
                pltpu.SemaphoreType.DMA((rider.remote_copies,)),
                pltpu.SemaphoreType.DMA((max(rider.local_copies, 1),)),
            ]
        )
    result = pl.pallas_call(
        functools.partial(with_rider, body, rider, own_scratch),
        out_shape=tuple(shapes),
        in_specs=[IN_VMEM] * len(arrays),
        out_specs=(IN_VMEM,) * len(shapes),
        scratch_shapes=scratch,
        compiler_params=pltpu.CompilerParams(collective_id=number, has_side_effects=True),
        cost_estimate=pl.CostEstimate(flops=0, bytes_accessed=40_000_000, transcendentals=0),
        name=name,
    )(*arrays)
    return result[0] if rider is None else result


def gather_kernel(chunks, peers, launch, x_ref, out_ref, local_sem, send, receive):
    me, partner, across, _ = tensor_peers()
    meet([{"tp": partner}, {"tp": across}] + peers)
    own = pltpu.make_async_copy(x_ref, out_ref.at[:, me], local_sem)
    own.start()
    count = len(chunks)
    over, side, relay = [], [], []
    for i, (h, rows) in enumerate(chunks):
        over.append(
            remote(
                x_ref.at[h, rows],
                out_ref.at[h, me, rows],
                send.at[i],
                receive.at[i],
                tp=across,
            )
        )
        over[-1].start()
    for i, (h, rows) in enumerate(chunks):
        side.append(
            remote(
                x_ref.at[h, rows],
                out_ref.at[h, me, rows],
                send.at[count + i],
                receive.at[count + i],
                tp=partner,
            )
        )
        side[-1].start()
    finish = launch()
    for i, (h, rows) in enumerate(chunks):
        over[i].wait_recv()
        relay.append(
            remote(
                out_ref.at[h, across, rows],
                out_ref.at[h, across, rows],
                send.at[2 * count + i],
                receive.at[2 * count + i],
                tp=partner,
            )
        )
        relay[-1].start()
    for i in range(count):
        side[i].wait_recv()
        relay[i].wait_recv()
    for i in range(count):
        over[i].wait_send()
        side[i].wait_send()
        relay[i].wait_send()
    own.wait()
    finish()


def tensor_gather(values, rider=None, number=0):
    halves, rows, width = values.shape
    chunks = row_chunks(halves, rows, 2)
    return call_tensor(
        functools.partial(gather_kernel, chunks),
        values,
        jax.ShapeDtypeStruct((halves, 4, rows, width), values.dtype),
        [
            pltpu.SemaphoreType.DMA,
            pltpu.SemaphoreType.DMA((3 * len(chunks),)),
            pltpu.SemaphoreType.DMA((3 * len(chunks),)),
        ],
        rider,
        number,
        "tensor_gather",
    )


def scatter_kernel(
    chunks, peers, launch, p_ref, out_ref, pair, mine, far, joined, send, receive
):
    me, partner, across, diagonal = tensor_peers()
    meet([{"tp": partner}, {"tp": across}] + peers)
    count = len(chunks)
    first, second, third = [], [], []
    for i, (h, rows) in enumerate(chunks):
        first.append(
            remote(
                p_ref.at[h, diagonal, rows],
                pair.at[h, rows],
                send.at[i],
                receive.at[i],
                tp=partner,
            )
        )
        first[-1].start()
    for i, (h, rows) in enumerate(chunks):
        second.append(
            remote(
                p_ref.at[h, partner, rows],
                mine.at[h, rows],
                send.at[count + i],
                receive.at[count + i],
                tp=partner,
            )
        )
        second[-1].start()
    finish = launch()
    for i, (h, rows) in enumerate(chunks):
        first[i].wait_recv()
        joined[h, rows] = (
            p_ref[h, across, rows].astype(F32) + pair[h, rows].astype(F32)
        ).astype(BF)
        third.append(
            remote(
                joined.at[h, rows],
                far.at[h, rows],
                send.at[2 * count + i],
                receive.at[2 * count + i],
                tp=across,
            )
        )
        if i > 0:
            third[i - 1].start()
    for i, (h, rows) in enumerate(chunks):
        second[i].wait_recv()
        out_ref[h, rows] = p_ref[h, me, rows].astype(F32) + mine[h, rows].astype(F32)
        if i == 0:
            third[-1].start()
    for i, (h, rows) in enumerate(chunks):
        third[i].wait_recv()
        out_ref[h, rows] += far[h, rows].astype(F32)
    for i in range(count):
        first[i].wait_send()
        second[i].wait_send()
        third[i].wait_send()
    finish()


def tensor_scatter(partial, rider=None, number=1):
    halves, _, rows, width = partial.shape
    chunks = row_chunks(halves, rows, 2)
    block = pltpu.VMEM((halves, rows, width), BF)
    return call_tensor(
        functools.partial(scatter_kernel, chunks),
        partial,
        jax.ShapeDtypeStruct((halves, rows, width), F32),
        [block] * 4
        + [
            pltpu.SemaphoreType.DMA((3 * len(chunks),)),
            pltpu.SemaphoreType.DMA((3 * len(chunks),)),
        ],
        rider,
        number,
        "tensor_scatter",
    )


def opening_kernel(
    n, x_ref, q_ref, k_ref, v_ref, o_ref, out_ref, qkv_ref, full_o_ref, local, send, receive
):
    me, partner, across, _ = tensor_peers()
    ctx = lax.axis_index("ctx")
    other = 1 - ctx
    z = lax.axis_index("fsdp")
    weights = [(q_ref, 0), (k_ref, 1), (v_ref, 2)]
    rows_w = q_ref.shape[0]
    cols_w = q_ref.shape[1]
    half = rows_w // 2
    o_half = o_ref.shape[0] // 2
    o_cols = o_ref.shape[1]
    others = [lax.rem(z + d, n) for d in range(1, n)]
    meet(
        [{"tp": partner}, {"tp": across}, {"ctx": other}] + [{"fsdp": target} for target in others]
    )
    used = [0]

    def launch(source, target, **where):
        i = used[0]
        used[0] += 1
        copy = remote(source, target, send.at[i], receive.at[i], **where)
        copy.start()
        return copy

    def weight_rows(h):
        return pl.ds(pl.multiple_of(h * half, half), half)

    def output_rows(h):
        return pl.ds(pl.multiple_of(h * o_half, o_half), o_half)

    def output_cols(block):
        return pl.ds(pl.multiple_of(block * o_cols, o_cols), o_cols)

    swap = launch(x_ref.at[other], out_ref.at[ctx, me], ctx=other)
    over = [launch(x_ref.at[ctx], out_ref.at[ctx, me], tp=across)]
    side = [launch(x_ref.at[ctx], out_ref.at[ctx, me], tp=partner)]
    along = {}
    order = sorted(range(1, n), key=lambda d: min(d, n - d))
    for d in order:
        target = others[d - 1]
        group = []
        for ref, at in weights:
            group.append(
                launch(
                    ref.at[weight_rows(ctx)],
                    qkv_ref.at[z, weight_rows(ctx), pl.ds(at * cols_w, cols_w)],
                    fsdp=target,
                )
            )
        group.append(
            launch(
                o_ref.at[output_rows(ctx)],
                full_o_ref.at[output_rows(ctx), output_cols(z)],
                fsdp=target,
            )
        )
        along[d] = group
    own = [pltpu.make_async_copy(x_ref.at[ctx], out_ref.at[ctx, me], local.at[0])]
    for ref, at in weights:
        own.append(
            pltpu.make_async_copy(
                ref, qkv_ref.at[z, :, pl.ds(at * cols_w, cols_w)], local.at[1 + at]
            )
        )
    own.append(pltpu.make_async_copy(o_ref, full_o_ref.at[:, output_cols(z)], local.at[4]))
    for copy in own:
        copy.start()
    swap.wait_recv()
    over.append(launch(out_ref.at[other, me], out_ref.at[other, me], tp=across))
    side.append(launch(out_ref.at[other, me], out_ref.at[other, me], tp=partner))
    over[0].wait_recv()
    relay = [launch(out_ref.at[ctx, across], out_ref.at[ctx, across], tp=partner)]
    handed = []
    for d in order:
        for copy in along[d]:
            copy.wait_recv()
        block = lax.rem(z + n - d, n)
        handed.append(
            launch(
                qkv_ref.at[block, weight_rows(ctx)],
                qkv_ref.at[block, weight_rows(ctx)],
                ctx=other,
            )
        )
        handed.append(
            launch(
                full_o_ref.at[output_rows(ctx), output_cols(block)],
                full_o_ref.at[output_rows(ctx), output_cols(block)],
                ctx=other,
            )
        )
        if d == order[0]:
            over[1].wait_recv()
            relay.append(launch(out_ref.at[other, across], out_ref.at[other, across], tp=partner))
    for copy in side + relay + handed:
        copy.wait_recv()
    for copy in [swap] + over + side + relay + handed:
        copy.wait_send()
    for d in order:
        for copy in along[d]:
            copy.wait_send()
    for copy in own:
        copy.wait()


def opening(n, rows, query, key, value, output):
    _, count, width = rows.shape
    copies = 7 + 6 * (n - 1)
    gathered, qkv, full_output = pl.pallas_call(
        functools.partial(opening_kernel, n),
        out_shape=(
            jax.ShapeDtypeStruct((2, 4, count, width), BF),
            jax.ShapeDtypeStruct((n, query.shape[0], 3 * query.shape[1]), BF),
            jax.ShapeDtypeStruct((output.shape[0], n * output.shape[1]), BF),
        ),
        in_specs=[IN_VMEM] * 5,
        out_specs=(IN_VMEM,) * 3,
        scratch_shapes=[
            pltpu.SemaphoreType.DMA((5,)),
            pltpu.SemaphoreType.DMA((copies,)),
            pltpu.SemaphoreType.DMA((copies,)),
        ],
        compiler_params=pltpu.CompilerParams(collective_id=2, has_side_effects=True),
        cost_estimate=pl.CostEstimate(flops=0, bytes_accessed=60_000_000, transcendentals=0),
        name="opening",
    )(rows, query, key, value, output)
    return gathered, qkv.reshape(n * query.shape[0], 3 * query.shape[1]), full_output


def grads_kernel(
    n,
    g_ref,
    v_ref,
    ug_ref,
    input_ref,
    out_ref,
    sums_ref,
    full_ug_ref,
    traded_ref,
    arrived,
    reduced,
    far,
    total,
    pair,
    joined,
    group,
    send,
    receive,
    vector_send,
    vector_receive,
    share_send,
    share_receive,
    local,
):
    me, _, _, _ = tensor_peers()
    ctx = lax.axis_index("ctx")
    other = 1 - ctx
    z = lax.axis_index("fsdp")
    blocks = [lax.rem(z + d, n) for d in range(n)]
    around = [lax.rem(me + d, 4) for d in range(1, 4)]
    meet(
        [{"ctx": other}]
        + [{"fsdp": block} for block in blocks[1:]]
        + [{"tp": index} for index in around]
    )
    swap = remote(v_ref, pair, vector_send.at[0], vector_receive.at[0], ctx=other)
    swap.start()
    order = sorted(range(1, n), key=lambda d: -min(d, n - d)) + [0]
    near = {}
    for d in order:
        near[d] = remote(
            g_ref.at[blocks[d], other], arrived.at[d], send.at[d], receive.at[d], ctx=other
        )
        near[d].start()
    shares = [
        remote(input_ref.at[other], traded_ref.at[ctx], share_send.at[0], share_receive.at[0], ctx=other),
        remote(ug_ref, full_ug_ref.at[ctx], share_send.at[1], share_receive.at[1], ctx=other),
    ]
    own = [
        pltpu.make_async_copy(input_ref.at[ctx], traded_ref.at[ctx], local.at[0]),
        pltpu.make_async_copy(ug_ref, full_ug_ref.at[ctx], local.at[1]),
    ]
    for copy in shares + own:
        copy.start()
    swap.wait_recv()
    joined[...] = v_ref[...] + pair[...]
    group[z] = joined[...]
    line = [
        remote(joined, group.at[z], vector_send.at[d], vector_receive.at[d], fsdp=blocks[d])
        for d in range(1, n)
    ]
    along = {}
    for step, d in enumerate(order):
        near[d].wait_recv()
        value = g_ref[blocks[d], ctx].astype(F32) + arrived[d].astype(F32)
        if d:
            reduced[d] = value.astype(BF)
            along[d] = remote(
                reduced.at[d], far.at[d], send.at[n + d], receive.at[n + d], fsdp=blocks[d]
            )
        else:
            total[...] = value
        if step:
            along[order[step - 1]].start()
        if step == 0:
            for copy in line:
                copy.start()
    for copy in line:
        copy.wait_recv()
    summed = group[0]
    for i in range(1, n):
        summed = summed + group[i]
    sums_ref[me] = summed
    ring = [
        remote(
            sums_ref.at[me],
            sums_ref.at[me],
            vector_send.at[n + i],
            vector_receive.at[n + i],
            tp=index,
        )
        for i, index in enumerate(around)
    ]
    for step, d in enumerate(order[:-1]):
        along[d].wait_recv()
        total[...] += far[d].astype(F32)
        if step == 0:
            for copy in ring:
                copy.start()
    out_ref[ctx] = total[...].astype(BF)
    last = remote(out_ref.at[ctx], out_ref.at[ctx], send.at[n], receive.at[n], ctx=other)
    for d in order:
        near[d].wait_send()
    last.start()
    for d in order[:-1]:
        along[d].wait_send()
    for copy in ring + shares:
        copy.wait_recv()
    for copy in [swap] + line + ring + shares:
        copy.wait_send()
    for copy in own:
        copy.wait()
    last.wait_recv()
    last.wait_send()


def sum_grads(n, parts, vectors, ug_share, traded):
    total_rows, width = parts.shape
    rows = total_rows // (2 * n)
    vector = pltpu.VMEM(vectors.shape, F32)
    out, sums, ug, traded = pl.pallas_call(
        functools.partial(grads_kernel, n),
        out_shape=(
            jax.ShapeDtypeStruct((2, rows, width), BF),
            jax.ShapeDtypeStruct((4,) + vectors.shape, F32),
            jax.ShapeDtypeStruct((2,) + ug_share.shape, BF),
            jax.ShapeDtypeStruct(traded.shape, BF),
        ),
        in_specs=[IN_VMEM] * 4,
        out_specs=(IN_VMEM,) * 4,
        scratch_shapes=[
            pltpu.VMEM((n, rows, width), BF),
            pltpu.VMEM((n, rows, width), BF),
            pltpu.VMEM((n, rows, width), BF),
            pltpu.VMEM((rows, width), F32),
            vector,
            vector,
            pltpu.VMEM((n,) + vectors.shape, F32),
            pltpu.SemaphoreType.DMA((2 * n,)),
            pltpu.SemaphoreType.DMA((2 * n,)),
            pltpu.SemaphoreType.DMA((n + 3,)),
            pltpu.SemaphoreType.DMA((n + 3,)),
            pltpu.SemaphoreType.DMA((2,)),
            pltpu.SemaphoreType.DMA((2,)),
            pltpu.SemaphoreType.DMA((2,)),
        ],
        compiler_params=pltpu.CompilerParams(collective_id=3, has_side_effects=True),
        cost_estimate=pl.CostEstimate(flops=0, bytes_accessed=120_000_000, transcendentals=0),
        name="sum_grads",
    )(parts.reshape(n, 2, rows, width), vectors, ug_share, traded)
    return (
        out.reshape(2 * rows, width),
        sums,
        ug.reshape(-1, ug.shape[2]),
        traded,
    )


def unit_rows(values):
    return values * lax.rsqrt(jnp.mean(values * values, axis=-1, keepdims=True) + norm_eps)


def rotate_pairs(values, angles):
    middle = values.shape[-1] // 2
    leading = values[..., :middle]
    trailing = values[..., middle:]
    cosine = jnp.cos(angles)[..., None, :]
    sine_part = jnp.sin(angles)[..., None, :]
    return jnp.concatenate(
        [leading * cosine - trailing * sine_part, trailing * cosine + leading * sine_part], axis=-1
    )


def angles_for(positions, head_size):
    middle = head_size // 2
    frequency = rope_base ** (-2.0 * jnp.arange(middle).astype(F32) / head_size)
    return positions.astype(F32)[..., None] * frequency


def prepare_heads(projected, angles, gains, head_size):
    heads_here = projected.shape[-1] // head_size
    shaped = projected.reshape(projected.shape[:-1] + (heads_here, head_size))
    normed = unit_rows(rotate_pairs(shaped, angles)) * gains.reshape(heads_here, head_size)
    return normed.reshape(projected.shape)


def product(left, right):
    return jnp.dot(left, right, preferred_element_type=F32)


def transposed_left(left, right):
    return lax.dot_general(left, right, (((0,), (0,)), ((), ())), preferred_element_type=F32)


def transposed_right(left, right):
    return lax.dot_general(left, right, (((1,), (1,)), ((), ())), preferred_element_type=F32)


def branch_mix(branch, base, rate):
    return unit_rows(base + rate * (unit_rows(branch) - base))


def activate(upper, gated_raw, amplitude, steepness):
    scaled = gated_raw * steepness
    return upper * amplitude * (scaled * jax.nn.sigmoid(scaled))


def trade(values, sizes):
    n = sizes["ctx"]
    me = lax.axis_index("ctx")
    if n == 2:
        own = lax.dynamic_index_in_dim(values, me, 0, keepdims=False)
        other = lax.dynamic_index_in_dim(values, 1 - me, 0, keepdims=False)
        got = lax.ppermute(other, "ctx", [(0, 1), (1, 0)])
        first = jnp.where(me == 0, own, got)
        second = jnp.where(me == 0, got, own)
        return jnp.stack([first, second])
    return lax.all_to_all(values, "ctx", split_axis=0, concat_axis=0, tiled=True)


def swap_halves(share, ctx):
    got = lax.ppermute(share, "ctx", [(0, 1), (1, 0)])
    first = jnp.where(ctx == 0, share, got)
    second = jnp.where(ctx == 0, got, share)
    return jnp.concatenate([first, second], axis=0)


def attend_both(query_low, key_low, value_low, ids):
    length, width = query_low.shape
    heads = width // HD
    q = query_low.reshape(length, heads, HD)
    k = key_low.reshape(length, heads, HD)
    v = value_low.reshape(length, heads, HD)
    scores = jnp.einsum("qhd,khd->hqk", q, k, preferred_element_type=F32) / math.sqrt(HD)
    allowed = ids[None, :] <= ids[:, None]
    scores = jnp.where(allowed[None], scores, -1e30)
    row_max = jnp.max(scores, axis=-1, keepdims=True)
    exponent = jnp.exp(scores - row_max)
    row_total = jnp.sum(exponent, axis=-1, keepdims=True)
    weights_low = (exponent / row_total).astype(BF)
    out = jnp.einsum("hqk,khd->qhd", weights_low, v, preferred_element_type=F32)
    return out.reshape(length, width).astype(BF), (row_max + jnp.log(row_total))[..., 0]


def attend_back(query_low, key_low, value_low, ids, logsum, grad):
    length, width = query_low.shape
    heads = width // HD
    q = query_low.reshape(length, heads, HD)
    k = key_low.reshape(length, heads, HD)
    v = value_low.reshape(length, heads, HD)
    g = grad.reshape(length, heads, HD)
    scores = jnp.einsum("qhd,khd->hqk", q, k, preferred_element_type=F32) / math.sqrt(HD)
    allowed = ids[None, :] <= ids[:, None]
    scores = jnp.where(allowed[None], scores, -1e30)
    soft = jnp.exp(scores - logsum[..., None])
    grad_v = jnp.einsum("hqk,qhd->khd", soft.astype(BF), g, preferred_element_type=F32)
    grad_w = jnp.einsum("qhd,khd->hqk", g, v, preferred_element_type=F32)
    grad_s = soft * (grad_w - jnp.sum(grad_w * soft, axis=-1, keepdims=True))
    low = grad_s.astype(BF)
    grad_q = jnp.einsum("hqk,khd->qhd", low, k, preferred_element_type=F32) / math.sqrt(HD)
    grad_k = jnp.einsum("hqk,qhd->khd", low, q, preferred_element_type=F32) / math.sqrt(HD)
    return (
        grad_q.reshape(length, width),
        grad_k.reshape(length, width),
        grad_v.reshape(length, width),
    )


def per_device(sizes):
    def run(
        residual,
        query_weight,
        key_weight,
        value_weight,
        output_weight,
        sharpness,
        attend_rate,
        up_weight,
        gate_weight,
        down_weight,
        amplitude,
        steepness,
        mixer_rate,
        block_ids,
        positions,
        cotangent,
    ):
        n = sizes["fsdp"]
        tp = sizes["tp"]
        rows, width = residual.shape[1:]
        hidden_here = up_weight.shape[1]
        heads_width = query_weight.shape[1]
        small = n <= 4
        shape4 = (2, tp, rows, width)

        ctx = lax.axis_index("ctx")

        def half_of(shard, index):
            half = shard.shape[0] // 2
            return lax.dynamic_slice_in_dim(shard, index * half, half, 0)

        ug_half = half_of(jnp.concatenate([up_weight, gate_weight], axis=1), ctx)
        down_half = half_of(down_weight.T, ctx)
        if small:
            gathered, full_qkv, full_output = opening(
                n, residual, query_weight, key_weight, value_weight, output_weight
            )
            gathered, ug_half = lax.optimization_barrier((gathered, ug_half))
            tensor_index = lax.axis_index("tp")
            mine = lax.dynamic_index_in_dim(gathered, tensor_index, 1, keepdims=False)
        else:
            mine = trade(residual, sizes)
            qkv_shard = jnp.concatenate([query_weight, key_weight, value_weight], axis=1)
            full_qkv = lax.all_gather(qkv_shard, "fsdp", axis=0, tiled=True)
            full_output = lax.all_gather(output_weight, "fsdp", axis=1, tiled=True)
            gathered = tensor_gather(mine)
        full_ug = lax.all_gather(ug_half, ("fsdp", "ctx"), axis=0, tiled=True)
        if not small:
            full_down = lax.all_gather(down_half, ("fsdp", "ctx"), axis=0, tiled=True)

        ids = lax.dynamic_index_in_dim(block_ids, ctx, 0, keepdims=False)
        my_positions = trade(positions, sizes).reshape(-1)
        angles = angles_for(my_positions, HD)

        flat_in = gathered.reshape(-1, width)
        raw = product(flat_in, full_qkv)
        raw_query, raw_key, raw_value = jnp.split(raw, 3, axis=1)

        def prepare_local(projected, gains):
            return prepare_heads(projected, angles, gains, HD)

        query_ready, query_back = jax.vjp(prepare_local, raw_query, sharpness)
        key_ready, key_back = jax.vjp(prepare_local, raw_key, sharpness)
        query_low = query_ready.astype(BF)
        key_low = key_ready.astype(BF)
        value_low = raw_value.astype(BF)
        attended, logsum = attend_both(query_low, key_low, value_low, ids)

        def reduce_rows(partial, *rider):
            return tensor_scatter(partial.astype(BF).reshape(shape4), *rider)

        def gather_rows(values, *rider):
            return tensor_gather(values.astype(BF), *rider)

        partial = product(attended, full_output)
        if small:
            attend_sum, down_halves = reduce_rows(partial, Spread(n, down_half), 5)
        else:
            attend_sum = reduce_rows(partial)
        residual_float = mine.astype(F32)
        first, attend_back_mix = jax.vjp(branch_mix, attend_sum, residual_float, attend_rate)
        if small:
            down_rest = half_of(down_weight.T, 1 - ctx)
            first_all, full_down = gather_rows(first, Hand(n, down_halves, down_rest), 6)
            full_down = full_down.reshape(width, hidden_here)
        else:
            first_all = gather_rows(first)
        first_all = first_all.reshape(-1, width)
        ug_raw = product(first_all, full_ug)
        up_raw, gate_raw = ug_raw[:, :hidden_here], ug_raw[:, hidden_here:]
        hidden, activate_back = jax.vjp(activate, up_raw, gate_raw, amplitude, steepness)
        hidden_low = hidden.astype(BF)
        down_sum = reduce_rows(transposed_right(hidden_low, full_down))
        outcome, mixer_back = jax.vjp(branch_mix, down_sum, first, mixer_rate)
        layer_out = trade(outcome.astype(BF), sizes)
        my_cot = trade(cotangent, sizes)
        grad_down_sum, grad_first, grad_mixer_part = mixer_back(my_cot.astype(F32))
        down_grad_all = gather_rows(grad_down_sum).reshape(-1, width)
        grad_hidden = product(down_grad_all, full_down)
        grad_down_part = transposed_left(down_grad_all, hidden_low)
        grad_up_raw, grad_gate_raw, grad_amplitude_part, grad_steepness_part = activate_back(
            grad_hidden
        )
        ug_grad = jnp.concatenate([grad_up_raw.astype(BF), grad_gate_raw.astype(BF)], axis=1)
        grad_ug_part = transposed_left(first_all, ug_grad)
        partial = transposed_right(ug_grad, full_ug)
        if small:
            terms = grad_down_part.astype(BF).reshape(n, 2, -1, hidden_here)
            summed, down_terms = reduce_rows(partial, Near(n, terms), 7)
        else:
            summed = reduce_rows(partial)
        grad_first = grad_first + summed
        grad_attend_sum, grad_residual, grad_attend_part = attend_back_mix(grad_first)
        if small:
            attend_grad_all, down_share = gather_rows(grad_attend_sum, Line(n, down_terms), 8)
        else:
            attend_grad_all = gather_rows(grad_attend_sum)
        attend_grad_all = attend_grad_all.reshape(-1, width)
        grad_output_part = transposed_left(attend_grad_all, attended)
        grad_attended = transposed_right(attend_grad_all, full_output).astype(BF)
        grad_query_ready, grad_key_ready, grad_value_ready = attend_back(
            query_low, key_low, value_low, ids, logsum, grad_attended
        )
        grad_raw_query, sharp_query = query_back(grad_query_ready)
        grad_raw_key, sharp_key = key_back(grad_key_ready)
        qkv_grad = jnp.concatenate(
            [grad_raw_query.astype(BF), grad_raw_key.astype(BF), grad_value_ready.astype(BF)], axis=1
        )
        partial = transposed_right(qkv_grad, full_qkv)
        if small:
            summed, grad_down = reduce_rows(partial, Swap(down_share), 9)
            grad_down = grad_down.reshape(-1, hidden_here)
        else:
            summed = reduce_rows(partial)
        grad_input = grad_residual + summed
        grad_input = grad_input.astype(BF)
        grad_qkv_part = transposed_left(flat_in, qkv_grad)

        def scatter_rows(part):
            return lax.psum_scatter(
                part.astype(BF), ("fsdp", "ctx"), scatter_dimension=0, tiled=True
            )

        vectors = [
            sharp_query + sharp_key,
            grad_amplitude_part,
            grad_steepness_part,
            grad_attend_part,
            grad_mixer_part,
        ]
        lengths = [vector.shape[0] for vector in vectors]
        packed = jnp.concatenate(vectors)
        packed = jnp.pad(packed, (0, -packed.shape[0] % 1024)).reshape(-1, 128)
        ug_share = scatter_rows(grad_ug_part)
        late = jnp.concatenate([grad_qkv_part.astype(BF), grad_output_part.astype(BF)], axis=1)
        if small:
            late, sums, grad_ug, grad_input = sum_grads(n, late, packed, ug_share, grad_input)
        else:
            late = swap_halves(scatter_rows(late), ctx)
            sums = lax.all_gather(lax.psum(packed, ("fsdp", "ctx")), "tp", axis=0)
            grad_down = swap_halves(scatter_rows(grad_down_part), ctx)
            grad_ug = swap_halves(ug_share, ctx)
            grad_input = trade(grad_input, sizes)
        late = late.astype(F32)
        grad_down = grad_down.astype(F32).T
        grad_ug = grad_ug.astype(F32)
        grad_input = grad_input.astype(F32)
        grad_up, grad_gate = grad_ug[:, :hidden_here], grad_ug[:, hidden_here:]
        grad_query, grad_key, grad_value = jnp.split(late[:, : 3 * heads_width], 3, axis=1)
        grad_output = late[:, 3 * heads_width :].T
        sums = sums.reshape(tp, -1)
        pieces = []
        start = 0
        for length in lengths:
            pieces.append(sums[:, start : start + length])
            start += length
        grad_sharpness, grad_amplitude, grad_steepness = [p.reshape(-1) for p in pieces[:3]]
        grad_attend, grad_mixer = [p.sum(axis=0) for p in pieces[3:]]
        return (
            layer_out,
            grad_input,
            grad_query,
            grad_key,
            grad_value,
            grad_output,
            grad_sharpness,
            grad_attend,
            grad_up,
            grad_gate,
            grad_down,
            grad_amplitude,
            grad_steepness,
            grad_mixer,
        )

    return run


def solution(mesh):
    return jax.shard_map(
        per_device(dict(mesh.shape)),
        mesh=mesh,
        in_specs=(
            P("fsdp", ("ctx", "tp"), None),
            P("fsdp", "tp"),
            P("fsdp", "tp"),
            P("fsdp", "tp"),
            P("tp", "fsdp"),
            P("tp"),
            P(),
            P("fsdp", "tp"),
            P("fsdp", "tp"),
            P("tp", "fsdp"),
            P("tp"),
            P("tp"),
            P(),
            P("fsdp", None),
            P("fsdp", "ctx"),
            P("fsdp", ("ctx", "tp"), None),
        ),
        out_specs=(
            P("fsdp", ("ctx", "tp"), None),
            P("fsdp", ("ctx", "tp"), None),
            P("fsdp", "tp"),
            P("fsdp", "tp"),
            P("fsdp", "tp"),
            P("tp", "fsdp"),
            P(),
            P(),
            P("fsdp", "tp"),
            P("fsdp", "tp"),
            P("tp", "fsdp"),
            P(),
            P(),
            P(),
        ),
        check_vma=False,
    )
```

```python
import functools
import math

import jax
import jax.numpy as jnp
from jax import lax
from jax.experimental import pallas as pl
from jax.experimental.layout import Layout, with_layout_constraint
from jax.experimental.pallas import tpu as pltpu
from jax.sharding import PartitionSpec as P

HD = 64
BLK = 256
norm_eps = 1e-06
rope_base = 10000.0
BF = jnp.bfloat16
F32 = jnp.float32
MESH = pl.DeviceIdType.MESH
IN_VMEM = pl.BlockSpec(memory_space=pltpu.VMEM)


def remote(source, target, send, receive, **where):
    return pltpu.make_async_remote_copy(
        src_ref=source,
        dst_ref=target,
        send_sem=send,
        recv_sem=receive,
        device_id=where,
        device_id_type=MESH,
    )


def meet(peers):
    barrier = pltpu.get_barrier_semaphore()
    for where in peers:
        pl.semaphore_signal(barrier, inc=1, device_id=where, device_id_type=MESH)
    pl.semaphore_wait(barrier, len(peers))


def tensor_peers():
    me = lax.axis_index("tp")
    core = lax.rem(me, 2)
    chip = lax.div(me, 2)
    return (
        me,
        chip * 2 + (1 - core),
        (1 - chip) * 2 + core,
        (1 - chip) * 2 + (1 - core),
    )


def row_chunks(halves, rows, parts):
    step = rows // parts
    return [(h, pl.ds(i * step, step)) for h in range(halves) for i in range(parts)]


def gather_kernel(chunks, x_ref, out_ref, local_sem, send, receive):
    me, partner, across, _ = tensor_peers()
    meet([{"tp": partner}, {"tp": across}])
    own = pltpu.make_async_copy(x_ref, out_ref.at[:, me], local_sem)
    own.start()
    count = len(chunks)
    over, side, relay = [], [], []
    for i, (h, rows) in enumerate(chunks):
        over.append(
            remote(
                x_ref.at[h, rows],
                out_ref.at[h, me, rows],
                send.at[i],
                receive.at[i],
                tp=across,
            )
        )
        over[-1].start()
    for i, (h, rows) in enumerate(chunks):
        side.append(
            remote(
                x_ref.at[h, rows],
                out_ref.at[h, me, rows],
                send.at[count + i],
                receive.at[count + i],
                tp=partner,
            )
        )
        side[-1].start()
    for i, (h, rows) in enumerate(chunks):
        over[i].wait_recv()
        relay.append(
            remote(
                out_ref.at[h, across, rows],
                out_ref.at[h, across, rows],
                send.at[2 * count + i],
                receive.at[2 * count + i],
                tp=partner,
            )
        )
        relay[-1].start()
    for i in range(count):
        side[i].wait_recv()
        relay[i].wait_recv()
    for i in range(count):
        over[i].wait_send()
        side[i].wait_send()
        relay[i].wait_send()
    own.wait()


def tensor_gather(values):
    halves, rows, width = values.shape
    chunks = row_chunks(halves, rows, 2)
    return pl.pallas_call(
        functools.partial(gather_kernel, chunks),
        out_shape=jax.ShapeDtypeStruct((halves, 4, rows, width), values.dtype),
        in_specs=[IN_VMEM],
        out_specs=IN_VMEM,
        scratch_shapes=[
            pltpu.SemaphoreType.DMA,
            pltpu.SemaphoreType.DMA((3 * len(chunks),)),
            pltpu.SemaphoreType.DMA((3 * len(chunks),)),
        ],
        compiler_params=pltpu.CompilerParams(collective_id=0, has_side_effects=True),
        cost_estimate=pl.CostEstimate(flops=0, bytes_accessed=40_000_000, transcendentals=0),
        name="tensor_gather",
    )(values)


def scatter_kernel(chunks, p_ref, out_ref, pair, mine, far, joined, send, receive):
    me, partner, across, diagonal = tensor_peers()
    meet([{"tp": partner}, {"tp": across}])
    count = len(chunks)
    first, second, third = [], [], []
    for i, (h, rows) in enumerate(chunks):
        first.append(
            remote(
                p_ref.at[h, diagonal, rows],
                pair.at[h, rows],
                send.at[i],
                receive.at[i],
                tp=partner,
            )
        )
        first[-1].start()
    for i, (h, rows) in enumerate(chunks):
        second.append(
            remote(
                p_ref.at[h, partner, rows],
                mine.at[h, rows],
                send.at[count + i],
                receive.at[count + i],
                tp=partner,
            )
        )
        second[-1].start()
    for i, (h, rows) in enumerate(chunks):
        first[i].wait_recv()
        joined[h, rows] = (
            p_ref[h, across, rows].astype(F32) + pair[h, rows].astype(F32)
        ).astype(BF)
        third.append(
            remote(
                joined.at[h, rows],
                far.at[h, rows],
                send.at[2 * count + i],
                receive.at[2 * count + i],
                tp=across,
            )
        )
        if i > 0:
            third[i - 1].start()
    for i, (h, rows) in enumerate(chunks):
        second[i].wait_recv()
        out_ref[h, rows] = p_ref[h, me, rows].astype(F32) + mine[h, rows].astype(F32)
        if i == 0:
            third[-1].start()
    for i, (h, rows) in enumerate(chunks):
        third[i].wait_recv()
        out_ref[h, rows] += far[h, rows].astype(F32)
    for i in range(count):
        first[i].wait_send()
        second[i].wait_send()
        third[i].wait_send()


def tensor_scatter(partial):
    halves, _, rows, width = partial.shape
    chunks = row_chunks(halves, rows, 2)
    block = pltpu.VMEM((halves, rows, width), BF)
    return pl.pallas_call(
        functools.partial(scatter_kernel, chunks),
        out_shape=jax.ShapeDtypeStruct((halves, rows, width), F32),
        in_specs=[IN_VMEM],
        out_specs=IN_VMEM,
        scratch_shapes=[block] * 4
        + [
            pltpu.SemaphoreType.DMA((3 * len(chunks),)),
            pltpu.SemaphoreType.DMA((3 * len(chunks),)),
        ],
        compiler_params=pltpu.CompilerParams(collective_id=1, has_side_effects=True),
        cost_estimate=pl.CostEstimate(flops=0, bytes_accessed=40_000_000, transcendentals=0),
        name="tensor_scatter",
    )(partial)


def opening_kernel(
    n, x_ref, q_ref, k_ref, v_ref, o_ref, out_ref, qkv_ref, full_o_ref, local, send, receive
):
    me, partner, across, _ = tensor_peers()
    ctx = lax.axis_index("ctx")
    other = 1 - ctx
    z = lax.axis_index("fsdp")
    weights = [(q_ref, 0), (k_ref, 1), (v_ref, 2)]
    rows_w = q_ref.shape[0]
    cols_w = q_ref.shape[1]
    half = rows_w // 2
    o_half = o_ref.shape[0] // 2
    o_cols = o_ref.shape[1]
    others = [lax.rem(z + d, n) for d in range(1, n)]
    meet(
        [{"tp": partner}, {"tp": across}, {"ctx": other}] + [{"fsdp": target} for target in others]
    )
    used = [0]

    def launch(source, target, **where):
        i = used[0]
        used[0] += 1
        copy = remote(source, target, send.at[i], receive.at[i], **where)
        copy.start()
        return copy

    def weight_rows(h):
        return pl.ds(pl.multiple_of(h * half, half), half)

    def output_rows(h):
        return pl.ds(pl.multiple_of(h * o_half, o_half), o_half)

    def output_cols(block):
        return pl.ds(pl.multiple_of(block * o_cols, o_cols), o_cols)

    swap = launch(x_ref.at[other], out_ref.at[ctx, me], ctx=other)
    over = [launch(x_ref.at[ctx], out_ref.at[ctx, me], tp=across)]
    side = [launch(x_ref.at[ctx], out_ref.at[ctx, me], tp=partner)]
    along = {}
    order = sorted(range(1, n), key=lambda d: min(d, n - d))
    for d in order:
        target = others[d - 1]
        group = []
        for ref, at in weights:
            group.append(
                launch(
                    ref.at[weight_rows(ctx)],
                    qkv_ref.at[z, weight_rows(ctx), pl.ds(at * cols_w, cols_w)],
                    fsdp=target,
                )
            )
        group.append(
            launch(
                o_ref.at[output_rows(ctx)],
                full_o_ref.at[output_rows(ctx), output_cols(z)],
                fsdp=target,
            )
        )
        along[d] = group
    own = [pltpu.make_async_copy(x_ref.at[ctx], out_ref.at[ctx, me], local.at[0])]
    for ref, at in weights:
        own.append(
            pltpu.make_async_copy(
                ref, qkv_ref.at[z, :, pl.ds(at * cols_w, cols_w)], local.at[1 + at]
            )
        )
    own.append(pltpu.make_async_copy(o_ref, full_o_ref.at[:, output_cols(z)], local.at[4]))
    for copy in own:
        copy.start()
    swap.wait_recv()
    over.append(launch(out_ref.at[other, me], out_ref.at[other, me], tp=across))
    side.append(launch(out_ref.at[other, me], out_ref.at[other, me], tp=partner))
    over[0].wait_recv()
    relay = [launch(out_ref.at[ctx, across], out_ref.at[ctx, across], tp=partner)]
    handed = []
    for d in order:
        for copy in along[d]:
            copy.wait_recv()
        block = lax.rem(z + n - d, n)
        handed.append(
            launch(
                qkv_ref.at[block, weight_rows(ctx)],
                qkv_ref.at[block, weight_rows(ctx)],
                ctx=other,
            )
        )
        handed.append(
            launch(
                full_o_ref.at[output_rows(ctx), output_cols(block)],
                full_o_ref.at[output_rows(ctx), output_cols(block)],
                ctx=other,
            )
        )
        if d == order[0]:
            over[1].wait_recv()
            relay.append(launch(out_ref.at[other, across], out_ref.at[other, across], tp=partner))
    for copy in side + relay + handed:
        copy.wait_recv()
    for copy in [swap] + over + side + relay + handed:
        copy.wait_send()
    for d in order:
        for copy in along[d]:
            copy.wait_send()
    for copy in own:
        copy.wait()


def opening(n, rows, query, key, value, output):
    _, count, width = rows.shape
    copies = 7 + 6 * (n - 1)
    gathered, qkv, full_output = pl.pallas_call(
        functools.partial(opening_kernel, n),
        out_shape=(
            jax.ShapeDtypeStruct((2, 4, count, width), BF),
            jax.ShapeDtypeStruct((n, query.shape[0], 3 * query.shape[1]), BF),
            jax.ShapeDtypeStruct((output.shape[0], n * output.shape[1]), BF),
        ),
        in_specs=[IN_VMEM] * 5,
        out_specs=(IN_VMEM,) * 3,
        scratch_shapes=[
            pltpu.SemaphoreType.DMA((5,)),
            pltpu.SemaphoreType.DMA((copies,)),
            pltpu.SemaphoreType.DMA((copies,)),
        ],
        compiler_params=pltpu.CompilerParams(collective_id=2, has_side_effects=True),
        cost_estimate=pl.CostEstimate(flops=0, bytes_accessed=60_000_000, transcendentals=0),
        name="opening",
    )(rows, query, key, value, output)
    return gathered, qkv.reshape(n * query.shape[0], 3 * query.shape[1]), full_output


def grads_kernel(
    n,
    g_ref,
    v_ref,
    early_ref,
    input_ref,
    out_ref,
    sums_ref,
    full_early_ref,
    traded_ref,
    arrived,
    reduced,
    far,
    total,
    pair,
    joined,
    group,
    send,
    receive,
    vector_send,
    vector_receive,
    share_send,
    share_receive,
    local,
):
    me, _, _, _ = tensor_peers()
    ctx = lax.axis_index("ctx")
    other = 1 - ctx
    z = lax.axis_index("fsdp")
    blocks = [lax.rem(z + d, n) for d in range(n)]
    around = [lax.rem(me + d, 4) for d in range(1, 4)]
    meet(
        [{"ctx": other}]
        + [{"fsdp": block} for block in blocks[1:]]
        + [{"tp": index} for index in around]
    )
    swap = remote(v_ref, pair, vector_send.at[0], vector_receive.at[0], ctx=other)
    swap.start()
    order = sorted(range(1, n), key=lambda d: -min(d, n - d)) + [0]
    near = {}
    for d in order:
        near[d] = remote(
            g_ref.at[blocks[d], other], arrived.at[d], send.at[d], receive.at[d], ctx=other
        )
        near[d].start()
    shares = [
        remote(input_ref.at[other], traded_ref.at[ctx], share_send.at[0], share_receive.at[0], ctx=other),
        remote(early_ref, full_early_ref.at[ctx], share_send.at[1], share_receive.at[1], ctx=other),
    ]
    own = [
        pltpu.make_async_copy(input_ref.at[ctx], traded_ref.at[ctx], local.at[0]),
        pltpu.make_async_copy(early_ref, full_early_ref.at[ctx], local.at[1]),
    ]
    for copy in shares + own:
        copy.start()
    swap.wait_recv()
    joined[...] = v_ref[...] + pair[...]
    group[z] = joined[...]
    line = [
        remote(joined, group.at[z], vector_send.at[d], vector_receive.at[d], fsdp=blocks[d])
        for d in range(1, n)
    ]
    along = {}
    for step, d in enumerate(order):
        near[d].wait_recv()
        value = g_ref[blocks[d], ctx].astype(F32) + arrived[d].astype(F32)
        if d:
            reduced[d] = value.astype(BF)
            along[d] = remote(
                reduced.at[d], far.at[d], send.at[n + d], receive.at[n + d], fsdp=blocks[d]
            )
        else:
            total[...] = value
        if step:
            along[order[step - 1]].start()
        if step == 0:
            for copy in line:
                copy.start()
    for copy in line:
        copy.wait_recv()
    summed = group[0]
    for i in range(1, n):
        summed = summed + group[i]
    sums_ref[me] = summed
    ring = [
        remote(
            sums_ref.at[me],
            sums_ref.at[me],
            vector_send.at[n + i],
            vector_receive.at[n + i],
            tp=index,
        )
        for i, index in enumerate(around)
    ]
    for step, d in enumerate(order[:-1]):
        along[d].wait_recv()
        total[...] += far[d].astype(F32)
        if step == 0:
            for copy in ring:
                copy.start()
    out_ref[ctx] = total[...].astype(BF)
    last = remote(out_ref.at[ctx], out_ref.at[ctx], send.at[n], receive.at[n], ctx=other)
    for d in order:
        near[d].wait_send()
    last.start()
    for d in order[:-1]:
        along[d].wait_send()
    for copy in ring + shares:
        copy.wait_recv()
    for copy in [swap] + line + ring + shares:
        copy.wait_send()
    for copy in own:
        copy.wait()
    last.wait_recv()
    last.wait_send()


def sum_grads(n, parts, vectors, early, traded):
    total_rows, width = parts.shape
    rows = total_rows // (2 * n)
    vector = pltpu.VMEM(vectors.shape, F32)
    out, sums, early, traded = pl.pallas_call(
        functools.partial(grads_kernel, n),
        out_shape=(
            jax.ShapeDtypeStruct((2, rows, width), BF),
            jax.ShapeDtypeStruct((4,) + vectors.shape, F32),
            jax.ShapeDtypeStruct((2,) + early.shape, BF),
            jax.ShapeDtypeStruct(traded.shape, BF),
        ),
        in_specs=[IN_VMEM] * 4,
        out_specs=(IN_VMEM,) * 4,
        scratch_shapes=[
            pltpu.VMEM((n, rows, width), BF),
            pltpu.VMEM((n, rows, width), BF),
            pltpu.VMEM((n, rows, width), BF),
            pltpu.VMEM((rows, width), F32),
            vector,
            vector,
            pltpu.VMEM((n,) + vectors.shape, F32),
            pltpu.SemaphoreType.DMA((2 * n,)),
            pltpu.SemaphoreType.DMA((2 * n,)),
            pltpu.SemaphoreType.DMA((n + 3,)),
            pltpu.SemaphoreType.DMA((n + 3,)),
            pltpu.SemaphoreType.DMA((2,)),
            pltpu.SemaphoreType.DMA((2,)),
            pltpu.SemaphoreType.DMA((2,)),
        ],
        compiler_params=pltpu.CompilerParams(collective_id=3, has_side_effects=True),
        cost_estimate=pl.CostEstimate(flops=0, bytes_accessed=120_000_000, transcendentals=0),
        name="sum_grads",
    )(parts.reshape(n, 2, rows, width), vectors, early, traded)
    return (
        out.reshape(2 * rows, width),
        sums,
        early.reshape(-1, early.shape[2]),
        traded,
    )


def unit_rows(values):
    return values * lax.rsqrt(jnp.mean(values * values, axis=-1, keepdims=True) + norm_eps)


def rotate_pairs(values, angles):
    middle = values.shape[-1] // 2
    leading = values[..., :middle]
    trailing = values[..., middle:]
    cosine = jnp.cos(angles)[..., None, :]
    sine_part = jnp.sin(angles)[..., None, :]
    return jnp.concatenate(
        [leading * cosine - trailing * sine_part, trailing * cosine + leading * sine_part], axis=-1
    )


def angles_for(positions, head_size):
    middle = head_size // 2
    frequency = rope_base ** (-2.0 * jnp.arange(middle).astype(F32) / head_size)
    return positions.astype(F32)[..., None] * frequency


def prepare_heads(projected, angles, gains, head_size):
    heads_here = projected.shape[-1] // head_size
    shaped = projected.reshape(projected.shape[:-1] + (heads_here, head_size))
    normed = unit_rows(rotate_pairs(shaped, angles)) * gains.reshape(heads_here, head_size)
    return normed.reshape(projected.shape)


def product(left, right):
    return jnp.dot(left, right, preferred_element_type=F32)


def transposed_left(left, right):
    return lax.dot_general(left, right, (((0,), (0,)), ((), ())), preferred_element_type=F32)


def transposed_right(left, right):
    return lax.dot_general(left, right, (((1,), (1,)), ((), ())), preferred_element_type=F32)


def branch_mix(branch, base, rate):
    return unit_rows(base + rate * (unit_rows(branch) - base))


def activate(upper, gated_raw, amplitude, steepness):
    scaled = gated_raw * steepness
    return upper * amplitude * (scaled * jax.nn.sigmoid(scaled))


def trade(values, sizes):
    n = sizes["ctx"]
    me = lax.axis_index("ctx")
    if n == 2:
        own = lax.dynamic_index_in_dim(values, me, 0, keepdims=False)
        other = lax.dynamic_index_in_dim(values, 1 - me, 0, keepdims=False)
        got = lax.ppermute(other, "ctx", [(0, 1), (1, 0)])
        first = jnp.where(me == 0, own, got)
        second = jnp.where(me == 0, got, own)
        return jnp.stack([first, second])
    return lax.all_to_all(values, "ctx", split_axis=0, concat_axis=0, tiled=True)


def tiles_of(length):
    return [pl.ds(i * BLK, BLK) for i in range(length // BLK)]


def scores_of(keys, query, col_ref, row_ref, tiles, a, j):
    scores = jnp.dot(keys[tiles[j], :], query, preferred_element_type=F32)
    if j >= a:
        scores = jnp.where(col_ref[tiles[j], :] <= row_ref[:, tiles[a]], scores, -1e30)
    return scores


def attend_kernel(q_ref, k_ref, v_ref, col_ref, row_ref, o_ref, lse_ref, keys):
    tiles = tiles_of(q_ref.shape[2])

    def one_head(h, carry):
        keys[...] = k_ref[h].T
        for a in range(len(tiles)):
            query = q_ref[h, :, tiles[a]]
            total = jnp.zeros((1, BLK), F32)
            out = jnp.zeros((HD, BLK), F32)
            for j in range(min(a + 2, len(tiles))):
                soft = jnp.exp(scores_of(keys, query, col_ref, row_ref, tiles, a, j))
                total += jnp.sum(soft, axis=0, keepdims=True)
                out += jnp.dot(v_ref[h, :, tiles[j]], soft.astype(BF), preferred_element_type=F32)
            o_ref[h, :, tiles[a]] = (out / total).astype(BF)
            lse_ref[h, :, tiles[a]] = jnp.log(total)
        return carry

    lax.fori_loop(0, q_ref.shape[0], one_head, 0)


def attend_both(query, key, value, ids):
    heads, _, length = query.shape
    return pl.pallas_call(
        attend_kernel,
        out_shape=(
            jax.ShapeDtypeStruct(query.shape, BF),
            jax.ShapeDtypeStruct((heads, 1, length), F32),
        ),
        in_specs=[IN_VMEM] * 5,
        out_specs=(IN_VMEM,) * 2,
        scratch_shapes=[pltpu.VMEM((length, HD), BF)],
        cost_estimate=pl.CostEstimate(flops=10**9, bytes_accessed=3 * 10**7, transcendentals=0),
        name="attend",
    )(query, key, value, ids[:, None], ids[None, :])


def attend_back_kernel(
    q_ref, k_ref, v_ref, col_ref, row_ref, lse_ref, o_ref, g_ref, dq_ref, dk_ref, dv_ref, keys, values
):
    tiles = tiles_of(q_ref.shape[2])
    last = (((1,), (1,)), ((), ()))

    def one_head(h, carry):
        keys[...] = k_ref[h].T
        values[...] = v_ref[h].T
        dk_ref[h] = jnp.zeros_like(dk_ref[h])
        dv_ref[h] = jnp.zeros_like(dv_ref[h])
        for a in range(len(tiles)):
            query = q_ref[h, :, tiles[a]]
            grad = g_ref[h, :, tiles[a]]
            lse = lse_ref[h, :, tiles[a]]
            delta = jnp.sum(
                grad.astype(F32) * o_ref[h, :, tiles[a]].astype(F32), axis=0, keepdims=True
            )
            dq = jnp.zeros((HD, BLK), F32)
            for j in range(min(a + 2, len(tiles))):
                scores = scores_of(keys, query, col_ref, row_ref, tiles, a, j)
                soft = jnp.exp(scores - lse)
                dp = jnp.dot(values[tiles[j], :], grad, preferred_element_type=F32)
                low = (soft * (dp - delta)).astype(BF)
                dv_ref[h, :, tiles[j]] += lax.dot_general(
                    grad, soft.astype(BF), last, preferred_element_type=F32
                )
                dk_ref[h, :, tiles[j]] += lax.dot_general(
                    query, low, last, preferred_element_type=F32
                )
                dq += jnp.dot(k_ref[h, :, tiles[j]], low, preferred_element_type=F32)
            dq_ref[h, :, tiles[a]] = dq * (1 / math.sqrt(HD))
        return carry

    lax.fori_loop(0, q_ref.shape[0], one_head, 0)


def attend_back(query, key, value, ids, logsum, out, grad):
    heads, _, length = query.shape
    shape = jax.ShapeDtypeStruct(query.shape, F32)
    return pl.pallas_call(
        attend_back_kernel,
        out_shape=(shape,) * 3,
        in_specs=[IN_VMEM] * 8,
        out_specs=(IN_VMEM,) * 3,
        scratch_shapes=[pltpu.VMEM((length, HD), BF)] * 2,
        cost_estimate=pl.CostEstimate(flops=3 * 10**9, bytes_accessed=6 * 10**7, transcendentals=0),
        name="attend_back",
    )(query, key, value, ids[:, None], ids[None, :], logsum, out, grad)


def tokens_minor(values):
    return values.T.reshape(-1, HD, values.shape[0])


def tokens_major(values):
    return values.reshape(-1, values.shape[2]).T


def swap_halves(share, ctx):
    got = lax.ppermute(share, "ctx", [(0, 1), (1, 0)])
    first = jnp.where(ctx == 0, share, got)
    second = jnp.where(ctx == 0, got, share)
    return jnp.concatenate([first, second], axis=0)


def per_device(sizes):
    def run(
        residual,
        query_weight,
        key_weight,
        value_weight,
        output_weight,
        sharpness,
        attend_rate,
        up_weight,
        gate_weight,
        down_weight,
        amplitude,
        steepness,
        mixer_rate,
        block_ids,
        positions,
        cotangent,
    ):
        n = sizes["fsdp"]
        tp = sizes["tp"]
        rows, width = residual.shape[1:]
        hidden_here = up_weight.shape[1]
        heads_width = query_weight.shape[1]
        small = n <= 4
        shape4 = (2, tp, rows, width)

        ctx = lax.axis_index("ctx")

        def own_half(shard):
            half = shard.shape[0] // 2
            return lax.dynamic_slice_in_dim(shard, ctx * half, half, 0)

        ug_half = own_half(jnp.concatenate([up_weight, gate_weight], axis=1))
        down_half = with_layout_constraint(own_half(down_weight.T), Layout((0, 1)))
        if small:
            gathered, full_qkv, full_output = opening(
                n, residual, query_weight, key_weight, value_weight, output_weight
            )
            gathered, ug_half, down_half = lax.optimization_barrier((gathered, ug_half, down_half))
            tensor_index = lax.axis_index("tp")
            mine = lax.dynamic_index_in_dim(gathered, tensor_index, 1, keepdims=False)
        else:
            mine = trade(residual, sizes)
            qkv_shard = jnp.concatenate([query_weight, key_weight, value_weight], axis=1)
            full_qkv = lax.all_gather(qkv_shard, "fsdp", axis=0, tiled=True)
            full_output = lax.all_gather(output_weight, "fsdp", axis=1, tiled=True)
            gathered = tensor_gather(mine)
        full_ug = lax.all_gather(ug_half, ("fsdp", "ctx"), axis=0, tiled=True)
        full_down = lax.all_gather(down_half, ("fsdp", "ctx"), axis=0, tiled=True)

        ids = lax.dynamic_index_in_dim(block_ids, ctx, 0, keepdims=False)
        my_positions = trade(positions, sizes).reshape(-1)
        angles = angles_for(my_positions, HD)

        flat_in = gathered.reshape(-1, width)
        raw = product(flat_in, full_qkv)
        raw_query, raw_key, raw_value = jnp.split(raw, 3, axis=1)

        def prepare_local(projected, gains):
            return prepare_heads(projected, angles, gains, HD)

        query_ready, query_back = jax.vjp(prepare_local, raw_query, sharpness)
        key_ready, key_back = jax.vjp(prepare_local, raw_key, sharpness)
        query_low = tokens_minor(query_ready.astype(BF) * BF(1 / math.sqrt(HD)))
        key_low = tokens_minor(key_ready.astype(BF))
        value_low = tokens_minor(raw_value.astype(BF))
        attended, logsum = attend_both(query_low, key_low, value_low, ids)
        flat_attended = attended.reshape(heads_width, -1)

        def reduce_rows(partial):
            return tensor_scatter(partial.astype(BF).reshape(shape4))

        def gather_rows(values):
            return tensor_gather(values.astype(BF)).reshape(-1, width)

        attend_sum = reduce_rows(transposed_left(flat_attended, full_output))
        residual_float = mine.astype(F32)
        first, attend_back_mix = jax.vjp(branch_mix, attend_sum, residual_float, attend_rate)
        first_all = gather_rows(first)
        ug_raw = product(first_all, full_ug)
        up_raw, gate_raw = ug_raw[:, :hidden_here], ug_raw[:, hidden_here:]
        hidden, activate_back = jax.vjp(activate, up_raw, gate_raw, amplitude, steepness)
        hidden_low = hidden.astype(BF)
        down_sum = reduce_rows(transposed_right(hidden_low, full_down))
        outcome, mixer_back = jax.vjp(branch_mix, down_sum, first, mixer_rate)
        layer_out = trade(outcome.astype(BF), sizes)
        my_cot = trade(cotangent, sizes)
        grad_down_sum, grad_first, grad_mixer_part = mixer_back(my_cot.astype(F32))
        down_grad_all = gather_rows(grad_down_sum)
        grad_hidden = product(down_grad_all, full_down)
        grad_down_part = transposed_left(down_grad_all, hidden_low)
        grad_up_raw, grad_gate_raw, grad_amplitude_part, grad_steepness_part = activate_back(
            grad_hidden
        )
        ug_grad = jnp.concatenate([grad_up_raw.astype(BF), grad_gate_raw.astype(BF)], axis=1)
        grad_first = grad_first + reduce_rows(transposed_right(ug_grad, full_ug))
        grad_ug_part = transposed_left(first_all, ug_grad)
        grad_attend_sum, grad_residual, grad_attend_part = attend_back_mix(grad_first)
        attend_grad_all = gather_rows(grad_attend_sum)
        grad_output_part = product(flat_attended, attend_grad_all).T
        grad_attended = transposed_right(full_output, attend_grad_all).astype(BF)
        grad_query_ready, grad_key_ready, grad_value_ready = [
            tokens_major(part)
            for part in attend_back(
                query_low,
                key_low,
                value_low,
                ids,
                logsum,
                attended,
                grad_attended.reshape(attended.shape),
            )
        ]
        grad_raw_query, sharp_query = query_back(grad_query_ready)
        grad_raw_key, sharp_key = key_back(grad_key_ready)
        qkv_grad = jnp.concatenate(
            [grad_raw_query.astype(BF), grad_raw_key.astype(BF), grad_value_ready.astype(BF)], axis=1
        )
        grad_input = grad_residual + reduce_rows(transposed_right(qkv_grad, full_qkv))
        grad_input = grad_input.astype(BF)
        grad_qkv_part = transposed_left(flat_in, qkv_grad)

        def scatter_rows(part):
            return lax.psum_scatter(
                part.astype(BF), ("fsdp", "ctx"), scatter_dimension=0, tiled=True
            )

        vectors = [
            sharp_query + sharp_key,
            grad_amplitude_part,
            grad_steepness_part,
            grad_attend_part,
            grad_mixer_part,
        ]
        lengths = [vector.shape[0] for vector in vectors]
        packed = jnp.concatenate(vectors)
        packed = jnp.pad(packed, (0, -packed.shape[0] % 1024)).reshape(-1, 128)
        early = scatter_rows(
            jnp.concatenate([grad_down_part.astype(BF), grad_ug_part.astype(BF)], axis=1)
        )
        late = jnp.concatenate([grad_qkv_part.astype(BF), grad_output_part.astype(BF)], axis=1)
        if small:
            late, sums, early, grad_input = sum_grads(n, late, packed, early, grad_input)
        else:
            late = swap_halves(scatter_rows(late), ctx)
            sums = lax.all_gather(lax.psum(packed, ("fsdp", "ctx")), "tp", axis=0)
            early = swap_halves(early, ctx)
            grad_input = trade(grad_input, sizes)
        late = late.astype(F32)
        grad_down = early[:, :hidden_here].astype(F32).T
        grad_ug = early[:, hidden_here:].astype(F32)
        grad_input = grad_input.astype(F32)
        grad_up, grad_gate = grad_ug[:, :hidden_here], grad_ug[:, hidden_here:]
        grad_query, grad_key, grad_value = jnp.split(late[:, : 3 * heads_width], 3, axis=1)
        grad_output = late[:, 3 * heads_width :].T
        sums = sums.reshape(tp, -1)
        pieces = []
        start = 0
        for length in lengths:
            pieces.append(sums[:, start : start + length])
            start += length
        grad_sharpness, grad_amplitude, grad_steepness = [p.reshape(-1) for p in pieces[:3]]
        grad_attend, grad_mixer = [p.sum(axis=0) for p in pieces[3:]]
        return (
            layer_out,
            grad_input,
            grad_query,
            grad_key,
            grad_value,
            grad_output,
            grad_sharpness,
            grad_attend,
            grad_up,
            grad_gate,
            grad_down,
            grad_amplitude,
            grad_steepness,
            grad_mixer,
        )

    return run


def solution(mesh):
    return jax.shard_map(
        per_device(dict(mesh.shape)),
        mesh=mesh,
        in_specs=(
            P("fsdp", ("ctx", "tp"), None),
            P("fsdp", "tp"),
            P("fsdp", "tp"),
            P("fsdp", "tp"),
            P("tp", "fsdp"),
            P("tp"),
            P(),
            P("fsdp", "tp"),
            P("fsdp", "tp"),
            P("tp", "fsdp"),
            P("tp"),
            P("tp"),
            P(),
            P("fsdp", None),
            P("fsdp", "ctx"),
            P("fsdp", ("ctx", "tp"), None),
        ),
        out_specs=(
            P("fsdp", ("ctx", "tp"), None),
            P("fsdp", ("ctx", "tp"), None),
            P("fsdp", "tp"),
            P("fsdp", "tp"),
            P("fsdp", "tp"),
            P("tp", "fsdp"),
            P(),
            P(),
            P("fsdp", "tp"),
            P("fsdp", "tp"),
            P("tp", "fsdp"),
            P(),
            P(),
            P(),
        ),
        check_vma=False,
    )
```

```python
import functools
import math

import jax
import jax.numpy as jnp
from jax import lax
from jax.experimental import pallas as pl
from jax.experimental.layout import Layout, with_layout_constraint
from jax.experimental.pallas import tpu as pltpu
from jax.sharding import PartitionSpec as P

HD = 64
BLK = 256
norm_eps = 1e-06
rope_base = 10000.0
BF = jnp.bfloat16
F32 = jnp.float32
MESH = pl.DeviceIdType.MESH
IN_VMEM = pl.BlockSpec(memory_space=pltpu.VMEM)


def remote(source, target, send, receive, **where):
    return pltpu.make_async_remote_copy(
        src_ref=source,
        dst_ref=target,
        send_sem=send,
        recv_sem=receive,
        device_id=where,
        device_id_type=MESH,
    )


def meet(peers):
    barrier = pltpu.get_barrier_semaphore()
    for where in peers:
        pl.semaphore_signal(barrier, inc=1, device_id=where, device_id_type=MESH)
    pl.semaphore_wait(barrier, len(peers))


def tensor_peers():
    me = lax.axis_index("tp")
    core = lax.rem(me, 2)
    chip = lax.div(me, 2)
    return (
        me,
        chip * 2 + (1 - core),
        (1 - chip) * 2 + core,
        (1 - chip) * 2 + (1 - core),
    )


def row_chunks(halves, rows, parts):
    step = rows // parts
    return [(h, pl.ds(i * step, step)) for h in range(halves) for i in range(parts)]


class Rider:
    arrays = ()
    shapes = ()
    scratch = ()
    remote_copies = 0
    local_copies = 0

    def place(self):
        ctx = lax.axis_index("ctx")
        z = lax.axis_index("fsdp")
        return ctx, 1 - ctx, z


class Near(Rider):
    def __init__(self, n, partial):
        self.n = n
        block = (n,) + partial.shape[2:]
        self.arrays = (partial,)
        self.shapes = (jax.ShapeDtypeStruct(block, BF),)
        self.scratch = (pltpu.VMEM(block, BF),)
        self.remote_copies = n

    def peers(self):
        return [{"ctx": self.place()[1]}]

    def start(self, inputs, outputs, scratch, send, receive, local):
        ctx, other, _ = self.place()
        partial, out, arrived = inputs[0], outputs[0], scratch[0]
        copies = [
            remote(partial.at[i, other], arrived.at[i], send.at[i], receive.at[i], ctx=other)
            for i in range(self.n)
        ]
        for copy in copies:
            copy.start()

        def finish():
            for i, copy in enumerate(copies):
                copy.wait_recv()
                out[i] = (partial[i, ctx].astype(F32) + arrived[i].astype(F32)).astype(BF)
            for copy in copies:
                copy.wait_send()

        return finish


def with_rider(body, rider, own_scratch, *refs):
    if rider is None:
        body([], lambda: (lambda: None), *refs)
        return
    sizes = [1, len(rider.arrays), 1, len(rider.shapes), own_scratch, len(rider.scratch), 3]
    groups = []
    start = 0
    for size in sizes:
        groups.append(refs[start : start + size])
        start += size
    x, inputs, out, outputs, scratch, extra, semaphores = groups

    def launch():
        return rider.start(inputs, outputs, extra, *semaphores)

    body(rider.peers(), launch, *x, *out, *scratch)


def call_tensor(body, array, shape, scratch, rider, number, name):
    own_scratch = len(scratch)
    arrays, shapes = [array], [shape]
    if rider is not None:
        arrays += rider.arrays
        shapes += rider.shapes
        scratch = (
            list(scratch)
            + list(rider.scratch)
            + [
                pltpu.SemaphoreType.DMA((rider.remote_copies,)),
                pltpu.SemaphoreType.DMA((rider.remote_copies,)),
                pltpu.SemaphoreType.DMA((max(rider.local_copies, 1),)),
            ]
        )
    result = pl.pallas_call(
        functools.partial(with_rider, body, rider, own_scratch),
        out_shape=tuple(shapes),
        in_specs=[IN_VMEM] * len(arrays),
        out_specs=(IN_VMEM,) * len(shapes),
        scratch_shapes=scratch,
        compiler_params=pltpu.CompilerParams(collective_id=number, has_side_effects=True),
        cost_estimate=pl.CostEstimate(flops=0, bytes_accessed=40_000_000, transcendentals=0),
        name=name,
    )(*arrays)
    return result[0] if rider is None else result


def gather_kernel(chunks, peers, launch, x_ref, out_ref, local_sem, send, receive):
    me, partner, across, _ = tensor_peers()
    meet([{"tp": partner}, {"tp": across}] + peers)
    own = pltpu.make_async_copy(x_ref, out_ref.at[:, me], local_sem)
    own.start()
    count = len(chunks)
    over, side, relay = [], [], []
    for i, (h, rows) in enumerate(chunks):
        over.append(
            remote(
                x_ref.at[h, rows],
                out_ref.at[h, me, rows],
                send.at[i],
                receive.at[i],
                tp=across,
            )
        )
        over[-1].start()
    for i, (h, rows) in enumerate(chunks):
        side.append(
            remote(
                x_ref.at[h, rows],
                out_ref.at[h, me, rows],
                send.at[count + i],
                receive.at[count + i],
                tp=partner,
            )
        )
        side[-1].start()
    finish = launch()
    for i, (h, rows) in enumerate(chunks):
        over[i].wait_recv()
        relay.append(
            remote(
                out_ref.at[h, across, rows],
                out_ref.at[h, across, rows],
                send.at[2 * count + i],
                receive.at[2 * count + i],
                tp=partner,
            )
        )
        relay[-1].start()
    for i in range(count):
        side[i].wait_recv()
        relay[i].wait_recv()
    for i in range(count):
        over[i].wait_send()
        side[i].wait_send()
        relay[i].wait_send()
    own.wait()
    finish()


def tensor_gather(values, rider=None, number=0):
    halves, rows, width = values.shape
    chunks = row_chunks(halves, rows, 2)
    return call_tensor(
        functools.partial(gather_kernel, chunks),
        values,
        jax.ShapeDtypeStruct((halves, 4, rows, width), values.dtype),
        [
            pltpu.SemaphoreType.DMA,
            pltpu.SemaphoreType.DMA((3 * len(chunks),)),
            pltpu.SemaphoreType.DMA((3 * len(chunks),)),
        ],
        rider,
        number,
        "tensor_gather",
    )


def scatter_kernel(
    chunks, peers, launch, p_ref, out_ref, pair, mine, far, joined, send, receive
):
    me, partner, across, diagonal = tensor_peers()
    meet([{"tp": partner}, {"tp": across}] + peers)
    count = len(chunks)
    first, second, third = [], [], []
    for i, (h, rows) in enumerate(chunks):
        first.append(
            remote(
                p_ref.at[h, diagonal, rows],
                pair.at[h, rows],
                send.at[i],
                receive.at[i],
                tp=partner,
            )
        )
        first[-1].start()
    for i, (h, rows) in enumerate(chunks):
        second.append(
            remote(
                p_ref.at[h, partner, rows],
                mine.at[h, rows],
                send.at[count + i],
                receive.at[count + i],
                tp=partner,
            )
        )
        second[-1].start()
    finish = launch()
    for i, (h, rows) in enumerate(chunks):
        first[i].wait_recv()
        joined[h, rows] = (
            p_ref[h, across, rows].astype(F32) + pair[h, rows].astype(F32)
        ).astype(BF)
        third.append(
            remote(
                joined.at[h, rows],
                far.at[h, rows],
                send.at[2 * count + i],
                receive.at[2 * count + i],
                tp=across,
            )
        )
        if i > 0:
            third[i - 1].start()
    for i, (h, rows) in enumerate(chunks):
        second[i].wait_recv()
        out_ref[h, rows] = p_ref[h, me, rows].astype(F32) + mine[h, rows].astype(F32)
        if i == 0:
            third[-1].start()
    for i, (h, rows) in enumerate(chunks):
        third[i].wait_recv()
        out_ref[h, rows] += far[h, rows].astype(F32)
    for i in range(count):
        first[i].wait_send()
        second[i].wait_send()
        third[i].wait_send()
    finish()


def tensor_scatter(partial, rider=None, number=1):
    halves, _, rows, width = partial.shape
    chunks = row_chunks(halves, rows, 2)
    block = pltpu.VMEM((halves, rows, width), BF)
    return call_tensor(
        functools.partial(scatter_kernel, chunks),
        partial,
        jax.ShapeDtypeStruct((halves, rows, width), F32),
        [block] * 4
        + [
            pltpu.SemaphoreType.DMA((3 * len(chunks),)),
            pltpu.SemaphoreType.DMA((3 * len(chunks),)),
        ],
        rider,
        number,
        "tensor_scatter",
    )


def opening_kernel(
    n, x_ref, q_ref, k_ref, v_ref, o_ref, out_ref, qkv_ref, full_o_ref, local, send, receive
):
    me, partner, across, _ = tensor_peers()
    ctx = lax.axis_index("ctx")
    other = 1 - ctx
    z = lax.axis_index("fsdp")
    weights = [(q_ref, 0), (k_ref, 1), (v_ref, 2)]
    rows_w = q_ref.shape[0]
    cols_w = q_ref.shape[1]
    half = rows_w // 2
    o_half = o_ref.shape[0] // 2
    o_cols = o_ref.shape[1]
    others = [lax.rem(z + d, n) for d in range(1, n)]
    meet(
        [{"tp": partner}, {"tp": across}, {"ctx": other}] + [{"fsdp": target} for target in others]
    )
    used = [0]

    def launch(source, target, **where):
        i = used[0]
        used[0] += 1
        copy = remote(source, target, send.at[i], receive.at[i], **where)
        copy.start()
        return copy

    def weight_rows(h):
        return pl.ds(pl.multiple_of(h * half, half), half)

    def output_rows(h):
        return pl.ds(pl.multiple_of(h * o_half, o_half), o_half)

    def output_cols(block):
        return pl.ds(pl.multiple_of(block * o_cols, o_cols), o_cols)

    swap = launch(x_ref.at[other], out_ref.at[ctx, me], ctx=other)
    over = [launch(x_ref.at[ctx], out_ref.at[ctx, me], tp=across)]
    side = [launch(x_ref.at[ctx], out_ref.at[ctx, me], tp=partner)]
    along = {}
    order = sorted(range(1, n), key=lambda d: min(d, n - d))
    for d in order:
        target = others[d - 1]
        group = []
        for ref, at in weights:
            group.append(
                launch(
                    ref.at[weight_rows(ctx)],
                    qkv_ref.at[z, weight_rows(ctx), pl.ds(at * cols_w, cols_w)],
                    fsdp=target,
                )
            )
        group.append(
            launch(
                o_ref.at[output_rows(ctx)],
                full_o_ref.at[output_rows(ctx), output_cols(z)],
                fsdp=target,
            )
        )
        along[d] = group
    own = [pltpu.make_async_copy(x_ref.at[ctx], out_ref.at[ctx, me], local.at[0])]
    for ref, at in weights:
        own.append(
            pltpu.make_async_copy(
                ref, qkv_ref.at[z, :, pl.ds(at * cols_w, cols_w)], local.at[1 + at]
            )
        )
    own.append(pltpu.make_async_copy(o_ref, full_o_ref.at[:, output_cols(z)], local.at[4]))
    for copy in own:
        copy.start()
    swap.wait_recv()
    over.append(launch(out_ref.at[other, me], out_ref.at[other, me], tp=across))
    side.append(launch(out_ref.at[other, me], out_ref.at[other, me], tp=partner))
    over[0].wait_recv()
    relay = [launch(out_ref.at[ctx, across], out_ref.at[ctx, across], tp=partner)]
    handed = []
    for d in order:
        for copy in along[d]:
            copy.wait_recv()
        block = lax.rem(z + n - d, n)
        handed.append(
            launch(
                qkv_ref.at[block, weight_rows(ctx)],
                qkv_ref.at[block, weight_rows(ctx)],
                ctx=other,
            )
        )
        handed.append(
            launch(
                full_o_ref.at[output_rows(ctx), output_cols(block)],
                full_o_ref.at[output_rows(ctx), output_cols(block)],
                ctx=other,
            )
        )
        if d == order[0]:
            over[1].wait_recv()
            relay.append(launch(out_ref.at[other, across], out_ref.at[other, across], tp=partner))
    for copy in side + relay + handed:
        copy.wait_recv()
    for copy in [swap] + over + side + relay + handed:
        copy.wait_send()
    for d in order:
        for copy in along[d]:
            copy.wait_send()
    for copy in own:
        copy.wait()


def opening(n, rows, query, key, value, output):
    _, count, width = rows.shape
    copies = 7 + 6 * (n - 1)
    gathered, qkv, full_output = pl.pallas_call(
        functools.partial(opening_kernel, n),
        out_shape=(
            jax.ShapeDtypeStruct((2, 4, count, width), BF),
            jax.ShapeDtypeStruct((n, query.shape[0], 3 * query.shape[1]), BF),
            jax.ShapeDtypeStruct((output.shape[0], n * output.shape[1]), BF),
        ),
        in_specs=[IN_VMEM] * 5,
        out_specs=(IN_VMEM,) * 3,
        scratch_shapes=[
            pltpu.SemaphoreType.DMA((5,)),
            pltpu.SemaphoreType.DMA((copies,)),
            pltpu.SemaphoreType.DMA((copies,)),
        ],
        compiler_params=pltpu.CompilerParams(collective_id=2, has_side_effects=True),
        cost_estimate=pl.CostEstimate(flops=0, bytes_accessed=60_000_000, transcendentals=0),
        name="opening",
    )(rows, query, key, value, output)
    return gathered, qkv.reshape(n * query.shape[0], 3 * query.shape[1]), full_output


def closing_kernel(
    n,
    g_ref,
    v_ref,
    early_ref,
    input_ref,
    out_ref,
    sums_ref,
    full_early_ref,
    traded_ref,
    far,
    pair,
    joined,
    group,
    send,
    receive,
    vector_send,
    vector_receive,
    share_send,
    share_receive,
    local,
):
    me, _, _, _ = tensor_peers()
    ctx = lax.axis_index("ctx")
    other = 1 - ctx
    z = lax.axis_index("fsdp")
    blocks = [lax.rem(z + d, n) for d in range(n)]
    around = [lax.rem(me + d, 4) for d in range(1, 4)]
    meet(
        [{"ctx": other}]
        + [{"fsdp": block} for block in blocks[1:]]
        + [{"tp": index} for index in around]
    )
    swap = remote(v_ref, pair, vector_send.at[0], vector_receive.at[0], ctx=other)
    swap.start()
    order = sorted(range(1, n), key=lambda d: -min(d, n - d))
    along = {}
    for d in order:
        along[d] = remote(
            g_ref.at[blocks[d]], far.at[d], send.at[d], receive.at[d], fsdp=blocks[d]
        )
        along[d].start()
    shares = [
        remote(early_ref, full_early_ref.at[ctx], share_send.at[0], share_receive.at[0], ctx=other),
        remote(
            input_ref.at[other], traded_ref.at[ctx], share_send.at[1], share_receive.at[1], ctx=other
        ),
    ]
    own = [
        pltpu.make_async_copy(early_ref, full_early_ref.at[ctx], local.at[0]),
        pltpu.make_async_copy(input_ref.at[ctx], traded_ref.at[ctx], local.at[1]),
    ]
    for copy in shares + own:
        copy.start()
    swap.wait_recv()
    joined[...] = v_ref[...] + pair[...]
    group[z] = joined[...]
    line = [
        remote(joined, group.at[z], vector_send.at[d], vector_receive.at[d], fsdp=blocks[d])
        for d in range(1, n)
    ]
    for copy in own:
        copy.wait()
    for copy in line:
        copy.start()
    total = g_ref[z].astype(F32)
    for d in order:
        along[d].wait_recv()
        total = total + far[d].astype(F32)
    out_ref[ctx] = total.astype(BF)
    for copy in line:
        copy.wait_recv()
    summed = group[0]
    for i in range(1, n):
        summed = summed + group[i]
    sums_ref[me] = summed
    ring = [
        remote(
            sums_ref.at[me],
            sums_ref.at[me],
            vector_send.at[n + i],
            vector_receive.at[n + i],
            tp=index,
        )
        for i, index in enumerate(around)
    ]
    last = remote(out_ref.at[ctx], out_ref.at[ctx], send.at[0], receive.at[0], ctx=other)
    last.start()
    for d in order:
        along[d].wait_send()
    for copy in ring:
        copy.start()
    for copy in ring + shares:
        copy.wait_recv()
    for copy in [swap] + line + ring + shares:
        copy.wait_send()
    last.wait_recv()
    last.wait_send()


def closing(n, terms, vectors, early, traded):
    _, rows, width = terms.shape
    vector = pltpu.VMEM(vectors.shape, F32)
    out, sums, early, traded = pl.pallas_call(
        functools.partial(closing_kernel, n),
        out_shape=(
            jax.ShapeDtypeStruct((2, rows, width), BF),
            jax.ShapeDtypeStruct((4,) + vectors.shape, F32),
            jax.ShapeDtypeStruct((2,) + early.shape, BF),
            jax.ShapeDtypeStruct(traded.shape, BF),
        ),
        in_specs=[IN_VMEM] * 4,
        out_specs=(IN_VMEM,) * 4,
        scratch_shapes=[
            pltpu.VMEM((n, rows, width), BF),
            vector,
            vector,
            pltpu.VMEM((n,) + vectors.shape, F32),
            pltpu.SemaphoreType.DMA((n,)),
            pltpu.SemaphoreType.DMA((n,)),
            pltpu.SemaphoreType.DMA((n + 3,)),
            pltpu.SemaphoreType.DMA((n + 3,)),
            pltpu.SemaphoreType.DMA((2,)),
            pltpu.SemaphoreType.DMA((2,)),
            pltpu.SemaphoreType.DMA((2,)),
        ],
        compiler_params=pltpu.CompilerParams(collective_id=3, has_side_effects=True),
        cost_estimate=pl.CostEstimate(flops=0, bytes_accessed=120_000_000, transcendentals=0),
        name="closing",
    )(terms, vectors, early, traded)
    return out.reshape(2 * rows, width), sums, early.reshape(-1, early.shape[2]), traded


def unit_rows(values):
    return values * lax.rsqrt(jnp.mean(values * values, axis=-1, keepdims=True) + norm_eps)


def rotate_pairs(values, angles):
    middle = values.shape[-1] // 2
    leading = values[..., :middle]
    trailing = values[..., middle:]
    cosine = jnp.cos(angles)[..., None, :]
    sine_part = jnp.sin(angles)[..., None, :]
    return jnp.concatenate(
        [leading * cosine - trailing * sine_part, trailing * cosine + leading * sine_part], axis=-1
    )


def angles_for(positions, head_size):
    middle = head_size // 2
    frequency = rope_base ** (-2.0 * jnp.arange(middle).astype(F32) / head_size)
    return positions.astype(F32)[..., None] * frequency


def prepare_heads(projected, angles, gains, head_size):
    heads_here = projected.shape[-1] // head_size
    shaped = projected.reshape(projected.shape[:-1] + (heads_here, head_size))
    normed = unit_rows(rotate_pairs(shaped, angles)) * gains.reshape(heads_here, head_size)
    return normed.reshape(projected.shape)


def product(left, right):
    return jnp.dot(left, right, preferred_element_type=F32)


def transposed_left(left, right):
    return lax.dot_general(left, right, (((0,), (0,)), ((), ())), preferred_element_type=F32)


def transposed_right(left, right):
    return lax.dot_general(left, right, (((1,), (1,)), ((), ())), preferred_element_type=F32)


def branch_mix(branch, base, rate):
    return unit_rows(base + rate * (unit_rows(branch) - base))


def activate(upper, gated_raw, amplitude, steepness):
    scaled = gated_raw * steepness
    return upper * amplitude * (scaled * jax.nn.sigmoid(scaled))


def trade(values, sizes):
    n = sizes["ctx"]
    me = lax.axis_index("ctx")
    if n == 2:
        own = lax.dynamic_index_in_dim(values, me, 0, keepdims=False)
        other = lax.dynamic_index_in_dim(values, 1 - me, 0, keepdims=False)
        got = lax.ppermute(other, "ctx", [(0, 1), (1, 0)])
        first = jnp.where(me == 0, own, got)
        second = jnp.where(me == 0, got, own)
        return jnp.stack([first, second])
    return lax.all_to_all(values, "ctx", split_axis=0, concat_axis=0, tiled=True)


def tiles_of(length):
    return [pl.ds(i * BLK, BLK) for i in range(length // BLK)]


def scores_of(keys, query, col_ref, row_ref, tiles, a, j):
    scores = jnp.dot(keys[tiles[j], :], query, preferred_element_type=F32)
    if j >= a:
        scores = jnp.where(col_ref[tiles[j], :] <= row_ref[:, tiles[a]], scores, -1e30)
    return scores


def attend_kernel(q_ref, k_ref, v_ref, col_ref, row_ref, o_ref, lse_ref, keys):
    tiles = tiles_of(q_ref.shape[2])

    def one_head(h, carry):
        keys[...] = k_ref[h].T
        for a in range(len(tiles)):
            query = q_ref[h, :, tiles[a]]
            total = jnp.zeros((1, BLK), F32)
            out = jnp.zeros((HD, BLK), F32)
            for j in range(min(a + 2, len(tiles))):
                soft = jnp.exp(scores_of(keys, query, col_ref, row_ref, tiles, a, j))
                total += jnp.sum(soft, axis=0, keepdims=True)
                out += jnp.dot(v_ref[h, :, tiles[j]], soft.astype(BF), preferred_element_type=F32)
            o_ref[h, :, tiles[a]] = (out / total).astype(BF)
            lse_ref[h, :, tiles[a]] = jnp.log(total)
        return carry

    lax.fori_loop(0, q_ref.shape[0], one_head, 0)


def attend_both(query, key, value, ids):
    heads, _, length = query.shape
    return pl.pallas_call(
        attend_kernel,
        out_shape=(
            jax.ShapeDtypeStruct(query.shape, BF),
            jax.ShapeDtypeStruct((heads, 1, length), F32),
        ),
        in_specs=[IN_VMEM] * 5,
        out_specs=(IN_VMEM,) * 2,
        scratch_shapes=[pltpu.VMEM((length, HD), BF)],
        cost_estimate=pl.CostEstimate(flops=10**9, bytes_accessed=3 * 10**7, transcendentals=0),
        name="attend",
    )(query, key, value, ids[:, None], ids[None, :])


def attend_back_kernel(
    q_ref, k_ref, v_ref, col_ref, row_ref, lse_ref, o_ref, g_ref, dq_ref, dk_ref, dv_ref, keys, values
):
    tiles = tiles_of(q_ref.shape[2])
    last = (((1,), (1,)), ((), ()))

    def one_head(h, carry):
        keys[...] = k_ref[h].T
        values[...] = v_ref[h].T
        dk_ref[h] = jnp.zeros_like(dk_ref[h])
        dv_ref[h] = jnp.zeros_like(dv_ref[h])
        for a in range(len(tiles)):
            query = q_ref[h, :, tiles[a]]
            grad = g_ref[h, :, tiles[a]]
            lse = lse_ref[h, :, tiles[a]]
            delta = jnp.sum(
                grad.astype(F32) * o_ref[h, :, tiles[a]].astype(F32), axis=0, keepdims=True
            )
            dq = jnp.zeros((HD, BLK), F32)
            for j in range(min(a + 2, len(tiles))):
                scores = scores_of(keys, query, col_ref, row_ref, tiles, a, j)
                soft = jnp.exp(scores - lse)
                dp = jnp.dot(values[tiles[j], :], grad, preferred_element_type=F32)
                low = (soft * (dp - delta)).astype(BF)
                dv_ref[h, :, tiles[j]] += lax.dot_general(
                    grad, soft.astype(BF), last, preferred_element_type=F32
                )
                dk_ref[h, :, tiles[j]] += lax.dot_general(
                    query, low, last, preferred_element_type=F32
                )
                dq += jnp.dot(k_ref[h, :, tiles[j]], low, preferred_element_type=F32)
            dq_ref[h, :, tiles[a]] = dq * (1 / math.sqrt(HD))
        return carry

    lax.fori_loop(0, q_ref.shape[0], one_head, 0)


def attend_back(query, key, value, ids, logsum, out, grad):
    heads, _, length = query.shape
    shape = jax.ShapeDtypeStruct(query.shape, F32)
    return pl.pallas_call(
        attend_back_kernel,
        out_shape=(shape,) * 3,
        in_specs=[IN_VMEM] * 8,
        out_specs=(IN_VMEM,) * 3,
        scratch_shapes=[pltpu.VMEM((length, HD), BF)] * 2,
        cost_estimate=pl.CostEstimate(flops=3 * 10**9, bytes_accessed=6 * 10**7, transcendentals=0),
        name="attend_back",
    )(query, key, value, ids[:, None], ids[None, :], logsum, out, grad)


def tokens_minor(values):
    return values.T.reshape(-1, HD, values.shape[0])


def tokens_major(values):
    return values.reshape(-1, values.shape[2]).T


def swap_halves(share, ctx):
    got = lax.ppermute(share, "ctx", [(0, 1), (1, 0)])
    first = jnp.where(ctx == 0, share, got)
    second = jnp.where(ctx == 0, got, share)
    return jnp.concatenate([first, second], axis=0)


def per_device(sizes):
    def run(
        residual,
        query_weight,
        key_weight,
        value_weight,
        output_weight,
        sharpness,
        attend_rate,
        up_weight,
        gate_weight,
        down_weight,
        amplitude,
        steepness,
        mixer_rate,
        block_ids,
        positions,
        cotangent,
    ):
        n = sizes["fsdp"]
        tp = sizes["tp"]
        rows, width = residual.shape[1:]
        hidden_here = up_weight.shape[1]
        heads_width = query_weight.shape[1]
        small = n <= 4
        shape4 = (2, tp, rows, width)

        ctx = lax.axis_index("ctx")

        def own_half(shard):
            half = shard.shape[0] // 2
            return lax.dynamic_slice_in_dim(shard, ctx * half, half, 0)

        late_half = own_half(jnp.concatenate([up_weight, gate_weight, down_weight.T], axis=1))
        if small:
            gathered, full_qkv, full_output = opening(
                n, residual, query_weight, key_weight, value_weight, output_weight
            )
            tensor_index = lax.axis_index("tp")
            mine = lax.dynamic_index_in_dim(gathered, tensor_index, 1, keepdims=False)
        else:
            mine = trade(residual, sizes)
            qkv_shard = jnp.concatenate([query_weight, key_weight, value_weight], axis=1)
            full_qkv = lax.all_gather(qkv_shard, "fsdp", axis=0, tiled=True)
            full_output = lax.all_gather(output_weight, "fsdp", axis=1, tiled=True)
            gathered = tensor_gather(mine)
        full_late = lax.all_gather(late_half, ("fsdp", "ctx"), axis=0, tiled=True)
        full_ug = full_late[:, : 2 * hidden_here]
        full_down = full_late[:, 2 * hidden_here :]

        ids = lax.dynamic_index_in_dim(block_ids, ctx, 0, keepdims=False)
        my_positions = trade(positions, sizes).reshape(-1)
        angles = angles_for(my_positions, HD)

        flat_in = gathered.reshape(-1, width)
        raw = product(flat_in, full_qkv)
        raw_query, raw_key, raw_value = jnp.split(raw, 3, axis=1)

        def prepare_local(projected, gains):
            return prepare_heads(projected, angles, gains, HD)

        query_ready, query_back = jax.vjp(prepare_local, raw_query, sharpness)
        key_ready, key_back = jax.vjp(prepare_local, raw_key, sharpness)
        query_low = tokens_minor(query_ready.astype(BF) * BF(1 / math.sqrt(HD)))
        key_low = tokens_minor(key_ready.astype(BF))
        value_low = tokens_minor(raw_value.astype(BF))
        attended, logsum = attend_both(query_low, key_low, value_low, ids)
        flat_attended = attended.reshape(heads_width, -1)

        def reduce_rows(partial, *rider):
            return tensor_scatter(partial.astype(BF).reshape(shape4), *rider)

        def gather_rows(values):
            return tensor_gather(values.astype(BF)).reshape(-1, width)

        attend_sum = reduce_rows(transposed_left(flat_attended, full_output))
        residual_float = mine.astype(F32)
        first, attend_back_mix = jax.vjp(branch_mix, attend_sum, residual_float, attend_rate)
        first_all = gather_rows(first)
        ug_raw = product(first_all, full_ug)
        up_raw, gate_raw = ug_raw[:, :hidden_here], ug_raw[:, hidden_here:]
        hidden, activate_back = jax.vjp(activate, up_raw, gate_raw, amplitude, steepness)
        hidden_low = hidden.astype(BF)
        down_sum = reduce_rows(transposed_right(hidden_low, full_down))
        outcome, mixer_back = jax.vjp(branch_mix, down_sum, first, mixer_rate)
        layer_out = trade(outcome.astype(BF), sizes)
        my_cot = trade(cotangent, sizes)
        grad_down_sum, grad_first, grad_mixer_part = mixer_back(my_cot.astype(F32))
        down_grad_all = gather_rows(grad_down_sum)
        grad_hidden = product(down_grad_all, full_down)
        grad_down_part = transposed_left(down_grad_all, hidden_low)
        grad_up_raw, grad_gate_raw, grad_amplitude_part, grad_steepness_part = activate_back(
            grad_hidden
        )
        ug_grad = jnp.concatenate([grad_up_raw.astype(BF), grad_gate_raw.astype(BF)], axis=1)
        grad_first = grad_first + reduce_rows(transposed_right(ug_grad, full_ug))
        grad_ug_part = transposed_left(first_all, ug_grad)
        grad_attend_sum, grad_residual, grad_attend_part = attend_back_mix(grad_first)
        attend_grad_all = gather_rows(grad_attend_sum)
        grad_output_part = product(flat_attended, attend_grad_all).T
        grad_attended = transposed_right(full_output, attend_grad_all).astype(BF)
        grad_query_ready, grad_key_ready, grad_value_ready = [
            tokens_major(part)
            for part in attend_back(
                query_low,
                key_low,
                value_low,
                ids,
                logsum,
                attended,
                grad_attended.reshape(attended.shape),
            )
        ]
        grad_raw_query, sharp_query = query_back(grad_query_ready)
        grad_raw_key, sharp_key = key_back(grad_key_ready)
        qkv_grad = jnp.concatenate(
            [grad_raw_query.astype(BF), grad_raw_key.astype(BF), grad_value_ready.astype(BF)], axis=1
        )
        grad_qkv_part = transposed_left(flat_in, qkv_grad)
        late = jnp.concatenate([grad_qkv_part.astype(BF), grad_output_part.astype(BF)], axis=1)
        partial = transposed_right(qkv_grad, full_qkv)
        if small:
            late = late.reshape(n, 2, -1, late.shape[1])
            summed, late_terms = reduce_rows(partial, Near(n, late), 5)
        else:
            summed = reduce_rows(partial)
        grad_input = (grad_residual + summed).astype(BF)

        def scatter_rows(part):
            return lax.psum_scatter(
                part.astype(BF), ("fsdp", "ctx"), scatter_dimension=0, tiled=True
            )

        vectors = [
            sharp_query + sharp_key,
            grad_amplitude_part,
            grad_steepness_part,
            grad_attend_part,
            grad_mixer_part,
        ]
        lengths = [vector.shape[0] for vector in vectors]
        packed = jnp.concatenate(vectors)
        packed = jnp.pad(packed, (0, -packed.shape[0] % 1024)).reshape(-1, 128)
        early = scatter_rows(
            jnp.concatenate([grad_down_part.astype(BF), grad_ug_part.astype(BF)], axis=1)
        )
        if small:
            late, sums, early, grad_input = closing(n, late_terms, packed, early, grad_input)
        else:
            late = swap_halves(scatter_rows(late), ctx)
            sums = lax.all_gather(lax.psum(packed, ("fsdp", "ctx")), "tp", axis=0)
            early = swap_halves(early, ctx)
            grad_input = trade(grad_input, sizes)
        late = late.astype(F32)
        grad_down = early[:, :hidden_here].astype(F32).T
        grad_ug = early[:, hidden_here:].astype(F32)
        grad_input = grad_input.astype(F32)
        grad_up, grad_gate = grad_ug[:, :hidden_here], grad_ug[:, hidden_here:]
        grad_query, grad_key, grad_value = jnp.split(late[:, : 3 * heads_width], 3, axis=1)
        grad_output = late[:, 3 * heads_width :].T
        sums = sums.reshape(tp, -1)
        pieces = []
        start = 0
        for length in lengths:
            pieces.append(sums[:, start : start + length])
            start += length
        grad_sharpness, grad_amplitude, grad_steepness = [p.reshape(-1) for p in pieces[:3]]
        grad_attend, grad_mixer = [p.sum(axis=0) for p in pieces[3:]]
        return (
            layer_out,
            grad_input,
            grad_query,
            grad_key,
            grad_value,
            grad_output,
            grad_sharpness,
            grad_attend,
            grad_up,
            grad_gate,
            grad_down,
            grad_amplitude,
            grad_steepness,
            grad_mixer,
        )

    return run


def solution(mesh):
    return jax.shard_map(
        per_device(dict(mesh.shape)),
        mesh=mesh,
        in_specs=(
            P("fsdp", ("ctx", "tp"), None),
            P("fsdp", "tp"),
            P("fsdp", "tp"),
            P("fsdp", "tp"),
            P("tp", "fsdp"),
            P("tp"),
            P(),
            P("fsdp", "tp"),
            P("fsdp", "tp"),
            P("tp", "fsdp"),
            P("tp"),
            P("tp"),
            P(),
            P("fsdp", None),
            P("fsdp", "ctx"),
            P("fsdp", ("ctx", "tp"), None),
        ),
        out_specs=(
            P("fsdp", ("ctx", "tp"), None),
            P("fsdp", ("ctx", "tp"), None),
            P("fsdp", "tp"),
            P("fsdp", "tp"),
            P("fsdp", "tp"),
            P("tp", "fsdp"),
            P(),
            P(),
            P("fsdp", "tp"),
            P("fsdp", "tp"),
            P("tp", "fsdp"),
            P(),
            P(),
            P(),
        ),
        check_vma=False,
    )
```

```python
import functools
import math

import jax
import jax.numpy as jnp
from jax import lax
from jax.experimental import pallas as pl
from jax.experimental.layout import Layout, with_layout_constraint
from jax.experimental.pallas import tpu as pltpu
from jax.sharding import PartitionSpec as P

HD = 64
BLK = 256
norm_eps = 1e-06
rope_base = 10000.0
BF = jnp.bfloat16
F32 = jnp.float32
MESH = pl.DeviceIdType.MESH
IN_VMEM = pl.BlockSpec(memory_space=pltpu.VMEM)


def remote(source, target, send, receive, **where):
    return pltpu.make_async_remote_copy(
        src_ref=source,
        dst_ref=target,
        send_sem=send,
        recv_sem=receive,
        device_id=where,
        device_id_type=MESH,
    )


def meet(peers):
    barrier = pltpu.get_barrier_semaphore()
    for where in peers:
        pl.semaphore_signal(barrier, inc=1, device_id=where, device_id_type=MESH)
    pl.semaphore_wait(barrier, len(peers))


def tensor_peers():
    me = lax.axis_index("tp")
    core = lax.rem(me, 2)
    chip = lax.div(me, 2)
    return (
        me,
        chip * 2 + (1 - core),
        (1 - chip) * 2 + core,
        (1 - chip) * 2 + (1 - core),
    )


def row_chunks(halves, rows, parts):
    step = rows // parts
    return [(h, pl.ds(i * step, step)) for h in range(halves) for i in range(parts)]


class Rider:
    arrays = ()
    shapes = ()
    scratch = ()
    remote_copies = 0
    local_copies = 0

    def place(self):
        ctx = lax.axis_index("ctx")
        z = lax.axis_index("fsdp")
        return ctx, 1 - ctx, z


class Near(Rider):
    def __init__(self, n, partial):
        self.n = n
        block = (n,) + partial.shape[2:]
        self.arrays = (partial,)
        self.shapes = (jax.ShapeDtypeStruct(block, BF),)
        self.scratch = (pltpu.VMEM(block, BF),)
        self.remote_copies = n

    def peers(self):
        return [{"ctx": self.place()[1]}]

    def start(self, inputs, outputs, scratch, send, receive, local):
        ctx, other, _ = self.place()
        partial, out, arrived = inputs[0], outputs[0], scratch[0]
        copies = [
            remote(partial.at[i, other], arrived.at[i], send.at[i], receive.at[i], ctx=other)
            for i in range(self.n)
        ]
        for copy in copies:
            copy.start()

        def finish():
            for i, copy in enumerate(copies):
                copy.wait_recv()
                out[i] = (partial[i, ctx].astype(F32) + arrived[i].astype(F32)).astype(BF)
            for copy in copies:
                copy.wait_send()

        return finish


def with_rider(body, rider, own_scratch, *refs):
    if rider is None:
        body([], lambda: (lambda: None), *refs)
        return
    sizes = [1, len(rider.arrays), 1, len(rider.shapes), own_scratch, len(rider.scratch), 3]
    groups = []
    start = 0
    for size in sizes:
        groups.append(refs[start : start + size])
        start += size
    x, inputs, out, outputs, scratch, extra, semaphores = groups

    def launch():
        return rider.start(inputs, outputs, extra, *semaphores)

    body(rider.peers(), launch, *x, *out, *scratch)


def call_tensor(body, array, shape, scratch, rider, number, name, out_spec=IN_VMEM, in_spec=IN_VMEM):
    own_scratch = len(scratch)
    arrays, shapes = [array], [shape]
    if rider is not None:
        arrays += rider.arrays
        shapes += rider.shapes
        scratch = (
            list(scratch)
            + list(rider.scratch)
            + [
                pltpu.SemaphoreType.DMA((rider.remote_copies,)),
                pltpu.SemaphoreType.DMA((rider.remote_copies,)),
                pltpu.SemaphoreType.DMA((max(rider.local_copies, 1),)),
            ]
        )
    result = pl.pallas_call(
        functools.partial(with_rider, body, rider, own_scratch),
        out_shape=tuple(shapes),
        in_specs=[in_spec] + [IN_VMEM] * (len(arrays) - 1),
        out_specs=(out_spec,) + (IN_VMEM,) * (len(shapes) - 1),
        scratch_shapes=scratch,
        compiler_params=pltpu.CompilerParams(collective_id=number, has_side_effects=True),
        cost_estimate=pl.CostEstimate(flops=0, bytes_accessed=40_000_000, transcendentals=0),
        name=name,
    )(*arrays)
    return result[0] if rider is None else result


def gather_kernel(chunks, peers, launch, x_ref, out_ref, local_sem, send, receive):
    me, partner, across, _ = tensor_peers()
    meet([{"tp": partner}, {"tp": across}] + peers)
    own = pltpu.make_async_copy(x_ref, out_ref.at[:, me], local_sem)
    own.start()
    count = len(chunks)
    over, side, relay = [], [], []
    for i, (h, rows) in enumerate(chunks):
        over.append(
            remote(
                x_ref.at[h, rows],
                out_ref.at[h, me, rows],
                send.at[i],
                receive.at[i],
                tp=across,
            )
        )
        over[-1].start()
    for i, (h, rows) in enumerate(chunks):
        side.append(
            remote(
                x_ref.at[h, rows],
                out_ref.at[h, me, rows],
                send.at[count + i],
                receive.at[count + i],
                tp=partner,
            )
        )
        side[-1].start()
    finish = launch()
    for i, (h, rows) in enumerate(chunks):
        over[i].wait_recv()
        relay.append(
            remote(
                out_ref.at[h, across, rows],
                out_ref.at[h, across, rows],
                send.at[2 * count + i],
                receive.at[2 * count + i],
                tp=partner,
            )
        )
        relay[-1].start()
    for i in range(count):
        side[i].wait_recv()
        relay[i].wait_recv()
    for i in range(count):
        over[i].wait_send()
        side[i].wait_send()
        relay[i].wait_send()
    own.wait()
    finish()


def tensor_gather(values, rider=None, number=0):
    halves, rows, width = values.shape
    chunks = row_chunks(halves, rows, 2)
    return call_tensor(
        functools.partial(gather_kernel, chunks),
        values,
        jax.ShapeDtypeStruct((halves, 4, rows, width), values.dtype),
        [
            pltpu.SemaphoreType.DMA,
            pltpu.SemaphoreType.DMA((3 * len(chunks),)),
            pltpu.SemaphoreType.DMA((3 * len(chunks),)),
        ],
        rider,
        number,
        "tensor_gather",
        pl.BlockSpec(memory_space=pl.ANY),
    )


def scatter_kernel(
    chunks,
    peers,
    launch,
    p_ref,
    out_ref,
    pair,
    mine,
    far,
    joined,
    passing,
    kept,
    local_sem,
    send,
    receive,
):
    me, partner, across, diagonal = tensor_peers()
    meet([{"tp": partner}, {"tp": across}] + peers)
    count = len(chunks)
    held = [
        pltpu.make_async_copy(p_ref.at[:, across], passing, local_sem.at[0]),
        pltpu.make_async_copy(p_ref.at[:, me], kept, local_sem.at[1]),
    ]
    for copy in held:
        copy.start()
    first, second, third = [], [], []
    for i, (h, rows) in enumerate(chunks):
        first.append(
            remote(
                p_ref.at[h, diagonal, rows],
                pair.at[h, rows],
                send.at[i],
                receive.at[i],
                tp=partner,
            )
        )
        first[-1].start()
    for i, (h, rows) in enumerate(chunks):
        second.append(
            remote(
                p_ref.at[h, partner, rows],
                mine.at[h, rows],
                send.at[count + i],
                receive.at[count + i],
                tp=partner,
            )
        )
        second[-1].start()
    finish = launch()
    for copy in held:
        copy.wait()
    for i, (h, rows) in enumerate(chunks):
        first[i].wait_recv()
        joined[h, rows] = (
            passing[h, rows].astype(F32) + pair[h, rows].astype(F32)
        ).astype(BF)
        third.append(
            remote(
                joined.at[h, rows],
                far.at[h, rows],
                send.at[2 * count + i],
                receive.at[2 * count + i],
                tp=across,
            )
        )
        if i > 0:
            third[i - 1].start()
    for i, (h, rows) in enumerate(chunks):
        second[i].wait_recv()
        out_ref[h, rows] = kept[h, rows].astype(F32) + mine[h, rows].astype(F32)
        if i == 0:
            third[-1].start()
    for i, (h, rows) in enumerate(chunks):
        third[i].wait_recv()
        out_ref[h, rows] += far[h, rows].astype(F32)
    for i in range(count):
        first[i].wait_send()
        second[i].wait_send()
        third[i].wait_send()
    finish()


def tensor_scatter(partial, rider=None, number=1):
    halves, _, rows, width = partial.shape
    chunks = row_chunks(halves, rows, 2)
    block = pltpu.VMEM((halves, rows, width), BF)
    return call_tensor(
        functools.partial(scatter_kernel, chunks),
        partial,
        jax.ShapeDtypeStruct((halves, rows, width), F32),
        [block] * 6
        + [
            pltpu.SemaphoreType.DMA((2,)),
            pltpu.SemaphoreType.DMA((3 * len(chunks),)),
            pltpu.SemaphoreType.DMA((3 * len(chunks),)),
        ],
        rider,
        number,
        "tensor_scatter",
        in_spec=pl.BlockSpec(memory_space=pl.ANY),
    )


def opening_kernel(
    n, x_ref, q_ref, k_ref, v_ref, o_ref, out_ref, qkv_ref, full_o_ref, local, send, receive
):
    me, partner, across, _ = tensor_peers()
    ctx = lax.axis_index("ctx")
    other = 1 - ctx
    z = lax.axis_index("fsdp")
    weights = [(q_ref, 0), (k_ref, 1), (v_ref, 2)]
    rows_w = q_ref.shape[0]
    cols_w = q_ref.shape[1]
    half = rows_w // 2
    o_half = o_ref.shape[0] // 2
    o_cols = o_ref.shape[1]
    others = [lax.rem(z + d, n) for d in range(1, n)]
    meet(
        [{"tp": partner}, {"tp": across}, {"ctx": other}] + [{"fsdp": target} for target in others]
    )
    used = [0]

    def launch(source, target, **where):
        i = used[0]
        used[0] += 1
        copy = remote(source, target, send.at[i], receive.at[i], **where)
        copy.start()
        return copy

    def weight_rows(h):
        return pl.ds(pl.multiple_of(h * half, half), half)

    def output_rows(h):
        return pl.ds(pl.multiple_of(h * o_half, o_half), o_half)

    def output_cols(block):
        return pl.ds(pl.multiple_of(block * o_cols, o_cols), o_cols)

    swap = launch(x_ref.at[other], out_ref.at[ctx, me], ctx=other)
    over = [launch(x_ref.at[ctx], out_ref.at[ctx, me], tp=across)]
    side = [launch(x_ref.at[ctx], out_ref.at[ctx, me], tp=partner)]
    along = {}
    order = sorted(range(1, n), key=lambda d: min(d, n - d))
    for d in order:
        target = others[d - 1]
        group = []
        for ref, at in weights:
            group.append(
                launch(
                    ref.at[weight_rows(ctx)],
                    qkv_ref.at[z, weight_rows(ctx), pl.ds(at * cols_w, cols_w)],
                    fsdp=target,
                )
            )
        group.append(
            launch(
                o_ref.at[output_rows(ctx)],
                full_o_ref.at[output_rows(ctx), output_cols(z)],
                fsdp=target,
            )
        )
        along[d] = group
    own = [pltpu.make_async_copy(x_ref.at[ctx], out_ref.at[ctx, me], local.at[0])]
    for ref, at in weights:
        own.append(
            pltpu.make_async_copy(
                ref, qkv_ref.at[z, :, pl.ds(at * cols_w, cols_w)], local.at[1 + at]
            )
        )
    own.append(pltpu.make_async_copy(o_ref, full_o_ref.at[:, output_cols(z)], local.at[4]))
    for copy in own:
        copy.start()
    swap.wait_recv()
    over.append(launch(out_ref.at[other, me], out_ref.at[other, me], tp=across))
    side.append(launch(out_ref.at[other, me], out_ref.at[other, me], tp=partner))
    over[0].wait_recv()
    relay = [launch(out_ref.at[ctx, across], out_ref.at[ctx, across], tp=partner)]
    handed = []
    for d in order:
        block = lax.rem(z + n - d, n)
        for copy, (_, at) in zip(along[d], weights):
            copy.wait_recv()
            piece = qkv_ref.at[block, weight_rows(ctx), pl.ds(at * cols_w, cols_w)]
            handed.append(launch(piece, piece, ctx=other))
        along[d][-1].wait_recv()
        piece = full_o_ref.at[output_rows(ctx), output_cols(block)]
        handed.append(launch(piece, piece, ctx=other))
        if d == order[0]:
            over[1].wait_recv()
            relay.append(launch(out_ref.at[other, across], out_ref.at[other, across], tp=partner))
    for copy in side + relay + handed:
        copy.wait_recv()
    for copy in [swap] + over + side + relay + handed:
        copy.wait_send()
    for d in order:
        for copy in along[d]:
            copy.wait_send()
    for copy in own:
        copy.wait()


def opening(n, rows, query, key, value, output):
    _, count, width = rows.shape
    copies = 7 + 8 * (n - 1)
    gathered, qkv, full_output = pl.pallas_call(
        functools.partial(opening_kernel, n),
        out_shape=(
            jax.ShapeDtypeStruct((2, 4, count, width), BF),
            jax.ShapeDtypeStruct((n, query.shape[0], 3 * query.shape[1]), BF),
            jax.ShapeDtypeStruct((output.shape[0], n * output.shape[1]), BF),
        ),
        in_specs=[IN_VMEM] * 5,
        out_specs=(IN_VMEM,) * 3,
        scratch_shapes=[
            pltpu.SemaphoreType.DMA((5,)),
            pltpu.SemaphoreType.DMA((copies,)),
            pltpu.SemaphoreType.DMA((copies,)),
        ],
        compiler_params=pltpu.CompilerParams(collective_id=2, has_side_effects=True),
        cost_estimate=pl.CostEstimate(flops=0, bytes_accessed=60_000_000, transcendentals=0),
        name="opening",
    )(rows, query, key, value, output)
    return gathered, qkv.reshape(n * query.shape[0], 3 * query.shape[1]), full_output


def closing_kernel(
    n,
    g_ref,
    v_ref,
    early_ref,
    input_ref,
    out_ref,
    sums_ref,
    full_early_ref,
    traded_ref,
    far,
    pair,
    joined,
    group,
    send,
    receive,
    vector_send,
    vector_receive,
    share_send,
    share_receive,
    local,
):
    me, _, _, _ = tensor_peers()
    ctx = lax.axis_index("ctx")
    other = 1 - ctx
    z = lax.axis_index("fsdp")
    blocks = [lax.rem(z + d, n) for d in range(n)]
    around = [lax.rem(me + d, 4) for d in range(1, 4)]
    meet(
        [{"ctx": other}]
        + [{"fsdp": block} for block in blocks[1:]]
        + [{"tp": index} for index in around]
    )
    swap = remote(v_ref, pair, vector_send.at[0], vector_receive.at[0], ctx=other)
    swap.start()
    order = sorted(range(1, n), key=lambda d: -min(d, n - d))
    along = {}
    for d in order:
        along[d] = remote(
            g_ref.at[blocks[d]], far.at[d], send.at[d], receive.at[d], fsdp=blocks[d]
        )
        along[d].start()
    shares = [
        remote(early_ref, full_early_ref.at[ctx], share_send.at[0], share_receive.at[0], ctx=other),
        remote(
            input_ref.at[other], traded_ref.at[ctx], share_send.at[1], share_receive.at[1], ctx=other
        ),
    ]
    own = [
        pltpu.make_async_copy(early_ref, full_early_ref.at[ctx], local.at[0]),
        pltpu.make_async_copy(input_ref.at[ctx], traded_ref.at[ctx], local.at[1]),
    ]
    for copy in shares + own:
        copy.start()
    swap.wait_recv()
    joined[...] = v_ref[...] + pair[...]
    group[z] = joined[...]
    line = [
        remote(joined, group.at[z], vector_send.at[d], vector_receive.at[d], fsdp=blocks[d])
        for d in range(1, n)
    ]
    for copy in own:
        copy.wait()
    for copy in line:
        copy.start()
    total = g_ref[z].astype(F32)
    for d in order:
        along[d].wait_recv()
        total = total + far[d].astype(F32)
    out_ref[ctx] = total.astype(BF)
    for copy in line:
        copy.wait_recv()
    summed = group[0]
    for i in range(1, n):
        summed = summed + group[i]
    sums_ref[me] = summed
    ring = [
        remote(
            sums_ref.at[me],
            sums_ref.at[me],
            vector_send.at[n + i],
            vector_receive.at[n + i],
            tp=index,
        )
        for i, index in enumerate(around)
    ]
    last = remote(out_ref.at[ctx], out_ref.at[ctx], send.at[0], receive.at[0], ctx=other)
    last.start()
    for d in order:
        along[d].wait_send()
    for copy in ring:
        copy.start()
    for copy in ring + shares:
        copy.wait_recv()
    for copy in [swap] + line + ring + shares:
        copy.wait_send()
    last.wait_recv()
    last.wait_send()


def closing(n, terms, vectors, early, traded):
    _, rows, width = terms.shape
    vector = pltpu.VMEM(vectors.shape, F32)
    out, sums, early, traded = pl.pallas_call(
        functools.partial(closing_kernel, n),
        out_shape=(
            jax.ShapeDtypeStruct((2, rows, width), BF),
            jax.ShapeDtypeStruct((4,) + vectors.shape, F32),
            jax.ShapeDtypeStruct((2,) + early.shape, BF),
            jax.ShapeDtypeStruct(traded.shape, BF),
        ),
        in_specs=[IN_VMEM] * 4,
        out_specs=(IN_VMEM,) * 4,
        scratch_shapes=[
            pltpu.VMEM((n, rows, width), BF),
            vector,
            vector,
            pltpu.VMEM((n,) + vectors.shape, F32),
            pltpu.SemaphoreType.DMA((n,)),
            pltpu.SemaphoreType.DMA((n,)),
            pltpu.SemaphoreType.DMA((n + 3,)),
            pltpu.SemaphoreType.DMA((n + 3,)),
            pltpu.SemaphoreType.DMA((2,)),
            pltpu.SemaphoreType.DMA((2,)),
            pltpu.SemaphoreType.DMA((2,)),
        ],
        compiler_params=pltpu.CompilerParams(collective_id=3, has_side_effects=True),
        cost_estimate=pl.CostEstimate(flops=0, bytes_accessed=120_000_000, transcendentals=0),
        name="closing",
    )(terms, vectors, early, traded)
    return out.reshape(2 * rows, width), sums, early.reshape(-1, early.shape[2]), traded


def unit_rows(values):
    return values * lax.rsqrt(jnp.mean(values * values, axis=-1, keepdims=True) + norm_eps)


def rotate_pairs(values, angles):
    middle = values.shape[-1] // 2
    leading = values[..., :middle]
    trailing = values[..., middle:]
    cosine = jnp.cos(angles)[..., None, :]
    sine_part = jnp.sin(angles)[..., None, :]
    return jnp.concatenate(
        [leading * cosine - trailing * sine_part, trailing * cosine + leading * sine_part], axis=-1
    )


def angles_for(positions, head_size):
    middle = head_size // 2
    frequency = rope_base ** (-2.0 * jnp.arange(middle).astype(F32) / head_size)
    return positions.astype(F32)[..., None] * frequency


def prepare_heads(projected, angles, gains, head_size):
    heads_here = projected.shape[-1] // head_size
    shaped = projected.reshape(projected.shape[:-1] + (heads_here, head_size))
    normed = unit_rows(rotate_pairs(shaped, angles)) * gains.reshape(heads_here, head_size)
    return normed.reshape(projected.shape)


def product(left, right):
    return jnp.dot(left, right, preferred_element_type=F32)


def transposed_left(left, right):
    return lax.dot_general(left, right, (((0,), (0,)), ((), ())), preferred_element_type=F32)


def transposed_right(left, right):
    return lax.dot_general(left, right, (((1,), (1,)), ((), ())), preferred_element_type=F32)


def branch_mix(branch, base, rate):
    return unit_rows(base + rate * (unit_rows(branch) - base))


def activate(upper, gated_raw, amplitude, steepness):
    scaled = gated_raw * steepness
    return upper * amplitude * (scaled * jax.nn.sigmoid(scaled))


def trade(values, sizes):
    n = sizes["ctx"]
    me = lax.axis_index("ctx")
    if n == 2:
        own = lax.dynamic_index_in_dim(values, me, 0, keepdims=False)
        other = lax.dynamic_index_in_dim(values, 1 - me, 0, keepdims=False)
        got = lax.ppermute(other, "ctx", [(0, 1), (1, 0)])
        first = jnp.where(me == 0, own, got)
        second = jnp.where(me == 0, got, own)
        return jnp.stack([first, second])
    return lax.all_to_all(values, "ctx", split_axis=0, concat_axis=0, tiled=True)


def finish_kernel(late_ref, early_ref, *outs):
    query, key, value, output, up, gate, down = outs
    cols = query.shape[1]
    for at, ref in enumerate((query, key, value)):
        ref[...] = late_ref[:, at * cols : (at + 1) * cols].astype(F32)
    output[...] = late_ref[:, 3 * cols :].astype(F32).T
    hidden = up.shape[1]
    down[...] = early_ref[:, :hidden].astype(F32).T
    up[...] = early_ref[:, hidden : 2 * hidden].astype(F32)
    gate[...] = early_ref[:, 2 * hidden :].astype(F32)


def finish(late, early, cols, hidden):
    rows = late.shape[0]
    shapes = [(rows, cols)] * 3 + [(late.shape[1] - 3 * cols, rows)]
    shapes += [(rows, hidden)] * 2 + [(hidden, rows)]
    return pl.pallas_call(
        finish_kernel,
        out_shape=[jax.ShapeDtypeStruct(shape, F32) for shape in shapes],
        in_specs=[IN_VMEM] * 2,
        out_specs=[IN_VMEM] * 7,
        cost_estimate=pl.CostEstimate(flops=0, bytes_accessed=8 * 10**6, transcendentals=0),
        name="finish",
    )(late, early)


def tiles_of(length):
    return [pl.ds(i * BLK, BLK) for i in range(length // BLK)]


def scores_of(keys, query, col_ref, row_ref, tiles, a, j):
    scores = jnp.dot(keys[tiles[j], :], query, preferred_element_type=F32)
    if j >= a:
        scores = jnp.where(col_ref[tiles[j], :] <= row_ref[:, tiles[a]], scores, -1e30)
    return scores


def attend_kernel(q_ref, k_ref, v_ref, col_ref, row_ref, o_ref, lse_ref, keys):
    tiles = tiles_of(q_ref.shape[2])

    def one_head(h, carry):
        keys[...] = k_ref[h].T
        for a in range(len(tiles)):
            query = q_ref[h, :, tiles[a]]
            total = jnp.zeros((1, BLK), F32)
            out = jnp.zeros((HD, BLK), F32)
            for j in range(min(a + 2, len(tiles))):
                soft = jnp.exp(scores_of(keys, query, col_ref, row_ref, tiles, a, j))
                total += jnp.sum(soft, axis=0, keepdims=True)
                out += jnp.dot(v_ref[h, :, tiles[j]], soft.astype(BF), preferred_element_type=F32)
            o_ref[h, :, tiles[a]] = (out / total).astype(BF)
            lse_ref[h, :, tiles[a]] = jnp.log(total)
        return carry

    lax.fori_loop(0, q_ref.shape[0], one_head, 0)


def attend_both(query, key, value, ids):
    heads, _, length = query.shape
    return pl.pallas_call(
        attend_kernel,
        out_shape=(
            jax.ShapeDtypeStruct(query.shape, BF),
            jax.ShapeDtypeStruct((heads, 1, length), F32),
        ),
        in_specs=[IN_VMEM] * 5,
        out_specs=(IN_VMEM,) * 2,
        scratch_shapes=[pltpu.VMEM((length, HD), BF)],
        cost_estimate=pl.CostEstimate(flops=10**9, bytes_accessed=3 * 10**7, transcendentals=0),
        name="attend",
    )(query, key, value, ids[:, None], ids[None, :])


def attend_back_kernel(
    q_ref, k_ref, v_ref, col_ref, row_ref, lse_ref, o_ref, g_ref, dq_ref, dk_ref, dv_ref, keys, values
):
    tiles = tiles_of(q_ref.shape[2])
    last = (((1,), (1,)), ((), ()))

    def one_head(h, carry):
        keys[...] = k_ref[h].T
        values[...] = v_ref[h].T
        dk_ref[h] = jnp.zeros_like(dk_ref[h])
        dv_ref[h] = jnp.zeros_like(dv_ref[h])
        for a in range(len(tiles)):
            query = q_ref[h, :, tiles[a]]
            grad = g_ref[h, :, tiles[a]]
            lse = lse_ref[h, :, tiles[a]]
            delta = jnp.sum(
                grad.astype(F32) * o_ref[h, :, tiles[a]].astype(F32), axis=0, keepdims=True
            )
            dq = jnp.zeros((HD, BLK), F32)
            for j in range(min(a + 2, len(tiles))):
                scores = scores_of(keys, query, col_ref, row_ref, tiles, a, j)
                soft = jnp.exp(scores - lse)
                dp = jnp.dot(values[tiles[j], :], grad, preferred_element_type=F32)
                low = (soft * (dp - delta)).astype(BF)
                dv_ref[h, :, tiles[j]] += lax.dot_general(
                    grad, soft.astype(BF), last, preferred_element_type=F32
                )
                dk_ref[h, :, tiles[j]] += lax.dot_general(
                    query, low, last, preferred_element_type=F32
                )
                dq += jnp.dot(k_ref[h, :, tiles[j]], low, preferred_element_type=F32)
            dq_ref[h, :, tiles[a]] = dq * (1 / math.sqrt(HD))
        return carry

    lax.fori_loop(0, q_ref.shape[0], one_head, 0)


def attend_back(query, key, value, ids, logsum, out, grad):
    heads, _, length = query.shape
    shape = jax.ShapeDtypeStruct(query.shape, F32)
    return pl.pallas_call(
        attend_back_kernel,
        out_shape=(shape,) * 3,
        in_specs=[IN_VMEM] * 8,
        out_specs=(IN_VMEM,) * 3,
        scratch_shapes=[pltpu.VMEM((length, HD), BF)] * 2,
        cost_estimate=pl.CostEstimate(flops=3 * 10**9, bytes_accessed=6 * 10**7, transcendentals=0),
        name="attend_back",
    )(query, key, value, ids[:, None], ids[None, :], logsum, out, grad)


def tokens_minor(values):
    return values.T.reshape(-1, HD, values.shape[0])


def tokens_major(values):
    return values.reshape(-1, values.shape[2]).T


def swap_halves(share, ctx):
    got = lax.ppermute(share, "ctx", [(0, 1), (1, 0)])
    first = jnp.where(ctx == 0, share, got)
    second = jnp.where(ctx == 0, got, share)
    return jnp.concatenate([first, second], axis=0)


def per_device(sizes):
    def run(
        residual,
        query_weight,
        key_weight,
        value_weight,
        output_weight,
        sharpness,
        attend_rate,
        up_weight,
        gate_weight,
        down_weight,
        amplitude,
        steepness,
        mixer_rate,
        block_ids,
        positions,
        cotangent,
    ):
        n = sizes["fsdp"]
        tp = sizes["tp"]
        rows, width = residual.shape[1:]
        hidden_here = up_weight.shape[1]
        heads_width = query_weight.shape[1]
        small = n <= 4
        shape4 = (2, tp, rows, width)

        ctx = lax.axis_index("ctx")

        def own_half(shard):
            half = shard.shape[0] // 2
            return lax.dynamic_slice_in_dim(shard, ctx * half, half, 0)

        late_half = own_half(jnp.concatenate([up_weight, gate_weight, down_weight.T], axis=1))
        if small:
            gathered, full_qkv, full_output = opening(
                n, residual, query_weight, key_weight, value_weight, output_weight
            )
            tensor_index = lax.axis_index("tp")
            mine = lax.dynamic_index_in_dim(gathered, tensor_index, 1, keepdims=False)
        else:
            mine = trade(residual, sizes)
            qkv_shard = jnp.concatenate([query_weight, key_weight, value_weight], axis=1)
            full_qkv = lax.all_gather(qkv_shard, "fsdp", axis=0, tiled=True)
            full_output = lax.all_gather(output_weight, "fsdp", axis=1, tiled=True)
            gathered = tensor_gather(mine)
        full_late = lax.all_gather(late_half, ("fsdp", "ctx"), axis=0, tiled=True)
        full_ug = full_late[:, : 2 * hidden_here]
        full_down = full_late[:, 2 * hidden_here :]

        ids = lax.dynamic_index_in_dim(block_ids, ctx, 0, keepdims=False)
        my_positions = trade(positions, sizes).reshape(-1)
        angles = angles_for(my_positions, HD)

        flat_in = gathered.reshape(-1, width)
        raw = product(flat_in, full_qkv)
        raw_query, raw_key, raw_value = jnp.split(raw, 3, axis=1)

        def prepare_local(projected, gains):
            return prepare_heads(projected, angles, gains, HD)

        query_ready, query_back = jax.vjp(prepare_local, raw_query, sharpness)
        key_ready, key_back = jax.vjp(prepare_local, raw_key, sharpness)
        query_low = tokens_minor(query_ready.astype(BF) * BF(1 / math.sqrt(HD)))
        key_low = tokens_minor(key_ready.astype(BF))
        value_low = tokens_minor(raw_value.astype(BF))
        attended, logsum = attend_both(query_low, key_low, value_low, ids)
        flat_attended = attended.reshape(heads_width, -1)

        def reduce_rows(partial, *rider):
            return tensor_scatter(partial.astype(BF).reshape(shape4), *rider)

        def gather_rows(values):
            return tensor_gather(values.astype(BF)).reshape(-1, width)

        attend_sum = reduce_rows(transposed_left(flat_attended, full_output))
        residual_float = mine.astype(F32)
        first, attend_back_mix = jax.vjp(branch_mix, attend_sum, residual_float, attend_rate)
        first_all = gather_rows(first)
        ug_raw = product(first_all, full_ug)
        up_raw, gate_raw = ug_raw[:, :hidden_here], ug_raw[:, hidden_here:]
        hidden, activate_back = jax.vjp(activate, up_raw, gate_raw, amplitude, steepness)
        hidden_low = hidden.astype(BF)
        down_sum = reduce_rows(transposed_right(hidden_low, full_down))
        outcome, mixer_back = jax.vjp(branch_mix, down_sum, first, mixer_rate)
        layer_out = trade(outcome.astype(BF), sizes)
        my_cot = trade(cotangent, sizes)
        grad_down_sum, grad_first, grad_mixer_part = mixer_back(my_cot.astype(F32))
        down_grad_all = gather_rows(grad_down_sum)
        grad_hidden = product(down_grad_all, full_down)
        grad_down_part = transposed_left(down_grad_all, hidden_low)
        grad_up_raw, grad_gate_raw, grad_amplitude_part, grad_steepness_part = activate_back(
            grad_hidden
        )
        ug_grad = jnp.concatenate([grad_up_raw.astype(BF), grad_gate_raw.astype(BF)], axis=1)
        grad_first = grad_first + reduce_rows(transposed_right(ug_grad, full_ug))
        grad_ug_part = transposed_left(first_all, ug_grad)
        grad_attend_sum, grad_residual, grad_attend_part = attend_back_mix(grad_first)
        attend_grad_all = gather_rows(grad_attend_sum)
        grad_output_part = product(flat_attended, attend_grad_all).T
        grad_attended = transposed_right(full_output, attend_grad_all).astype(BF)
        grad_query_ready, grad_key_ready, grad_value_ready = [
            tokens_major(part)
            for part in attend_back(
                query_low,
                key_low,
                value_low,
                ids,
                logsum,
                attended,
                grad_attended.reshape(attended.shape),
            )
        ]
        grad_raw_query, sharp_query = query_back(grad_query_ready)
        grad_raw_key, sharp_key = key_back(grad_key_ready)
        qkv_grad = jnp.concatenate(
            [grad_raw_query.astype(BF), grad_raw_key.astype(BF), grad_value_ready.astype(BF)], axis=1
        )
        grad_qkv_part = transposed_left(flat_in, qkv_grad)
        late = jnp.concatenate([grad_qkv_part.astype(BF), grad_output_part.astype(BF)], axis=1)
        partial = transposed_right(qkv_grad, full_qkv)
        if small:
            late = late.reshape(n, 2, -1, late.shape[1])
            summed, late_terms = reduce_rows(partial, Near(n, late), 5)
        else:
            summed = reduce_rows(partial)
        grad_input = (grad_residual + summed).astype(BF)

        def scatter_rows(part):
            return lax.psum_scatter(
                part.astype(BF), ("fsdp", "ctx"), scatter_dimension=0, tiled=True
            )

        vectors = [
            sharp_query + sharp_key,
            grad_amplitude_part,
            grad_steepness_part,
            grad_attend_part,
            grad_mixer_part,
        ]
        lengths = [vector.shape[0] for vector in vectors]
        packed = jnp.concatenate(vectors)
        packed = jnp.pad(packed, (0, -packed.shape[0] % 1024)).reshape(-1, 128)
        early = scatter_rows(
            jnp.concatenate([grad_down_part.astype(BF), grad_ug_part.astype(BF)], axis=1)
        )
        if small:
            late, sums, early, grad_input = closing(n, late_terms, packed, early, grad_input)
        else:
            late = swap_halves(scatter_rows(late), ctx)
            sums = lax.all_gather(lax.psum(packed, ("fsdp", "ctx")), "tp", axis=0)
            early = swap_halves(early, ctx)
            grad_input = trade(grad_input, sizes)
        grad_query, grad_key, grad_value, grad_output, grad_up, grad_gate, grad_down = finish(
            late, early, heads_width, hidden_here
        )
        grad_input = grad_input.astype(F32)
        sums = sums.reshape(tp, -1)
        pieces = []
        start = 0
        for length in lengths:
            pieces.append(sums[:, start : start + length])
            start += length
        grad_sharpness, grad_amplitude, grad_steepness = [p.reshape(-1) for p in pieces[:3]]
        grad_attend, grad_mixer = [p.sum(axis=0) for p in pieces[3:]]
        return (
            layer_out,
            grad_input,
            grad_query,
            grad_key,
            grad_value,
            grad_output,
            grad_sharpness,
            grad_attend,
            grad_up,
            grad_gate,
            grad_down,
            grad_amplitude,
            grad_steepness,
            grad_mixer,
        )

    return run


def solution(mesh):
    return jax.shard_map(
        per_device(dict(mesh.shape)),
        mesh=mesh,
        in_specs=(
            P("fsdp", ("ctx", "tp"), None),
            P("fsdp", "tp"),
            P("fsdp", "tp"),
            P("fsdp", "tp"),
            P("tp", "fsdp"),
            P("tp"),
            P(),
            P("fsdp", "tp"),
            P("fsdp", "tp"),
            P("tp", "fsdp"),
            P("tp"),
            P("tp"),
            P(),
            P("fsdp", None),
            P("fsdp", "ctx"),
            P("fsdp", ("ctx", "tp"), None),
        ),
        out_specs=(
            P("fsdp", ("ctx", "tp"), None),
            P("fsdp", ("ctx", "tp"), None),
            P("fsdp", "tp"),
            P("fsdp", "tp"),
            P("fsdp", "tp"),
            P("tp", "fsdp"),
            P(),
            P(),
            P("fsdp", "tp"),
            P("fsdp", "tp"),
            P("tp", "fsdp"),
            P(),
            P(),
            P(),
        ),
        check_vma=False,
    )
```
